32 devices in a mesh: data: 32 (over z, y, x, core).
Axes of the slice: x: 2, y: 2, z: 4, core: 2. Of those that a mesh axis runs over, the one named last changes fastest.
Arguments:
- tokens: bfloat16 [262144, 384], P('data')
- out_grad: bfloat16 [262144, 384], P('data')
- w_up: bfloat16 [2, 384, 1536], replicated
- w_down: bfloat16 [2, 1536, 384], replicated
- a_up_old: float32 [2, 384, 384], replicated
- s_up_old: float32 [2, 1536, 1536], replicated
- a_down_old: float32 [2, 1536, 1536], replicated
- s_down_old: float32 [2, 384, 384], replicated
- a_up_inv: float32 [2, 384, 384], replicated
- s_up_inv: float32 [2, 1536, 1536], replicated
- a_down_inv: float32 [2, 1536, 1536], replicated
- s_down_inv: float32 [2, 384, 384], replicated
- factor_decay: float32 [], replicated
Outputs:
- output 1: float32 [2, 384, 1536], replicated
- output 2: float32 [2, 1536, 384], replicated
- output 3: float32 [2, 384, 384], replicated
- output 4: float32 [2, 1536, 1536], replicated
- output 5: float32 [2, 1536, 1536], replicated
- output 6: float32 [2, 384, 384], replicated
All inputs are finite; a program needn't handle non-finite values.
Results may differ from the reference program's by a relative error of at most 0.00153868.
Values are sent between devices in bfloat16 or wider.
A program may use at most 1 GiB of HBM per device.

```python
import math
import jax
import jax.numpy as jnp
from jax import lax

D = 384
FF = 1536
TOK_DEV = 8192
SHARDS = 32
BLOCKS = 2


def gelu_fn(pre_act):
    return jax.nn.gelu(pre_act, approximate=True)


def spd_draw(rng_key, width, diag_low, diag_high):
    key_diag, key_low = jax.random.split(rng_key)
    diag_part = jax.random.uniform(key_diag, (BLOCKS, width), jnp.float32, diag_low, diag_high)
    low_rank = jax.random.normal(key_low, (BLOCKS, width, 64), jnp.float32)
    outer_part = jnp.einsum("bik,bjk->bij", low_rank, low_rank) / math.sqrt(width * 64.0)
    return outer_part + diag_part[:, :, None] * jnp.eye(width, dtype=jnp.float32)[None]


def shifted_rows(key_scale, key_shift, key_noise):
    row_scale = jnp.exp(1.5 * jax.random.uniform(key_scale, (SHARDS, 1, 1), jnp.float32, -1.0, 1.0))
    row_shift = 0.7 * jax.random.normal(key_shift, (SHARDS, 1, D), jnp.float32)
    row_noise = jax.random.normal(key_noise, (SHARDS, TOK_DEV, D), jnp.float32)
    return (row_noise * row_scale + row_shift).reshape(SHARDS * TOK_DEV, D).astype(jnp.bfloat16)


def setup_inputs(seed: int = 0) -> dict:
    sub_keys = jax.random.split(jax.random.key(seed), 17)
    w_up = jax.random.normal(sub_keys[6], (BLOCKS, D, FF), jnp.float32) / math.sqrt(D)
    w_down = jax.random.normal(sub_keys[7], (BLOCKS, FF, D), jnp.float32) / math.sqrt(FF)
    return {
        "tokens": shifted_rows(sub_keys[0], sub_keys[1], sub_keys[2]),
        "out_grad": shifted_rows(sub_keys[3], sub_keys[4], sub_keys[5]),
        "w_up": w_up.astype(jnp.bfloat16),
        "w_down": w_down.astype(jnp.bfloat16),
        "a_up_old": 0.3 * spd_draw(sub_keys[8], D, 0.5, 1.5),
        "s_up_old": 0.3 * spd_draw(sub_keys[9], FF, 0.5, 1.5),
        "a_down_old": 0.3 * spd_draw(sub_keys[10], FF, 0.5, 1.5),
        "s_down_old": 0.3 * spd_draw(sub_keys[11], D, 0.5, 1.5),
        "a_up_inv": spd_draw(sub_keys[12], D, 0.5, 1.5),
        "s_up_inv": spd_draw(sub_keys[13], FF, 0.5, 1.5),
        "a_down_inv": spd_draw(sub_keys[14], FF, 0.5, 1.5),
        "s_down_inv": spd_draw(sub_keys[15], D, 0.5, 1.5),
        "factor_decay": jax.random.uniform(sub_keys[16], (), jnp.float32, 0.6, 0.9),
    }


def cross_sum(left, right):
    return jnp.dot(left.T, right, preferred_element_type=jnp.float32)


def reference(tokens, out_grad, w_up, w_down, a_up_old, s_up_old, a_down_old, s_down_old,
              a_up_inv, s_up_inv, a_down_inv, s_down_inv, factor_decay):
    batch_total = SHARDS * TOK_DEV

    def shard_step(carry, rows_pair):
        tok_rows, grad_rows = rows_pair
        layer_ins = []
        pre_ups = []
        hiddens = []
        layer_in = tok_rows
        for block_idx in range(BLOCKS):
            pre_up = jnp.dot(layer_in, w_up[block_idx], preferred_element_type=jnp.float32).astype(jnp.bfloat16)
            hidden = gelu_fn(pre_up.astype(jnp.float32)).astype(jnp.bfloat16)
            layer_ins.append(layer_in)
            pre_ups.append(pre_up)
            hiddens.append(hidden)
            if block_idx + 1 < BLOCKS:
                layer_in = jnp.dot(hidden, w_down[block_idx], preferred_element_type=jnp.float32).astype(jnp.bfloat16)
        found = [[], [], [], [], [], []]
        grad_down = grad_rows
        for block_idx in reversed(range(BLOCKS)):
            hidden = hiddens[block_idx]
            layer_in = layer_ins[block_idx]
            d_hidden = jnp.dot(grad_down, w_down[block_idx].T, preferred_element_type=jnp.float32).astype(jnp.bfloat16)
            gelu_back = jax.vjp(gelu_fn, pre_ups[block_idx].astype(jnp.float32))[1]
            grad_up = gelu_back(d_hidden.astype(jnp.float32))[0].astype(jnp.bfloat16)
            terms = (cross_sum(layer_in, grad_up), cross_sum(hidden, grad_down),
                     cross_sum(layer_in, layer_in), cross_sum(grad_up, grad_up),
                     cross_sum(hidden, hidden), cross_sum(grad_down, grad_down))
            for slot, term in enumerate(terms):
                found[slot].insert(0, term)
            if block_idx > 0:
                grad_down = jnp.dot(grad_up, w_up[block_idx].T, preferred_element_type=jnp.float32).astype(jnp.bfloat16)
        return tuple(acc_sum + jnp.stack(items) for acc_sum, items in zip(carry, found)), None

    zero_init = (jnp.zeros((BLOCKS, D, FF), jnp.float32), jnp.zeros((BLOCKS, FF, D), jnp.float32),
                 jnp.zeros((BLOCKS, D, D), jnp.float32), jnp.zeros((BLOCKS, FF, FF), jnp.float32),
                 jnp.zeros((BLOCKS, FF, FF), jnp.float32), jnp.zeros((BLOCKS, D, D), jnp.float32))
    rows_in = (tokens.reshape(SHARDS, TOK_DEV, D), out_grad.reshape(SHARDS, TOK_DEV, D))
    totals = lax.scan(shard_step, zero_init, rows_in)[0]
    dw_up, dw_down, a_up, s_up, a_down, s_down = [total / batch_total for total in totals]
    decay_keep = factor_decay
    decay_fresh = 1.0 - factor_decay
    a_up_new = decay_keep * a_up_old + decay_fresh * a_up
    s_up_new = decay_keep * s_up_old + decay_fresh * s_up
    a_down_new = decay_keep * a_down_old + decay_fresh * a_down
    s_down_new = decay_keep * s_down_old + decay_fresh * s_down
    precond_up = jnp.einsum("bij,bjk->bik", jnp.einsum("bij,bjk->bik", a_up_inv, dw_up), s_up_inv)
    precond_down = jnp.einsum("bij,bjk->bik", jnp.einsum("bij,bjk->bik", a_down_inv, dw_down), s_down_inv)
    return (precond_up, precond_down, a_up_new, s_up_new, a_down_new, s_down_new)
```

```python
import functools

import jax
import jax.numpy as jnp
from jax import lax
from jax.experimental import pallas as pl
from jax.experimental.pallas import tpu as pltpu
from jax.sharding import PartitionSpec as P

bf16 = jnp.bfloat16
f32 = jnp.float32
MESH = pl.DeviceIdType.MESH
ORDER_X = (1, 2, 3, 4)
ORDER_Y = (2, 1, 3, 4)
ORDER_Z = (3, 4, 1, 2)


D, FF, B = 384, 1536, 256
NB = FF // B
TRI = sum((j + 1) * B for j in range(NB))
NN = (((1,), (0,)), ((), ()))
NT = (((1,), (1,)), ((), ()))
TN = (((0,), (0,)), ((), ()))
TT = (((0,), (1,)), ((), ()))
GELU_K = 0.7978845608028654
GELU_C = 0.044715 * GELU_K
MIB = 1 << 20


def mm(left, right, dims):
    return lax.dot_general(left, right, dims, preferred_element_type=f32)


def half_sig(pre):
    cubic = GELU_C * (pre * pre)
    return 0.5 * jnp.tanh(pre * (cubic + GELU_K)) + 0.5, cubic


def gelu_back(pre, sig, cubic):
    hid = pre * sig
    return hid, sig + (hid * (1.0 - sig)) * (6.0 * cubic + 2.0 * GELU_K)


def add_tri(acc, mat):
    off = 0
    for j in range(NB):
        rows = (j + 1) * B
        acc[off:off + rows, :] += mm(mat[:rows, :], mat[j * B:rows, :], NT)
        off += rows


def add_small_tn(acc, rows):
    acc[0] += mm(rows[:, 0:128], rows[...], TN)
    acc[1, :, 0:256] += mm(rows[:, 128:256], rows[:, 128:384], TN)
    acc[1, :, 256:384] += mm(rows[:, 256:384], rows[:, 256:384], TN)


def add_small_nt(acc, cols):
    acc[0] += mm(cols[0:128, :], cols[...], NT)
    acc[1, :, 0:256] += mm(cols[128:256, :], cols[128:384, :], NT)
    acc[1, :, 256:384] += mm(cols[256:384, :], cols[256:384, :], NT)


def zero_first(accs):
    @pl.when(pl.program_id(0) == 0)
    def _():
        for acc in accs:
            acc[...] = jnp.zeros_like(acc)


def my_bits():
    me = lax.axis_index("data")
    return me, [(me // (1 << d)) % 2 for d in range(5)]


class Chain:
    def __init__(self, row0, rows, cols, order):
        self.row0, self.rows, self.cols, self.order = row0, rows, cols, order


def entry_barrier():
    me, bits = my_bits()
    barrier = pltpu.get_barrier_semaphore()
    for d in range(5):
        pl.semaphore_signal(barrier, inc=1, device_id=(me + (1 - 2 * bits[d]) * (1 << d),), device_id_type=MESH)
    pl.semaphore_wait(barrier, 5)


class Job:
    def __init__(self, kind, chain, src=None, shard=None, shard_row=0, dst=None, start=0.0):
        self.kind, self.chain, self.start = kind, chain, start
        self.src, self.shard, self.shard_row, self.dst = src, shard, shard_row, dst
        self.n_events = {"rs": 7, "ag": 7, "ar": 11, "fan": 6}[kind]

    def scratch(self):
        ch = self.chain
        out = []
        if self.kind in ("rs", "ar"):
            out += [pltpu.VMEM((ch.rows, ch.cols), f32), pltpu.VMEM((ch.rows * 31 // 16, ch.cols), f32)]
        elif self.kind == "ag":
            out += [pltpu.VMEM((ch.rows // 16, ch.cols), f32)]
        n = 5 if self.kind != "ar" else 10
        out += [pltpu.SemaphoreType.DMA((2,)), pltpu.SemaphoreType.DMA((n,)), pltpu.SemaphoreType.DMA((n,))]
        return out

    def messages(self):
        ch = self.chain
        size = ch.rows * ch.cols * 4
        rs = [(size, 0)] + [(size >> (k + 1), ch.order[k]) for k in range(4)]
        ag = [(size >> (k + 1), ch.order[k]) for k in (3, 2, 1, 0)] + [(size, 0)]
        return {"rs": rs + [(0, None)], "ag": [(0, None)] + ag, "fan": ag, "ar": rs + ag + [(0, None)]}[self.kind]

    def bind(self, refs, scr):
        ch = self.chain
        rows, half = ch.rows, ch.rows // 2
        me, bits = my_bits()
        core = bits[0]
        peers = [me + (1 - 2 * bits[d]) * (1 << d) for d in range(5)]
        offs, lens = [0], [rows]
        for d in ch.order:
            lens.append(lens[-1] // 2)
            offs.append(offs[-1] + bits[d] * lens[-1])
        starts = [0, rows, rows * 3 // 2, rows * 7 // 4, rows * 15 // 8]
        al = lambda v: pl.multiple_of(v, 8)
        if self.kind == "ag":
            buf, sem_l, sem_s, sem_r = scr
            sem0 = 0
        elif self.kind == "fan":
            sem_l, sem_s, sem_r = scr
            sem0 = 0
        else:
            work, recv, sem_l, sem_s, sem_r = scr
            sem0 = 5
        src = refs.get(self.src)
        dst = refs.get(self.dst)
        shard = refs.get(self.shard)

        def remote(a, b, i, d):
            return pltpu.make_async_remote_copy(src_ref=a, dst_ref=b, send_sem=sem_s.at[i], recv_sem=sem_r.at[i],
                                                device_id=(peers[d],), device_id_type=MESH)

        events = []
        if self.kind in ("rs", "ar"):
            load = pltpu.make_async_copy(src.at[core, pl.ds(ch.row0, rows), :], work, sem_l.at[0])
            first = remote(src.at[1 - core, pl.ds(ch.row0, rows), :], recv.at[pl.ds(0, rows), :], 0, 0)
            sends = [first]
            for k in range(4):
                gone = al(offs[k] + (1 - bits[ch.order[k]]) * lens[k + 1])
                sends.append(remote(work.at[pl.ds(gone, lens[k + 1]), :], recv.at[pl.ds(starts[k + 1], lens[k + 1]), :],
                                    k + 1, ch.order[k]))

            def add(at, frm, count):
                for q in range(0, count, 64):
                    step = min(count - q, 64)
                    a = al(at + q)
                    b = al(frm + q)
                    work[pl.ds(a, step), :] = work[pl.ds(a, step), :] + recv[pl.ds(b, step), :]

            def begin():
                load.start()
                first.start()

            def fold(k):
                def run():
                    if k == 0:
                        load.wait()
                    sends[k].wait_recv()
                    if k < 4:
                        n = lens[k + 1]
                        b = bits[ch.order[k]]
                        add(offs[k] + (1 - b) * n, starts[k] + (1 - b) * n, n)
                        sends[k + 1].start()
                        add(offs[k] + b * n, starts[k] + b * n, n)
                    else:
                        add(offs[4], starts[4], lens[4])
                        tail()
                return run

            events += [begin] + [fold(k) for k in range(5)]
            final = work.at[pl.ds(al(offs[4]), lens[4]), :]
            if self.kind == "rs":
                out = pltpu.make_async_copy(final, shard.at[pl.ds(self.shard_row, lens[4]), :], sem_l.at[1])

                def tail():
                    out.start()

                def end():
                    out.wait()
                    for s in sends:
                        s.wait_send()

                events.append(end)
                return events
        elif self.kind == "fan":
            final = self.after.prod.at[pl.ds(self.row, lens[4]), :]
        else:
            final = buf
            load = pltpu.make_async_copy(shard.at[pl.ds(self.shard_row, lens[4]), :], buf, sem_l.at[0])

            def begin():
                load.start()

            events.append(begin)

        place = pltpu.make_async_copy(final, dst.at[core, pl.ds(al(ch.row0 + offs[4]), lens[4]), :], sem_l.at[1])
        outs = [remote(final, dst.at[core, pl.ds(al(ch.row0 + offs[4]), lens[4]), :], sem0, ch.order[3])]
        for i, k in enumerate((3, 2, 1)):
            part = dst.at[core, pl.ds(al(ch.row0 + offs[k]), lens[k]), :]
            outs.append(remote(part, part, sem0 + 1 + i, ch.order[k - 1]))
        part = dst.at[core, pl.ds(ch.row0, rows), :]
        outs.append(remote(part, part, sem0 + 4, 0))

        def tail():
            place.start()
            outs[0].start()

        if self.kind == "ag":
            def second():
                load.wait()
                tail()
            events.append(second)
        if self.kind == "fan":
            events.append(tail)

        def spread(i):
            def run():
                if i == 1:
                    place.wait()
                outs[i - 1].wait_recv()
                outs[i].start()
            return run

        events += [spread(i) for i in range(1, 5)]

        def end():
            outs[4].wait_recv()
            for s in (sends if self.kind == "ar" else []) + outs:
                s.wait_send()

        events.append(end)
        return events


RATE = {0: 600e3, 1: 44e3, 2: 44e3, 3: 44e3, 4: 22e3}
LINK = {0: 0, 1: 1, 2: 2, 3: 3, 4: 3}


def plan(jobs, ticks, tick_us, lag=2.5):
    free = {}
    state = [[0, 1e9 if getattr(job, "after", None) else job.start] for job in jobs]
    slots = [[] for _ in range(ticks)]
    rest = []

    def fire(j, now):
        e, _ = state[j]
        msgs = jobs[j].messages()
        ready = now
        if e < len(msgs) and msgs[e][1] is not None:
            size, d = msgs[e]
            begin = max(now, free.get(LINK[d], 0.0))
            ready = begin + size / RATE[d]
            free[LINK[d]] = ready
            ready += lag
        elif e + 1 < jobs[j].n_events:
            ready = now + lag
        state[j] = [e + 1, ready]
        if e + 1 == jobs[j].n_events:
            for i, job in enumerate(jobs):
                if getattr(job, "after", None) is jobs[j]:
                    state[i][1] = now

    for t in range(ticks):
        now = t * tick_us
        order = sorted((s[1], j) for j, s in enumerate(state) if s[0] < jobs[j].n_events and s[1] <= now)
        for _, j in order:
            slots[t].append((j, state[j][0]))
            fire(j, now)
    now = ticks * tick_us
    while True:
        todo = sorted((s[1], j) for j, s in enumerate(state) if s[0] < jobs[j].n_events)
        if not todo:
            return slots, rest, now
        ready, j = todo[0]
        now = max(now, ready)
        rest.append((j, state[j][0]))
        fire(j, now)


def stage1(tok, grad, w_up, w_down, pre_out, next_out, tri, small_u, small_q, hid_s, up_s, down_s):
    zero_first((tri, small_u, small_q))

    @pl.when(pl.program_id(0) == 0)
    def _():
        up_s[...] = w_up[0].T
        down_s[...] = w_down[0].T

    pre = mm(up_s[...], tok[...], NT).astype(bf16)
    pre_out[...] = pre
    pre = pre.astype(f32)
    hid_s[...] = (pre * half_sig(pre)[0]).astype(bf16)
    add_tri(tri, hid_s)
    next_out[...] = mm(down_s[...], hid_s[...], NN).astype(bf16)
    add_small_tn(small_u, tok)
    add_small_tn(small_q, grad)


def stage2(u_t, grad, w_up, pre_out, tri, small_u, dwd, hid_s, up_s):
    zero_first((tri, small_u, dwd))

    @pl.when(pl.program_id(0) == 0)
    def _():
        up_s[...] = w_up[0].T

    pre = mm(up_s[...], u_t[...], NN).astype(bf16)
    pre_out[...] = pre
    pre = pre.astype(f32)
    hid_s[...] = (pre * half_sig(pre)[0]).astype(bf16)
    add_small_nt(small_u, u_t)
    add_tri(tri, hid_s)
    dwd[0] += mm(grad[...], hid_s[:FF // 2, :], TT)
    dwd[1] += mm(grad[...], hid_s[FF // 2:, :], TT)


def stage3(pre_in, grad, u_t, w_down, w_up, err_out, tri, dwu, g_s):
    zero_first((tri, dwu))
    d_hid = mm(w_down[0], grad[...], NT).astype(bf16).astype(f32)
    pre = pre_in[...].astype(f32)
    sig, cubic = half_sig(pre)
    g_s[...] = (d_hid * gelu_back(pre, sig, cubic)[1]).astype(bf16)
    add_tri(tri, g_s)
    dwu[0] += mm(u_t[...], g_s[:FF // 2, :], NT)
    dwu[1] += mm(u_t[...], g_s[FF // 2:, :], NT)
    err_out[...] = mm(w_up[0], g_s[...], NN).astype(bf16)


def stage4(pre_in, tok, err_t, w_down, g_out, small_q, dwd, dwu, hid_s):
    zero_first((small_q, dwd, dwu))
    d_hid = mm(w_down[0], err_t[...], NN).astype(bf16).astype(f32)
    pre = pre_in[...].astype(f32)
    sig, cubic = half_sig(pre)
    hid, slope = gelu_back(pre, sig, cubic)
    hid_s[...] = hid.astype(bf16)
    g_out[...] = (d_hid * slope).astype(bf16)
    add_small_nt(small_q, err_t)
    dwd[0] += mm(err_t[...], hid_s[:FF // 2, :], NT)
    dwd[1] += mm(err_t[...], hid_s[FF // 2:, :], NT)
    dwu[0] += mm(tok[...], g_out[:FF // 2, :], TT)
    dwu[1] += mm(tok[...], g_out[FF // 2:, :], TT)


def stage5(g_in, tri):
    zero_first((tri,))
    add_tri(tri, g_in)


SMALL = (2, 128, 384)
WIDE = (2, 384, 768)
TRI_SHAPE = (2, TRI // 2, B)
TRI_CHAINS = [Chain(0, 640, B, ORDER_X), Chain(640, 640, B, ORDER_Y), Chain(1280, 512, B, ORDER_X),
              Chain(1792, 512, B, ORDER_Y), Chain(2304, 384, B, ORDER_Z)]
WIDE_CHAINS = [Chain(0, 128, 768, ORDER_X), Chain(128, 128, 768, ORDER_Y), Chain(256, 128, 768, ORDER_Z)]
SMALL_CHAINS = [Chain(0, 128, 384, ORDER_Y)]
FORMS = {"tri": (TRI_SHAPE, TRI_CHAINS), "wide": (WIDE, WIDE_CHAINS), "small": (SMALL, SMALL_CHAINS)}


def form_jobs(kind, form, name):
    shape, chains = FORMS[form]
    jobs, row = [], 0
    for chain in chains:
        jobs.append(Job(kind, chain, src=name + ":src", shard=name + ":shard", shard_row=row, dst=name + ":dst"))
        row += chain.rows // 16
    return jobs


class First:
    n_events = 2
    kind = "first"
    start = 0.0

    def __init__(self, name):
        self.name = name

    def scratch(self):
        return [pltpu.VMEM((24, 768), f32), pltpu.VMEM((24, 768), f32), pltpu.VMEM((24, 768), f32),
                pltpu.VMEM((FF, 768), f32), pltpu.SemaphoreType.DMA((2,)), pltpu.SemaphoreType.DMA((1,)),
                pltpu.SemaphoreType.DMA((1,))]

    def messages(self):
        return [(24 * 768 * 4 + 4000000, 0), (0, None)]

    def bind(self, refs, scr):
        own, other, prod, inv_v, sem_l, sem_s, sem_r = scr
        me, bits = my_bits()
        core = bits[0]
        shard, inv, block = refs[self.name + ":shard"], refs[self.name + ":inv"], refs[self.name + ":block"]
        load = pltpu.make_async_copy(shard, own, sem_l.at[0])
        inv_load = pltpu.make_async_copy(inv.at[block, :, pl.ds(pl.multiple_of(core * 768, 128), 768)], inv_v, sem_l.at[1])
        swap = pltpu.make_async_remote_copy(src_ref=shard, dst_ref=other, send_sem=sem_s.at[0], recv_sem=sem_r.at[0],
                                            device_id=(me + 1 - 2 * core,), device_id_type=MESH)

        def begin():
            load.start()
            swap.start()
            inv_load.start()

        def product():
            load.wait()
            inv_load.wait()
            swap.wait_recv()
            swap.wait_send()
            here = inv_v[pl.ds(pl.multiple_of(core * 768, 8), 768), :]
            there = inv_v[pl.ds(pl.multiple_of((1 - core) * 768, 8), 768), :]
            prod[...] = precise(own[...], here) + precise(other[...], there)

        return [begin, product]


class Fan(Job):
    def __init__(self, chain, row, dst, after):
        Job.__init__(self, "fan", chain, dst=dst)
        self.row, self.after = row, after


def precise(left, right):
    return lax.dot_general(left, right, NN, precision=lax.Precision.HIGHEST, preferred_element_type=f32)


def first_jobs(name):
    first = First(name)
    row, jobs = 0, [first]
    for chain in WIDE_CHAINS:
        jobs.append(Fan(chain, row, name + ":dst", first))
        row += 8
    return jobs


def rows_spec(tile):
    return pl.BlockSpec((tile, D), lambda i: (i, 0))


def cols_spec(height, tile):
    return pl.BlockSpec((height, tile), lambda i: (0, i))


def whole_spec(shape):
    zeros = (0,) * len(shape)
    return pl.BlockSpec(shape, lambda i: zeros, pipeline_mode=pl.Buffered(1))


def block_spec(shape, b):
    return pl.BlockSpec((1,) + shape[1:], lambda i: (b, 0, 0), pipeline_mode=pl.Buffered(1))


ANY = pl.BlockSpec(memory_space=pl.ANY)


def run_stage(body, name, tile, steps, ins, outs, scratch, jobs, extra, comm_ins, comm_outs, tick_us, flops, cid):
    def spec(kind, shape):
        if kind == "r":
            return rows_spec(tile)
        if kind == "c":
            return cols_spec(shape[0], tile)
        if kind == "w":
            return whole_spec(shape)
        return block_spec(shape, kind)

    slots, rest, end = plan(jobs, steps, tick_us)
    if DEBUG:
        print(name, "planned end", end, "compute", steps * tick_us, "rest", len(rest))
    scr = [job.scratch() for job in jobs]
    n_in, n_cin, n_out, n_cout, n_scr = len(ins), len(comm_ins), len(outs), len(comm_outs), len(scratch)

    def kernel(*refs):
        refs = list(refs)
        take = lambda n: [refs.pop(0) for _ in range(n)]
        c_in, m_in, c_out, m_out, c_scr = take(n_in), take(n_cin), take(n_out), take(n_cout), take(n_scr)
        named = dict(extra)
        named.update(zip(comm_ins, m_in))
        named.update(zip(comm_outs, m_out))
        step = pl.program_id(0)
        events = []
        if jobs:
            pl.when(step == 0)(entry_barrier)
            for job, s in zip(jobs, scr):
                mine = take(len(s))
                if job.kind == "first":
                    job.prod = mine[2]
                events.append(job.bind(named, mine))
        for t in range(steps):
            if slots[t]:
                @pl.when(step == t)
                def _(t=t):
                    for j, e in slots[t]:
                        events[j][e]()
        if body is not None:
            body(*c_in, *c_out, *c_scr)
        if rest:
            @pl.when(step == steps - 1)
            def _():
                for j, e in rest:
                    events[j][e]()

    params = dict(vmem_limit_bytes=63 * MIB)
    if jobs:
        params.update(collective_id=cid, has_side_effects=True)
    outputs = pl.pallas_call(
        kernel, grid=(steps,),
        in_specs=[spec(kind, arr.shape) for arr, kind in ins] + [ANY] * n_cin,
        out_specs=[spec(kind, shape) for shape, dtype, kind in outs] + [ANY] * n_cout,
        out_shape=[jax.ShapeDtypeStruct(shape, dtype) for shape, dtype, kind in outs]
        + [jax.ShapeDtypeStruct(shape, f32) for shape in comm_outs.values()],
        scratch_shapes=list(scratch) + [x for s in scr for x in s],
        compiler_params=pltpu.CompilerParams(**params),
        cost_estimate=pl.CostEstimate(flops=flops, bytes_accessed=40 * MIB, transcendentals=0),
        name=name)(*[arr for arr, _ in ins], *comm_ins.values())
    return outputs[:n_out], dict(zip(comm_outs, outputs[n_out:]))


DEBUG = False


def final_kernel(decay, t0, t1, t2, t3, old_s, old_a, s0, s1, s2, s3, old_u, old_q, n0, n1, n2, n3, inv_u, inv_q,
                 new_s, new_a, new_u, new_q, p_up, p_down, pk, od, nw, tr, sem_in, sem_out):
    rho = decay[0]
    scale = (1.0 - rho) * decay[1]
    units = []
    for src, old, new, b in ((t0, old_a, new_a, 0), (t1, old_a, new_a, 1), (t2, old_s, new_s, 0), (t3, old_s, new_s, 1)):
        off = 0
        for j in range(NB):
            units.append((src, old, new, b, j, off))
            off += (j + 1) * B

    def loads(u):
        src, old, new, b, j, off = units[u]
        rows, s = (j + 1) * B, u % 3
        return (pltpu.make_async_copy(src.at[pl.ds(off, rows), :], pk.at[s, pl.ds(0, rows), :], sem_in.at[s, 0]),
                pltpu.make_async_copy(old.at[b, pl.ds(0, rows), pl.ds(j * B, B)], od.at[s, pl.ds(0, rows), :], sem_in.at[s, 1]))

    def stores(u):
        src, old, new, b, j, off = units[u]
        rows, s = (j + 1) * B, u % 3
        ops = [pltpu.make_async_copy(nw.at[s, pl.ds(0, rows), :], new.at[b, pl.ds(0, rows), pl.ds(j * B, B)], sem_out.at[s, 0])]
        if j:
            ops.append(pltpu.make_async_copy(tr.at[s, :, pl.ds(0, j * B)], new.at[b, pl.ds(j * B, B), pl.ds(0, j * B)], sem_out.at[s, 1]))
        return ops

    def small(acc, old, new, b):
        top = rho * old[b, 0:128, :] + scale * acc[0]
        mid = rho * old[b, 128:256, 128:384] + scale * acc[1, :, 0:256]
        low = rho * old[b, 256:384, 256:384] + scale * acc[1, :, 256:384]
        new[b, 0:128, :] = top
        new[b, 128:256, 128:384] = mid
        new[b, 256:384, 256:384] = low
        new[b, 128:384, 0:128] = top[:, 128:384].T
        new[b, 256:384, 128:256] = mid[:, 128:256].T

    def up(n, b, h):
        p_up[b, :, h * 768:(h + 1) * 768] = precise(inv_u[b], n[h]) * decay[1]

    def down(n, b, h):
        p_down[b, h * 768:(h + 1) * 768, :] = precise(n[h].T, inv_q[b]) * decay[1]

    side = [functools.partial(small, *a) for a in
            ((s0, old_u, new_u, 0), (s1, old_u, new_u, 1), (s2, old_q, new_q, 0), (s3, old_q, new_q, 1))]
    for n, b, f in ((n0, 0, up), (n1, 1, up), (n2, 0, down), (n3, 1, down)):
        for h in range(2):
            side.append(functools.partial(f, n, b, h))
    for u in (0, 1):
        for c in loads(u):
            c.start()
    for u, (src, old, new, b, j, off) in enumerate(units):
        s = u % 3
        if u % 2 == 0:
            side[u // 2]()
        if u >= 3:
            for c in stores(u - 3):
                c.wait()
        for c in loads(u):
            c.wait()
        for i in range(j + 1):
            part = rho * od[s, i * B:(i + 1) * B, :] + scale * pk[s, i * B:(i + 1) * B, :]
            nw[s, i * B:(i + 1) * B, :] = part
            if i < j:
                tr[s, :, i * B:(i + 1) * B] = part.T
        for c in stores(u):
            c.start()
        if u + 2 < len(units):
            for c in loads(u + 2):
                c.start()
    for u in range(len(units) - 3, len(units)):
        for c in stores(u):
            c.wait()


def finish(decay, tris, smalls, prods, s_up_old, a_down_old, a_up_old, s_down_old, inv_u, inv_q):
    vmem = pl.BlockSpec(memory_space=pltpu.VMEM)
    big = jax.ShapeDtypeStruct(s_up_old.shape, f32)
    small = jax.ShapeDtypeStruct(a_up_old.shape, f32)
    return pl.pallas_call(
        final_kernel,
        in_specs=[pl.BlockSpec(memory_space=pltpu.SMEM)] + [ANY] * 6 + [vmem] * 12,
        out_specs=[ANY] * 2 + [vmem] * 4,
        out_shape=[big, big, small, small, jax.ShapeDtypeStruct((2, D, FF), f32), jax.ShapeDtypeStruct((2, FF, D), f32)],
        scratch_shapes=[pltpu.VMEM((3, FF, B), f32), pltpu.VMEM((3, FF, B), f32), pltpu.VMEM((3, FF, B), f32),
                        pltpu.VMEM((3, B, FF), f32), pltpu.SemaphoreType.DMA((3, 2)), pltpu.SemaphoreType.DMA((3, 2))],
        compiler_params=pltpu.CompilerParams(vmem_limit_bytes=63 * MIB),
        name="finish")(decay, *[t.reshape(TRI, B) for t in tris], s_up_old, a_down_old, *smalls, a_up_old, s_down_old,
                       *prods, inv_u, inv_q)


def solution(mesh):
    axis_size = mesh.shape["data"]
    tile = 512

    def local_step(tok, grad, w_up, w_down, a_up_old, s_up_old, a_down_old, s_down_old,
                   a_up_inv, s_up_inv, a_down_inv, s_down_inv, factor_decay):
        total = tok.shape[0]
        steps = total // tile
        inv_n = 1.0 / (total * axis_size)
        acts = pltpu.VMEM((FF, tile), bf16)
        w_t = pltpu.VMEM((FF, D), bf16)
        unit = 2 * total * FF * D
        shard = {"tri": (TRI // 32, B), "wide": (24, 768), "small": (8, 384)}

        def comm(rs=(), ag=(), ar=(), first=()):
            jobs, c_ins, c_outs, extra = [], {}, {}, {}
            for name, form, arr in ar:
                jobs += form_jobs("ar", form, name)
                c_ins[name + ":src"] = arr.reshape(FORMS[form][0])
                c_outs[name + ":dst"] = FORMS[form][0]
            for name, arr, inverse, block in first:
                jobs += first_jobs(name)
                c_ins[name + ":shard"] = arr
                c_ins[name + ":inv"] = inverse
                c_outs[name + ":dst"] = WIDE
                extra[name + ":block"] = block
            for name, form, arr in ag:
                jobs += form_jobs("ag", form, name)
                c_ins[name + ":shard"] = arr
                c_outs[name + ":dst"] = FORMS[form][0]
            for name, form, arr in rs:
                jobs += form_jobs("rs", form, name)
                c_ins[name + ":src"] = arr.reshape(FORMS[form][0])
                c_outs[name + ":shard"] = shard[form]
            return jobs, extra, c_ins, c_outs

        (pre0, u1, ad0, au0, sd1), _ = run_stage(
            stage1, "stage1", tile, steps, ((tok, "r"), (grad, "r"), (w_up, 0), (w_down, 0)),
            (((FF, total), bf16, "c"), ((D, total), bf16, "c"), ((TRI, B), f32, "w"), (SMALL, f32, "w"), (SMALL, f32, "w")),
            [acts, w_t, pltpu.VMEM((D, FF), bf16)], *comm(), 4.0, 5 * unit, 0)
        (pre1, ad1, au1, dwd1), c2 = run_stage(
            stage2, "stage2", tile, steps, ((u1, "c"), (grad, "r"), (w_up, 1)),
            (((FF, total), bf16, "c"), ((TRI, B), f32, "w"), (SMALL, f32, "w"), (WIDE, f32, "w")),
            [acts, w_t], *comm(rs=(("ad0", "tri", ad0), ("au0", "small", au0), ("sd1", "small", sd1))),
            3.8, 5 * unit, 1)
        (e1, su1, dwu1), c3 = run_stage(
            stage3, "stage3", tile, steps, ((pre1, "c"), (grad, "r"), (u1, "c"), (w_down, 1), (w_up, 1)),
            (((D, total), bf16, "c"), ((TRI, B), f32, "w"), (WIDE, f32, "w")),
            [acts], *comm(rs=(("ad1", "tri", ad1), ("au1", "small", au1), ("dwd1", "wide", dwd1)),
                          ag=(("ad0", "tri", c2["ad0:shard"]), ("au0", "small", c2["au0:shard"]), ("sd1", "small", c2["sd1:shard"]))),
            5.0, 6 * unit, 2)
        (g0, sd0, dwd0, dwu0), c4 = run_stage(
            stage4, "stage4", tile, steps, ((pre0, "c"), (tok, "r"), (e1, "c"), (w_down, 0)),
            (((FF, total), bf16, "c"), (SMALL, f32, "w"), (WIDE, f32, "w"), (WIDE, f32, "w")),
            [acts], *comm(rs=(("su1", "tri", su1), ("dwu1", "wide", dwu1)),
                          ag=(("ad1", "tri", c3["ad1:shard"]), ("au1", "small", c3["au1:shard"])),
                          first=(("dwd1", c3["dwd1:shard"], a_down_inv, 1),)),
            3.5, 4 * unit, 3)
        (su0,), c5 = run_stage(
            stage5, "stage5", tile, steps, ((g0, "c"),), (((TRI, B), f32, "w"),),
            [], *comm(rs=(("sd0", "small", sd0), ("dwd0", "wide", dwd0), ("dwu0", "wide", dwu0)),
                      ag=(("su1", "tri", c4["su1:shard"]),),
                      first=(("dwu1", c4["dwu1:shard"], s_up_inv, 1),)),
            1.8, 3 * unit, 4)
        _, c6 = run_stage(
            None, "tail", tile, 1, (), (), [],
            *comm(ar=(("su0", "tri", su0),), ag=(("sd0", "small", c5["sd0:shard"]),),
                  first=(("dwd0", c5["dwd0:shard"], a_down_inv, 0), ("dwu0", c5["dwu0:shard"], s_up_inv, 0))),
            0.1, unit, 5)
        decay = jnp.stack((factor_decay, jnp.float32(inv_n)))
        new_s, new_a, new_u, new_q, p_up, p_down = finish(
            decay, (c3["ad0:dst"], c4["ad1:dst"], c6["su0:dst"], c5["su1:dst"]),
            (c3["au0:dst"], c4["au1:dst"], c6["sd0:dst"], c3["sd1:dst"]),
            (c6["dwu0:dst"], c5["dwu1:dst"], c6["dwd0:dst"], c4["dwd1:dst"]),
            s_up_old, a_down_old, a_up_old, s_down_old, a_up_inv, s_down_inv)
        return p_up, p_down, new_u, new_s, new_a, new_q

    batch_spec = P("data", None)
    replicated = P()
    return jax.shard_map(local_step, mesh=mesh, in_specs=(batch_spec, batch_spec) + (replicated,) * 11,
                         out_specs=(replicated,) * 6, check_vma=False)
```

```python
import functools

import jax
import jax.numpy as jnp
from jax import lax
from jax.experimental import pallas as pl
from jax.experimental.pallas import tpu as pltpu
from jax.sharding import PartitionSpec as P

bf16 = jnp.bfloat16
f32 = jnp.float32
D, FF, B = 384, 1536, 256
NB = FF // B
TRI = sum((j + 1) * B for j in range(NB))
NN = (((1,), (0,)), ((), ()))
NT = (((1,), (1,)), ((), ()))
TN = (((0,), (0,)), ((), ()))
TT = (((0,), (1,)), ((), ()))
GELU_K = 0.7978845608028654
GELU_C = 0.044715 * GELU_K
MIB = 1 << 20


def mm(left, right, dims):
    return lax.dot_general(left, right, dims, preferred_element_type=f32)


def half_sig(pre):
    cubic = GELU_C * (pre * pre)
    return 0.5 * jnp.tanh(pre * (cubic + GELU_K)) + 0.5, cubic


def gelu_back(pre, sig, cubic):
    hid = pre * sig
    return hid, sig + (hid * (1.0 - sig)) * (6.0 * cubic + 2.0 * GELU_K)


def add_tri(acc, mat):
    off = 0
    for j in range(NB):
        rows = (j + 1) * B
        acc[off:off + rows, :] += mm(mat[:rows, :], mat[j * B:rows, :], NT)
        off += rows


def add_small_tn(acc, rows):
    acc[0] += mm(rows[:, 0:128], rows[...], TN)
    acc[1, :, 0:256] += mm(rows[:, 128:256], rows[:, 128:384], TN)
    acc[1, :, 256:384] += mm(rows[:, 256:384], rows[:, 256:384], TN)


def add_small_nt(acc, cols):
    acc[0] += mm(cols[0:128, :], cols[...], NT)
    acc[1, :, 0:256] += mm(cols[128:256, :], cols[128:384, :], NT)
    acc[1, :, 256:384] += mm(cols[256:384, :], cols[256:384, :], NT)


def zero_first(accs):
    @pl.when(pl.program_id(0) == 0)
    def _():
        for acc in accs:
            acc[...] = jnp.zeros_like(acc)


MESH = pl.DeviceIdType.MESH
ORDER_X, ORDER_Y, ORDER_Z = (1, 2, 3, 4), (2, 1, 3, 4), (3, 4, 1, 2)
LINKS = {0: {0: 6e5}, 1: {1: 45e3}, 2: {2: 45e3}, 3: {3: 45e3}, 4: {3: 45e3, 4: 23e3}}
LAG = 2.5
SLACK = 3.0


def PRIORITY(f):
    return f.b


LAST = 10


def my_bits():
    me = lax.axis_index("data")
    bits = [(me // (1 << d)) % 2 for d in range(5)]
    return bits, [me + (1 - 2 * bits[d]) * (1 << d) for d in range(5)]


def entry_barrier():
    peers = my_bits()[1]
    barrier = pltpu.get_barrier_semaphore()
    for peer in peers:
        pl.semaphore_signal(barrier, inc=1, device_id=(peer,), device_id_type=MESH)
    pl.semaphore_wait(barrier, len(peers))


def al(row):
    return pl.multiple_of(row, 8)


class Flow:
    def __init__(self, name, row0, rows, cols, order, shard_row, wide):
        self.name, self.row0, self.rows, self.cols, self.order = name, row0, rows, cols, order
        self.shard_row, self.wide = shard_row, wide
        self.at, self.start = 0, 0.0
        self.part = name + ":part%d" % row0

    def fan(self):
        other = Flow(self.name, self.row0, self.rows, self.cols, self.order, self.shard_row, True)
        other.at = 5
        return other

    def dim(self, s):
        if s in (0, LAST - 1):
            return 0
        return self.order[s - 1] if s < 5 else self.order[LAST - 2 - s]

    def length(self, s):
        return self.rows >> s if s < 5 else self.rows >> (LAST - 1 - s)

    def kept(self, steps):
        return self.rows >> (steps - 1)

    def open(self, a, b):
        self.a, self.b = a, b
        n = b - a
        out = [pltpu.SemaphoreType.DMA((2,)), pltpu.SemaphoreType.DMA((n,)), pltpu.SemaphoreType.DMA((n,))]
        if a < 5:
            out.append(pltpu.VMEM((self.rows if a == 0 else self.kept(a), self.cols), f32))
            out.append(pltpu.VMEM((sum(self.length(s) for s in range(a, min(b, 5))), self.cols), f32))
        elif a == 5 and not self.wide:
            out.append(pltpu.VMEM((self.kept(5), self.cols), f32))
        return out

    def bind(self, named, scr):
        a, b, row0, rows = self.a, self.b, self.row0, self.rows
        sem_l, sem_s, sem_r = scr[:3]
        bits, peers = my_bits()
        core = bits[0]
        lens, offs = [rows], [0]
        for d in self.order:
            lens.append(lens[-1] // 2)
            offs.append(offs[-1] + bits[d] * lens[-1])
        src, dst = named.get(self.name + ":src"), named.get(self.name + ":dst")
        part_in, part_out = named.get(self.part + ":in"), named.get(self.part + ":out")
        base = offs[min(max(a, 1), 5) - 1]
        work = recv = None
        if a < 5:
            work, recv = scr[3:]
        elif a == 5:
            work = named[self.name + ":first"].at[pl.ds(self.shard_row, 8), :] if self.wide else scr[3]
        sends, begin_recv, locals_ = {}, {}, []

        def remote(s, x, y):
            return pltpu.make_async_remote_copy(src_ref=x, dst_ref=y, send_sem=sem_s.at[s - a], recv_sem=sem_r.at[s - a],
                                                device_id=(peers[self.dim(s)],), device_id_type=MESH)

        def final():
            return work if a == 5 else work.at[pl.ds(al(offs[4] - base), lens[4]), :]

        def spot(k):
            return dst.at[core, pl.ds(al(row0 + offs[k]), lens[k]), :]

        at = 0
        for s in range(a, b):
            if s < 5:
                begin_recv[s] = at
                to = recv.at[pl.ds(at, self.length(s)), :]
                at += self.length(s)
                if s == 0:
                    sends[s] = remote(s, src.at[1 - core, pl.ds(row0, rows), :], to)
                else:
                    gone = al(offs[s - 1] - base + (1 - bits[self.dim(s)]) * lens[s])
                    sends[s] = remote(s, work.at[pl.ds(gone, lens[s]), :], to)
            else:
                k = LAST - 1 - s
                sends[s] = remote(s, final() if s == 5 else spot(k), spot(k))
        load = place = save = None
        if a == 0:
            load = pltpu.make_async_copy(src.at[core, pl.ds(row0, rows), :], work, sem_l.at[0])
        elif a < 5 or (a == 5 and not self.wide):
            load = pltpu.make_async_copy(part_in, work, sem_l.at[0])
        if a <= 5 < b:
            place = pltpu.make_async_copy(final(), spot(4), sem_l.at[1])
        if b <= 5:
            kept = work.at[pl.ds(al(offs[b - 1] - base), lens[b - 1]), :]
            save = pltpu.make_async_copy(kept, part_out, sem_l.at[1])

        def add(row, frm, count):
            for q in range(0, count, 64):
                step = min(count - q, 64)
                x, y = al(row + q), al(frm + q)
                work[pl.ds(x, step), :] = work[pl.ds(x, step), :] + recv[pl.ds(y, step), :]

        def take(s, then):
            if s == a and load is not None and a == 0:
                load.wait()
            sends[s].wait_recv()
            if s == 5 and place is not None:
                place.wait()
            if s >= 5:
                then()
            elif s == 4 or s + 1 == b:
                add(offs[s] - base, begin_recv[s], lens[s])
                then()
            else:
                half = lens[s + 1]
                bit = bits[self.dim(s + 1)]
                add(offs[s] - base + (1 - bit) * half, begin_recv[s] + (1 - bit) * half, half)
                then()
                add(offs[s] - base + bit * half, begin_recv[s] + bit * half, half)

        def send(s):
            if s == 5:
                place.start()
            sends[s].start()

        def begin():
            load.start()
            if a == 0:
                send(0)

        def go(s):
            if s > a:
                take(s - 1, lambda: send(s))
            else:
                if load is not None:
                    load.wait()
                send(s)

        def stop():
            take(b - 1, save.start if save is not None else lambda: None)

        def end():
            if save is not None:
                save.wait()
            for s in range(a, b):
                sends[s].wait_send()

        return {"begin": begin, "go": go, "stop": lambda s: stop(), "end": end}


class First:
    def __init__(self, name, flows, inverse, block):
        self.name, self.flows, self.inverse, self.block, self.done = name, flows, inverse, block, False
        self.fans = [f.fan() for f in flows]

    def open(self):
        rows = pltpu.VMEM((24, 768), f32)
        return [pltpu.SemaphoreType.DMA((4,)), pltpu.SemaphoreType.DMA((3,)), pltpu.SemaphoreType.DMA((3,)),
                rows, rows, rows, pltpu.VMEM((FF, 768), f32)]

    def bind(self, named, scr):
        sem_l, sem_s, sem_r, own, other, prod, inv_v = scr
        named[self.name + ":first"] = prod
        bits, peers = my_bits()
        core = bits[0]
        inv = named[self.name + ":inv"]
        copies, swaps = [], []
        for i, flow in enumerate(self.flows):
            rows = named.get(flow.part + ":out", named.get(flow.part + ":in"))
            spot = pl.ds(flow.shard_row, 8)
            copies.append(pltpu.make_async_copy(rows, own.at[spot, :], sem_l.at[i]))
            swaps.append(pltpu.make_async_remote_copy(
                src_ref=rows, dst_ref=other.at[spot, :], send_sem=sem_s.at[i], recv_sem=sem_r.at[i],
                device_id=(peers[0],), device_id_type=MESH))
        copies.append(pltpu.make_async_copy(
            inv.at[self.block, :, pl.ds(pl.multiple_of(core * 768, 128), 768)], inv_v, sem_l.at[3]))

        def begin():
            for copy in copies + swaps:
                copy.start()

        def go(s):
            for copy in copies + swaps:
                copy.wait()
            prod[...] = (precise(own[...], inv_v[pl.ds(al(core * 768), 768), :])
                         + precise(other[...], inv_v[pl.ds(al((1 - core) * 768), 768), :]))

        return {"begin": begin, "go": go}


def plan(flows, firsts, tick_us, last, over=4.0):
    times = [0.0]
    for us in tick_us:
        times.append(times[-1] + us)
    limit = 1e9 if last else times[-1]
    free, now_rest = {}, times[-1]
    slots, rest = [[] for _ in tick_us], []
    ready = {f: f.start for f in flows}
    phase = {f: "new" for f in flows}
    for f in flows:
        f.a = f.b = f.at
    fstate = {f: "new" for f in firsts}
    fready = {}

    def arrival(f, s, now):
        links = LINKS[f.dim(s)]
        size = f.length(s) * f.cols * 4
        begin = max([now] + [free.get(link, 0.0) for link in links])
        return begin, max(begin + size / rate for rate in links.values()), size

    def send(f, s, now):
        begin, end, size = arrival(f, s, now)
        for link, rate in LINKS[f.dim(s)].items():
            free[link] = begin + size / rate
        f.b = s + 1
        ready[f] = end + LAG

    def allowed(f, s, now):
        return last or (now < limit and arrival(f, s, now)[1] + LAG < limit + over)

    def clear(f, s, now):
        return arrival(f, s, now)[0] <= now + SLACK

    def move(f, now):
        if ready[f] > now:
            return None
        if phase[f] == "new":
            if f.at >= LAST or f.wide and f.at == 5:
                return None
            if not allowed(f, f.at, now + (LAG if 0 < f.at <= 5 else 0.0)):
                return None
            if not clear(f, f.at, now):
                return None
            if f.at == 0:
                phase[f] = "run"
                send(f, 0, now)
                return "begin", 0
            if f.at <= 5:
                phase[f] = "loaded"
                ready[f] = now + LAG
                f.b = f.at + 1
                return "begin", 0
            phase[f] = "run"
            send(f, f.at, now)
            return "go", f.at
        if phase[f] == "loaded":
            phase[f] = "run"
            send(f, f.at, now)
            return "go", f.at
        if phase[f] == "run":
            s = f.b
            if s == LAST or f.wide and s == 5 or not allowed(f, s, now):
                phase[f] = "saved"
                ready[f] = now + LAG
                return "stop", s
            if not clear(f, s, now):
                return None
            send(f, s, now)
            return "go", s
        if phase[f] == "saved":
            phase[f] = "done"
            return "end", 0
        return None

    def first_move(f, now):
        if f.done or fready.get(f, 0.0) > now:
            return None
        if fstate[f] == "new":
            ok = all(x.b == 5 and phase.get(x, "done") in ("new", "done") for x in f.flows)
            if not ok or not (last or now + 20.0 < limit):
                return None
            fstate[f] = "loaded"
            fready[f] = now + 5.0
            return "begin", 0
        if fstate[f] == "loaded":
            fstate[f] = "done"
            return "go", 0
        return None

    def sweep(now, out):
        again = True
        while again:
            again = False
            for f in sorted(flows, key=PRIORITY):
                e = move(f, now)
                if e:
                    out.append((f,) + e)
                    again = True
                    break
            for f in firsts:
                e = first_move(f, now)
                if e:
                    out.append((f,) + e)
                    again = True
                    if fstate[f] == "done":
                        for x in f.fans:
                            flows.append(x)
                            x.a = 5
                            phase[x] = "run"
                            send(x, 5, now)
                            out.append((x, "go", 5))

    for t, now in enumerate(times[:-1]):
        sweep(now, slots[t])
    now = times[-1]
    while True:
        sweep(now, rest)
        later = [ready[f] for f in flows if phase[f] in ("loaded", "run", "saved") and ready[f] > now]
        later += [fready[f] for f in firsts if fstate[f] == "loaded" and fready[f] > now]
        held = any(phase[f] in ("loaded", "run") or last and phase[f] == "new" and f.at < LAST and not (f.wide and f.at == 5)
                   for f in flows)
        if not later and not held:
            return slots, rest, now
        now = min(later + ([now + 1.0] if held else []))


def tri_col(acc, mat, j):
    rows = (j + 1) * B
    off = B * j * (j + 1) // 2
    acc[off:off + rows, :] += mm(mat[:rows, :], mat[j * B:rows, :], NT)


def staged(dot, act, backs, shifts, accs, setup=None):
    step, last = pl.program_id(0), pl.num_programs(0) - 1

    def shift():
        for old, new in shifts:
            old[...] = new[...]

    @pl.when(step == 0)
    def _():
        for acc in accs:
            acc[...] = jnp.zeros_like(acc)
        if setup is not None:
            setup()
        for k in range(NB):
            act(k, dot(k))

    @pl.when((step > 0) & (step < last))
    def _():
        shift()
        for k, back in enumerate(backs):
            value = dot(k)
            back()
            act(k, value)

    @pl.when(step == last)
    def _():
        shift()
        for back in backs:
            back()


def block(k):
    return slice(k * B, (k + 1) * B)


def tri_pieces(acc, mat, *more):
    pieces = [(5,), (4,), (3, 0), (2, 1)]

    def run(cols, fns):
        for j in cols:
            tri_col(acc, mat, j)
        for fn in fns:
            fn()

    return [functools.partial(run, cols, ()) for cols in pieces] + [functools.partial(run, (), fns) for fns in more]


def gelu_act(pre_out, new_s):
    def act(k, value):
        pre = value.astype(bf16)
        pre_out[block(k), :] = pre
        pre = pre.astype(f32)
        new_s[block(k), :] = (pre * half_sig(pre)[0]).astype(bf16)
    return act


def stage1(tok, grad, w_up, w_down, tok_b, grad_b, pre_out, next_out, tri, small_u, small_q, new_s, hid_s, up_s, down_s):
    def setup():
        up_s[...] = w_up[0].T
        down_s[...] = w_down[0].T

    def dot(k):
        return mm(up_s[block(k), :], tok[...], NT)

    def down():
        next_out[...] = mm(down_s[...], hid_s[...], NN).astype(bf16)

    backs = tri_pieces(tri, hid_s, (down,), (lambda: add_small_tn(small_u, tok_b), lambda: add_small_tn(small_q, grad_b)))
    staged(dot, gelu_act(pre_out, new_s), backs, ((hid_s, new_s),), (tri, small_u, small_q), setup)


def add_wide(acc, left, mat, dims, h):
    acc[h] += mm(left[...], mat[h * FF // 2:(h + 1) * FF // 2, :], dims)


def stage2(u_t, w_up, u_b, grad_b, pre_out, tri, small_u, dwd, new_s, hid_s, up_s):
    def setup():
        up_s[...] = w_up[0].T

    def dot(k):
        return mm(up_s[block(k), :], u_t[...], NN)

    wide = [functools.partial(add_wide, dwd, grad_b, hid_s, TT, h) for h in range(2)]
    backs = tri_pieces(tri, hid_s, wide[:1], (wide[1], lambda: add_small_nt(small_u, u_b)))
    staged(dot, gelu_act(pre_out, new_s), backs, ((hid_s, new_s),), (tri, small_u, dwd), setup)


def stage3(pre_in, grad, w_down, w_up, u_b, err_out, tri, dwu, new_s, g_s):
    def dot(k):
        return mm(w_down[0, block(k), :], grad[...], NT)

    def act(k, value):
        d_hid = value.astype(bf16).astype(f32)
        pre = pre_in[block(k), :].astype(f32)
        sig, cubic = half_sig(pre)
        new_s[block(k), :] = (d_hid * gelu_back(pre, sig, cubic)[1]).astype(bf16)

    def up():
        err_out[...] = mm(w_up[0], g_s[...], NN).astype(bf16)

    wide = [functools.partial(add_wide, dwu, u_b, g_s, NT, h) for h in range(2)]
    staged(dot, act, tri_pieces(tri, g_s, wide, (up,)), ((g_s, new_s),), (tri, dwu))


def stage4(pre_in, err_t, w_down, tok_b, err_b, g_out, small_q, dwd, dwu, new_h, hid_s, new_g, g_s):
    def dot(k):
        return mm(w_down[0, block(k), :], err_t[...], NN)

    def act(k, value):
        d_hid = value.astype(bf16).astype(f32)
        pre = pre_in[block(k), :].astype(f32)
        sig, cubic = half_sig(pre)
        hid, slope = gelu_back(pre, sig, cubic)
        new_h[block(k), :] = hid.astype(bf16)
        grad_up = (d_hid * slope).astype(bf16)
        new_g[block(k), :] = grad_up
        g_out[block(k), :] = grad_up

    def part(q, h):
        if q:
            dwd[h, :, :] += mm(err_b[...], hid_s[h * FF // 2:(h + 1) * FF // 2, :], NT)
        else:
            dwu[h, :, :] += mm(tok_b[...], g_s[h * FF // 2:(h + 1) * FF // 2, :], TT)

    backs = [functools.partial(part, q, h) for q in range(2) for h in range(2)]
    backs += [lambda: add_small_nt(small_q, err_b), lambda: None]
    staged(dot, act, backs, ((hid_s, new_h), (g_s, new_g)), (small_q, dwd, dwu))


def stage5(g_in, tri):
    zero_first((tri,))
    add_tri(tri, g_in)


SMALL = (2, 128, 384)
WIDE = (2, 384, 768)
TRI_SHAPE = (2, TRI // 2, B)
FORMS = {
    "tri": (TRI_SHAPE, ((512, ORDER_Y), (384, ORDER_X), (512, ORDER_X), (384, ORDER_Z), (384, ORDER_X), (512, ORDER_Y))),
    "wide": (WIDE, ((128, ORDER_Z), (128, ORDER_X), (128, ORDER_Y))),
    "small": (SMALL, ((128, ORDER_Y),)),
}


def flows_of(name, form):
    shape, cuts = FORMS[form]
    flows, row = [], 0
    for rows, order in cuts:
        flows.append(Flow(name, row, rows, shape[2], order, row // 16, form == "wide"))
        row += rows
    return flows


def precise(left, right):
    return lax.dot_general(left, right, NN, precision=lax.Precision.HIGHEST, preferred_element_type=f32)


def thirds(x):
    parts = []
    for _ in range(3):
        parts.append(x.astype(bf16))
        x = x - parts[-1].astype(f32)
    return parts


def tile_spec(kind, shape, tile):
    n = shape[0 if kind[0] == "r" else 1] // tile

    def at(i):
        if "b" in kind:
            return jnp.maximum(i - 1, 0)
        return jnp.minimum(i, n - 1) if "f" in kind else i

    if kind[0] == "r":
        return pl.BlockSpec((tile, D), lambda i: (at(i), 0))
    return pl.BlockSpec((shape[0], tile), lambda i: (0, at(i)))


def whole_spec(shape):
    zeros = (0,) * len(shape)
    return pl.BlockSpec(shape, lambda i: zeros, pipeline_mode=pl.Buffered(1))


def block_spec(shape, b):
    return pl.BlockSpec((1,) + shape[1:], lambda i: (b, 0, 0), pipeline_mode=pl.Buffered(1))


ANY = pl.BlockSpec(memory_space=pl.ANY)


class Board:
    def __init__(self):
        self.flows, self.firsts, self.arrays, self.forms, self.fresh = [], [], {}, {}, 0

    def add(self, name, form, array, inverse=None, block=0):
        flows = flows_of(name, form)
        self.flows += flows
        self.forms[name] = FORMS[form][0]
        self.arrays[name + ":src"] = array.reshape(self.forms[name])
        if inverse is not None:
            self.firsts.append(First(name, flows, inverse, block))
            self.arrays[name + ":inv"] = inverse

    def plan(self, tick_us, last):
        for f in self.flows:
            f.at = f.b if hasattr(f, "b") else f.at
        flows = [f for f in self.flows if f.at < LAST and not (f.wide and f.at == 5)]
        idle = [f for f in self.flows if f.wide and f.at == 5]
        for f in idle:
            f.a = f.b = f.at
        slots, rest, end = plan(flows, self.firsts, tick_us, last)
        runs = [f for f in self.firsts if f.fans[0] in flows]
        self.firsts = [f for f in self.firsts if f not in runs]
        self.flows = [f for f in flows + idle if f.b < LAST or f.a < f.b]
        moving = [f for f in flows if f.a < f.b]
        ins, outs = [], {}
        for f in moving:
            if f.a == 0:
                ins.append(f.name + ":src")
            elif f.a < 5 or (f.a == 5 and not f.wide):
                ins.append(f.part + ":in")
            if f.b <= 5:
                outs[f.part + ":out"] = (f.kept(f.b), f.cols)
            else:
                outs[f.name + ":dst"] = self.forms[f.name]
        for first in runs:
            ins.append(first.name + ":inv")
            ins += [f.part + ":in" for f in first.flows if f.part + ":out" not in outs]
        ins += [name for name in outs if name in self.arrays]
        return slots, rest, end, moving, runs, list(dict.fromkeys(ins)), outs

    def keep(self, outs, values):
        for name, value in zip(outs, values):
            self.arrays[name.replace(":out", ":in")] = value


def run_stage(board, body, name, tile, tick_us, ins, outs, scratch, flops, cid, last=False):
    def spec(kind, shape):
        if kind == "w":
            return whole_spec(shape)
        return block_spec(shape, kind) if isinstance(kind, int) else tile_spec(kind, shape, tile)

    steps = len(tick_us)
    slots, rest, end, moving, runs, m_ins, m_outs = board.plan(tick_us, last)
    scr = [job.open(job.a, job.b) if isinstance(job, Flow) else job.open() for job in runs + moving]
    n_in, n_min, n_out, n_mout, n_scr = len(ins), len(m_ins), len(outs), len(m_outs), len(scratch)

    def kernel(*refs):
        refs = list(refs)

        def pull(n):
            return [refs.pop(0) for _ in range(n)]

        c_in, m_in, c_out, m_out, c_scr = pull(n_in), pull(n_min), pull(n_out), pull(n_mout), pull(n_scr)
        named = dict(zip(m_ins, m_in))
        named.update(zip(m_outs, m_out))
        step = pl.program_id(0)
        events = {}
        if moving:
            pl.when(step == 0)(entry_barrier)
        for job, s in zip(runs + moving, scr):
            events[job] = job.bind(named, pull(len(s)))

        def fire(slot):
            for job, what, s in slot:
                if what in ("go", "stop"):
                    events[job][what](s)
                else:
                    events[job][what]()

        for t in range(steps):
            if slots[t]:
                pl.when(step == t)(functools.partial(fire, slots[t]))
        if body is not None:
            body(*c_in, *c_out, *c_scr)
        if rest:
            pl.when(step == steps - 1)(functools.partial(fire, rest))

    params = dict(vmem_limit_bytes=63 * MIB)
    if moving:
        params.update(collective_id=cid, has_side_effects=True)
    values = pl.pallas_call(
        kernel, grid=(steps,),
        in_specs=[spec(kind, arr.shape) for arr, kind in ins] + [ANY] * n_min,
        out_specs=[spec(kind, shape) for shape, dtype, kind in outs] + [ANY] * n_mout,
        out_shape=[jax.ShapeDtypeStruct(shape, dtype) for shape, dtype, kind in outs]
        + [jax.ShapeDtypeStruct(shape, f32) for shape in m_outs.values()],
        scratch_shapes=list(scratch) + [x for s in scr for x in s],
        input_output_aliases={n_in + m_ins.index(m): n_out + i for i, m in enumerate(m_outs) if m in m_ins},
        compiler_params=pltpu.CompilerParams(**params),
        cost_estimate=pl.CostEstimate(flops=flops, bytes_accessed=40 * MIB, transcendentals=0),
        name=name)(*[arr for arr, _ in ins], *[board.arrays[m] for m in m_ins])
    board.keep(m_outs, values[n_out:])
    return values[:n_out]


def final_kernel(decay, t0, t1, t2, t3, n0, n1, n2, n3, old_s, old_a, s0, s1, s2, s3, old_u, old_q, inv_u, inv_q,
                 new_s, new_a, p_up, p_down, new_u, new_q, pk, od, nw, tr, nv, pv, pt, inv_s, sem_in, sem_out):
    rho = decay[0]
    scale = (1.0 - rho) * decay[1]
    deep = pk.shape[0]
    units = []
    for q, (src, old, new) in enumerate(((t0, old_a, new_a), (t1, old_a, new_a), (t2, old_s, new_s), (t3, old_s, new_s))):
        n = (n0, n1, n2, n3)[q]
        off = 0
        for j in range(NB):
            units.append((q, src, old, new, q % 2, j, off, n))
            off += (j + 1) * B

    def loads(u):
        q, src, old, new, b, j, off, n = units[u]
        rows, s = (j + 1) * B, u % deep
        parts = ((src.at[pl.ds(off, rows), :], pk.at[s, pl.ds(0, rows), :]),
                 (old.at[b, pl.ds(0, rows), pl.ds(j * B, B)], od.at[s, pl.ds(0, rows), :]),
                 (n.at[j // 3, :, pl.ds(j % 3 * B, B)], nv.at[s]))
        return [pltpu.make_async_copy(x, y, sem_in.at[s, i]) for i, (x, y) in enumerate(parts)]

    def stores(u):
        q, src, old, new, b, j, off, n = units[u]
        rows, s = (j + 1) * B, u % deep
        parts = [(nw.at[s, pl.ds(0, rows), :], new.at[b, pl.ds(0, rows), pl.ds(j * B, B)])]
        if q < 2:
            parts.append((pv.at[s], p_up.at[b, :, pl.ds(j * B, B)]))
        else:
            parts.append((pt.at[s], p_down.at[b, pl.ds(j * B, B), :]))
        if j:
            parts.append((tr.at[s, :, pl.ds(0, j * B)], new.at[b, pl.ds(j * B, B), pl.ds(0, j * B)]))
        return [pltpu.make_async_copy(x, y, sem_out.at[s, i]) for i, (x, y) in enumerate(parts)]

    for u in range(deep - 1):
        for c in loads(u):
            c.start()
    h = 128
    for acc, old, new, b in ((s0, old_u, new_u, 0), (s1, old_u, new_u, 1), (s2, old_q, new_q, 0), (s3, old_q, new_q, 1)):
        top = rho * old[b, :h, :] + scale * acc[0]
        mid = rho * old[b, h:B, h:] + scale * acc[1, :, :B]
        low = rho * old[b, B:, B:] + scale * acc[1, :, B:]
        new[b, :h, :] = top
        new[b, h:B, h:] = mid
        new[b, B:, B:] = low
        new[b, h:, :h] = top[:, h:].T
        new[b, B:, h:B] = mid[:, h:].T
    for u, (q, src, old, new, b, j, off, n) in enumerate(units):
        s = u % deep
        for c in loads(u):
            c.wait()
        if u >= deep:
            for c in stores(u - deep):
                c.wait()
        for i in range(j + 1):
            here = slice(i * B, (i + 1) * B)
            part = rho * od[s, here, :] + scale * pk[s, here, :]
            nw[s, here, :] = part
            if i < j:
                tr[s, :, here] = part.T
        if j == 0:
            x, y, z = thirds((inv_u if q < 2 else inv_q)[b])
            for i, third in enumerate((x, x, y, x, y, z)):
                inv_s[:, i * D:(i + 1) * D] = third
        x, y, z = thirds(nv[s])
        prod = mm(inv_s[...], jnp.concatenate((x, y, x, z, y, x), axis=0), NN) * decay[1]
        if q < 2:
            pv[s] = prod
        else:
            pt[s] = prod.T
        for c in stores(u):
            c.start()
        if u + deep - 1 < len(units):
            for c in loads(u + deep - 1):
                c.start()
    for u in range(len(units) - deep, len(units)):
        for c in stores(u):
            c.wait()


def finish(decay, tris, smalls, prods, s_up_old, a_down_old, a_up_old, s_down_old, inv_u, inv_q):
    vmem = pl.BlockSpec(memory_space=pltpu.VMEM)
    big = jax.ShapeDtypeStruct(s_up_old.shape, f32)
    small = jax.ShapeDtypeStruct(a_up_old.shape, f32)
    deep = 4
    return pl.pallas_call(
        final_kernel,
        in_specs=[pl.BlockSpec(memory_space=pltpu.SMEM)] + [ANY] * 10 + [vmem] * 8,
        out_specs=[ANY] * 4 + [vmem] * 2,
        out_shape=[big, big, jax.ShapeDtypeStruct((2, D, FF), f32), jax.ShapeDtypeStruct((2, FF, D), f32), small, small],
        scratch_shapes=[pltpu.VMEM((deep, FF, B), f32)] * 3 + [pltpu.VMEM((deep, B, FF), f32)]
        + [pltpu.VMEM((deep, D, B), f32)] * 2 + [pltpu.VMEM((deep, B, D), f32), pltpu.VMEM((D, 6 * D), bf16)] + [pltpu.SemaphoreType.DMA((deep, 3))] * 2,
        compiler_params=pltpu.CompilerParams(vmem_limit_bytes=63 * MIB),
        name="finish")(decay, *[t.reshape(TRI, B) for t in tris], *prods, s_up_old, a_down_old, *smalls,
                       a_up_old, s_down_old, inv_u, inv_q)


def solution(mesh):
    axis_size = mesh.shape["data"]
    tile = 512

    def local_step(tok, grad, w_up, w_down, a_up_old, s_up_old, a_down_old, s_down_old,
                   a_up_inv, s_up_inv, a_down_inv, s_down_inv, factor_decay):
        total = tok.shape[0]
        steps = total // tile
        inv_n = 1.0 / (total * axis_size)
        acts = [pltpu.VMEM((FF, tile), bf16)] * 2
        w_t = pltpu.VMEM((FF, D), bf16)
        unit = 2 * total * FF * D
        wide_out, small_out, tri_out = (WIDE, f32, "w"), (SMALL, f32, "w"), ((TRI, B), f32, "w")
        long_out, short_out = ((FF, total), bf16, "cf"), ((D, total), bf16, "cb")
        board = Board()
        pre0, u1, ad0, au0, sd1 = run_stage(
            board, stage1, "stage1", tile, [0.0] * (steps + 1),
            ((tok, "rf"), (grad, "rf"), (w_up, 0), (w_down, 0), (tok, "rb"), (grad, "rb")),
            (long_out, short_out, tri_out, small_out, small_out), acts + [w_t, pltpu.VMEM((D, FF), bf16)], 5 * unit, 0)
        board.add("ad0", "tri", ad0)
        board.add("au0", "small", au0)
        board.add("sd1", "small", sd1)
        pre1, ad1, au1, dwd1 = run_stage(
            board, stage2, "stage2", tile, [2.0] + [3.5] * steps, ((u1, "cf"), (w_up, 1), (u1, "cb"), (grad, "rb")),
            (long_out, tri_out, small_out, wide_out), acts + [w_t], 5 * unit, 1)
        board.add("ad1", "tri", ad1)
        board.add("au1", "small", au1)
        board.add("dwd1", "wide", dwd1, a_down_inv, 1)
        e1, su1, dwu1 = run_stage(
            board, stage3, "stage3", tile, [2.0] + [4.1] * steps,
            ((pre1, "cf"), (grad, "rf"), (w_down, 1), (w_up, 1), (u1, "cb")), (short_out, tri_out, wide_out), acts, 6 * unit, 2)
        board.add("su1", "tri", su1)
        board.add("dwu1", "wide", dwu1, s_up_inv, 1)
        g0, sd0, dwd0, dwu0 = run_stage(
            board, stage4, "stage4", tile, [2.0] + [3.1] * steps,
            ((pre0, "cf"), (e1, "cf"), (w_down, 0), (tok, "rb"), (e1, "cb")),
            (long_out, small_out, wide_out, wide_out), acts * 2, 4 * unit, 3)
        board.add("sd0", "small", sd0)
        board.add("dwd0", "wide", dwd0, a_down_inv, 0)
        board.add("dwu0", "wide", dwu0, s_up_inv, 0)
        su0, = run_stage(board, stage5, "stage5", tile, [1.9] * steps, ((g0, "c"),), (tri_out,), [], 3 * unit, 4)
        board.add("su0", "tri", su0)
        run_stage(board, None, "tail", tile, [0.1], (), (), [], unit, 5, last=True)
        done = board.arrays
        decay = jnp.stack((factor_decay, jnp.float32(inv_n)))
        new_s, new_a, p_up, p_down, new_u, new_q = finish(
            decay, [done[n + ":dst"] for n in ("ad0", "ad1", "su0", "su1")],
            [done[n + ":dst"] for n in ("au0", "au1", "sd0", "sd1")],
            [done[n + ":dst"] for n in ("dwu0", "dwu1", "dwd0", "dwd1")],
            s_up_old, a_down_old, a_up_old, s_down_old, a_up_inv, s_down_inv)
        return p_up, p_down, new_u, new_s, new_a, new_q

    batch_spec = P("data", None)
    replicated = P()
    return jax.shard_map(local_step, mesh=mesh, in_specs=(batch_spec, batch_spec) + (replicated,) * 11,
                         out_specs=(replicated,) * 6, check_vma=False)
```

```python
import functools

import jax
import jax.numpy as jnp
from jax import lax
from jax.experimental import pallas as pl
from jax.experimental.pallas import tpu as pltpu
from jax.sharding import PartitionSpec as P

bf16 = jnp.bfloat16
f32 = jnp.float32
D, FF, B = 384, 1536, 256
NB = FF // B
TRI = sum((j + 1) * B for j in range(NB))
NN = (((1,), (0,)), ((), ()))
NT = (((1,), (1,)), ((), ()))
TN = (((0,), (0,)), ((), ()))
TT = (((0,), (1,)), ((), ()))
GELU_K = 0.7978845608028654
GELU_C = 0.044715 * GELU_K
MIB = 1 << 20


def mm(left, right, dims):
    return lax.dot_general(left, right, dims, preferred_element_type=f32)


def half_sig(pre):
    cubic = GELU_C * (pre * pre)
    return 0.5 * jnp.tanh(pre * (cubic + GELU_K)) + 0.5, cubic


def gelu_back(pre, sig, cubic):
    hid = pre * sig
    return hid, sig + (hid * (1.0 - sig)) * (6.0 * cubic + 2.0 * GELU_K)


def add_tri(acc, mat):
    off = 0
    for j in range(NB):
        rows = (j + 1) * B
        acc[off:off + rows, :] += mm(mat[:rows, :], mat[j * B:rows, :], NT)
        off += rows


def add_small_tn(acc, rows):
    acc[0] += mm(rows[:, 0:128], rows[...], TN)
    acc[1, :, 0:256] += mm(rows[:, 128:256], rows[:, 128:384], TN)
    acc[1, :, 256:384] += mm(rows[:, 256:384], rows[:, 256:384], TN)


def add_small_nt(acc, cols):
    acc[0] += mm(cols[0:128, :], cols[...], NT)
    acc[1, :, 0:256] += mm(cols[128:256, :], cols[128:384, :], NT)
    acc[1, :, 256:384] += mm(cols[256:384, :], cols[256:384, :], NT)


def zero_first(accs):
    @pl.when(pl.program_id(0) == 0)
    def _():
        for acc in accs:
            acc[...] = jnp.zeros_like(acc)


MESH = pl.DeviceIdType.MESH
ORDER_X, ORDER_Y, ORDER_Z, ORDER_A, ORDER_B = (
    tuple(map(int, order)) for order in ("1234", "2134", "3412", "1342", "2341"))
LINKS = {0: {0: 6e5}, 1: {1: 45e3}, 2: {2: 45e3}, 3: {3: 45e3}, 4: {3: 45e3, 4: 23e3}}
LAG = 2.5
SLACK = 3.0


def PRIORITY(f):
    return f.b


LAST = 10


def my_bits():
    me = lax.axis_index("data")
    bits = [(me // (1 << d)) % 2 for d in range(5)]
    return bits, [me + (1 - 2 * bits[d]) * (1 << d) for d in range(5)]


def entry_barrier():
    peers = my_bits()[1]
    barrier = pltpu.get_barrier_semaphore()
    for peer in peers:
        pl.semaphore_signal(barrier, inc=1, device_id=(peer,), device_id_type=MESH)
    pl.semaphore_wait(barrier, len(peers))


def al(row):
    return pl.multiple_of(row, 8)


class Flow:
    def __init__(self, name, row0, rows, cols, order, shard_row, wide):
        self.name, self.row0, self.rows, self.cols, self.order = name, row0, rows, cols, order
        self.shard_row, self.wide, self.old = shard_row, wide, None
        self.at, self.start = 0, 0.0
        self.part = name + ":part%d" % row0

    def fan(self):
        other = Flow(self.name, self.row0, self.rows, self.cols, self.order, self.shard_row, True)
        other.at = 5
        return other

    def dim(self, s):
        if s in (0, LAST - 1):
            return 0
        return self.order[s - 1] if s < 5 else self.order[LAST - 2 - s]

    def length(self, s):
        return self.rows >> s if s < 5 else self.rows >> (LAST - 1 - s)

    def kept(self, steps):
        return self.rows >> (steps - 1)

    def open(self, a, b):
        self.a, self.b = a, b
        n = b - a
        out = [pltpu.SemaphoreType.DMA((3,)), pltpu.SemaphoreType.DMA((n,)), pltpu.SemaphoreType.DMA((n,))]
        if a < 5:
            out.append(pltpu.VMEM((self.rows if a == 0 else self.kept(a), self.cols), f32))
            out.append(pltpu.VMEM((sum(self.length(s) for s in range(a, min(b, 5))), self.cols), f32))
            if self.mixes():
                out.append(pltpu.VMEM((self.kept(5), self.cols), f32))
        elif a == 5 and not self.wide:
            out.append(pltpu.VMEM((self.kept(5), self.cols), f32))
        return out

    def mixes(self):
        return self.old is not None and self.a < 5 <= self.b

    def bind(self, named, scr):
        a, b, row0, rows = self.a, self.b, self.row0, self.rows
        sem_l, sem_s, sem_r = scr[:3]
        bits, peers = my_bits()
        core = bits[0]
        lens, offs = [rows], [0]
        for d in self.order:
            lens.append(lens[-1] // 2)
            offs.append(offs[-1] + bits[d] * lens[-1])
        src, dst = named.get(self.name + ":src"), named.get(self.name + ":dst")
        part_in, part_out = named.get(self.part + ":in"), named.get(self.part + ":out")
        base = offs[min(max(a, 1), 5) - 1]
        work = recv = None
        if a < 5:
            work, recv = scr[3:5]
        elif a == 5:
            work = named[self.name + ":first"].at[pl.ds(self.shard_row, 8), :] if self.wide else scr[3]
        sends, begin_recv, locals_ = {}, {}, []

        def remote(s, x, y):
            return pltpu.make_async_remote_copy(src_ref=x, dst_ref=y, send_sem=sem_s.at[s - a], recv_sem=sem_r.at[s - a],
                                                device_id=(peers[self.dim(s)],), device_id_type=MESH)

        def final():
            return work if a == 5 else work.at[pl.ds(al(offs[4] - base), lens[4]), :]

        def spot(k):
            return dst.at[core, pl.ds(al(row0 + offs[k]), lens[k]), :]

        at = 0
        for s in range(a, b):
            if s < 5:
                begin_recv[s] = at
                to = recv.at[pl.ds(at, self.length(s)), :]
                at += self.length(s)
                if s == 0:
                    sends[s] = remote(s, src.at[1 - core, pl.ds(row0, rows), :], to)
                else:
                    gone = al(offs[s - 1] - base + (1 - bits[self.dim(s)]) * lens[s])
                    sends[s] = remote(s, work.at[pl.ds(gone, lens[s]), :], to)
            else:
                k = LAST - 1 - s
                sends[s] = remote(s, final() if s == 5 else spot(k), spot(k))
        load = place = save = old = None
        if self.mixes():
            old_array, half = self.old
            spot4 = core * half + row0 + offs[4]
            j = sum((spot4 // (B // 2 * m * (m + 1)) + 31) // 32 for m in range(1, NB))
            old = pltpu.make_async_copy(
                named[self.name + ":old"].at[old_array, pl.ds(al(spot4 - B // 2 * j * (j + 1)), lens[4]),
                                             pl.ds(pl.multiple_of(j * B, B), B)], scr[5], sem_l.at[2])
        if a == 0:
            load = pltpu.make_async_copy(src.at[core, pl.ds(row0, rows), :], work, sem_l.at[0])
        elif a < 5 or (a == 5 and not self.wide):
            load = pltpu.make_async_copy(part_in, work, sem_l.at[0])
        if a <= 5 < b:
            place = pltpu.make_async_copy(final(), spot(4), sem_l.at[1])
        if b <= 5:
            kept = work.at[pl.ds(al(offs[b - 1] - base), lens[b - 1]), :]
            save = pltpu.make_async_copy(kept, part_out, sem_l.at[1])

        def add(row, frm, count):
            for q in range(0, count, 64):
                step = min(count - q, 64)
                x, y = al(row + q), al(frm + q)
                work[pl.ds(x, step), :] = work[pl.ds(x, step), :] + recv[pl.ds(y, step), :]

        def mix():
            rho = named["decay"][0]
            x, y = pl.ds(al(offs[4] - base), lens[4]), pl.ds(begin_recv[4], lens[4])
            total = (work[x, :] + recv[y, :]) * named["decay"][1]
            work[x, :] = rho * scr[5][...] + (1.0 - rho) * total

        def take(s, then):
            if s == a and load is not None and a == 0:
                load.wait()
            sends[s].wait_recv()
            if s == 5 and place is not None:
                place.wait()
            if s >= 5:
                then()
            elif s == 4 and old is not None:
                old.wait()
                mix()
                then()
            elif s == 4 or s + 1 == b:
                add(offs[s] - base, begin_recv[s], lens[s])
                then()
            else:
                half = lens[s + 1]
                bit = bits[self.dim(s + 1)]
                add(offs[s] - base + (1 - bit) * half, begin_recv[s] + (1 - bit) * half, half)
                then()
                add(offs[s] - base + bit * half, begin_recv[s] + bit * half, half)

        def send(s):
            if s == 5:
                place.start()
            sends[s].start()

        def begin():
            load.start()
            if old is not None:
                old.start()
            if a == 0:
                send(0)

        def go(s):
            if s > a:
                take(s - 1, lambda: send(s))
            else:
                if load is not None:
                    load.wait()
                send(s)

        def stop():
            take(b - 1, save.start if save is not None else lambda: None)

        def end():
            if save is not None:
                save.wait()
            for s in range(a, b):
                sends[s].wait_send()

        return {"begin": begin, "go": go, "stop": lambda s: stop(), "end": end}


class First:
    def __init__(self, name, flows, inverse, block):
        self.name, self.flows, self.inverse, self.block, self.done = name, flows, inverse, block, False
        self.fans = [f.fan() for f in flows]

    def open(self):
        rows = pltpu.VMEM((24, 768), f32)
        return [pltpu.SemaphoreType.DMA((4,)), pltpu.SemaphoreType.DMA((3,)), pltpu.SemaphoreType.DMA((3,)),
                rows, rows, rows, pltpu.VMEM((FF, 768), f32)]

    def bind(self, named, scr):
        sem_l, sem_s, sem_r, own, other, prod, inv_v = scr
        named[self.name + ":first"] = prod
        bits, peers = my_bits()
        core = bits[0]
        inv = named[self.name + ":inv"]
        copies, swaps = [], []
        for i, flow in enumerate(self.flows):
            rows = named.get(flow.part + ":out", named.get(flow.part + ":in"))
            spot = pl.ds(flow.shard_row, 8)
            copies.append(pltpu.make_async_copy(rows, own.at[spot, :], sem_l.at[i]))
            swaps.append(pltpu.make_async_remote_copy(
                src_ref=rows, dst_ref=other.at[spot, :], send_sem=sem_s.at[i], recv_sem=sem_r.at[i],
                device_id=(peers[0],), device_id_type=MESH))
        copies.append(pltpu.make_async_copy(
            inv.at[self.block, :, pl.ds(pl.multiple_of(core * 768, 128), 768)], inv_v, sem_l.at[3]))

        def begin():
            for copy in copies + swaps:
                copy.start()

        def go(s):
            for copy in copies + swaps:
                copy.wait()
            prod[...] = (precise(own[...], inv_v[pl.ds(al(core * 768), 768), :])
                         + precise(other[...], inv_v[pl.ds(al((1 - core) * 768), 768), :]))

        return {"begin": begin, "go": go}


def plan(flows, firsts, tick_us, last, over=4.0):
    times = [0.0]
    for us in tick_us:
        times.append(times[-1] + us)
    limit = 1e9 if last else times[-1]
    free, now_rest = {}, times[-1]
    slots, rest = [[] for _ in tick_us], []
    ready = {f: f.start for f in flows}
    phase = {f: "new" for f in flows}
    for f in flows:
        f.a = f.b = f.at
    fstate = {f: "new" for f in firsts}
    fready = {}

    def arrival(f, s, now):
        links = LINKS[f.dim(s)]
        size = f.length(s) * f.cols * 4
        begin = max([now] + [free.get(link, 0.0) for link in links])
        return begin, max(begin + size / rate for rate in links.values()), size

    def send(f, s, now):
        begin, end, size = arrival(f, s, now)
        for link, rate in LINKS[f.dim(s)].items():
            free[link] = begin + size / rate
        f.b = s + 1
        ready[f] = end + LAG

    def allowed(f, s, now):
        return last or (now < limit and arrival(f, s, now)[1] + LAG < limit + over)

    def clear(f, s, now):
        return arrival(f, s, now)[0] <= now + SLACK

    def move(f, now):
        if ready[f] > now:
            return None
        if phase[f] == "new":
            if f.at >= LAST or f.wide and f.at == 5:
                return None
            if not allowed(f, f.at, now + (LAG if 0 < f.at <= 5 else 0.0)):
                return None
            if not clear(f, f.at, now):
                return None
            if f.at == 0:
                phase[f] = "run"
                send(f, 0, now)
                return "begin", 0
            if f.at <= 5:
                phase[f] = "loaded"
                ready[f] = now + LAG
                f.b = f.at + 1
                return "begin", 0
            phase[f] = "run"
            send(f, f.at, now)
            return "go", f.at
        if phase[f] == "loaded":
            phase[f] = "run"
            send(f, f.at, now)
            return "go", f.at
        if phase[f] == "run":
            s = f.b
            if s == LAST or f.wide and s == 5 or not allowed(f, s, now):
                phase[f] = "saved"
                ready[f] = now + LAG
                return "stop", s
            if not clear(f, s, now):
                return None
            send(f, s, now)
            return "go", s
        if phase[f] == "saved":
            phase[f] = "done"
            return "end", 0
        return None

    def first_move(f, now):
        if f.done or fready.get(f, 0.0) > now:
            return None
        if fstate[f] == "new":
            ok = all(x.b == 5 and phase.get(x, "done") in ("new", "done") for x in f.flows)
            if not ok or not (last or now + 20.0 < limit):
                return None
            fstate[f] = "loaded"
            fready[f] = now + 5.0
            return "begin", 0
        if fstate[f] == "loaded":
            fstate[f] = "done"
            return "go", 0
        return None

    def sweep(now, out):
        again = True
        while again:
            again = False
            for f in sorted(flows, key=PRIORITY):
                e = move(f, now)
                if e:
                    out.append((f,) + e)
                    again = True
                    break
            for f in firsts:
                e = first_move(f, now)
                if e:
                    out.append((f,) + e)
                    again = True
                    if fstate[f] == "done":
                        for x in f.fans:
                            flows.append(x)
                            x.a = 5
                            phase[x] = "run"
                            send(x, 5, now)
                            out.append((x, "go", 5))

    for t, now in enumerate(times[:-1]):
        sweep(now, slots[t])
    now = times[-1]
    while True:
        sweep(now, rest)
        later = [ready[f] for f in flows if phase[f] in ("loaded", "run", "saved") and ready[f] > now]
        later += [fready[f] for f in firsts if fstate[f] == "loaded" and fready[f] > now]
        held = any(phase[f] in ("loaded", "run") or last and phase[f] == "new" and f.at < LAST and not (f.wide and f.at == 5)
                   for f in flows)
        if not later and not held:
            return slots, rest, now
        now = min(later + ([now + 1.0] if held else []))


def tri_col(acc, mat, j):
    rows = (j + 1) * B
    off = B * j * (j + 1) // 2
    acc[off:off + rows, :] += mm(mat[:rows, :], mat[j * B:rows, :], NT)


def staged(dot, act, backs, shifts, accs, setup=None):
    step, last = pl.program_id(0), pl.num_programs(0) - 1

    def shift():
        for old, new in shifts:
            old[...] = new[...]

    @pl.when(step == 0)
    def _():
        for acc in accs:
            acc[...] = jnp.zeros_like(acc)
        if setup is not None:
            setup()
        for k in range(NB):
            act(k, dot(k))

    @pl.when((step > 0) & (step < last))
    def _():
        shift()
        for k, back in enumerate(backs):
            value = dot(k)
            back()
            act(k, value)

    @pl.when(step == last)
    def _():
        shift()
        for back in backs:
            back()


def plain(dot, act, backs, accs, setup):
    @pl.when(pl.program_id(0) == 0)
    def _():
        for acc in accs:
            acc[...] = jnp.zeros_like(acc)
        setup()

    for k in range(NB):
        act(k, dot(k))
    for back in backs:
        back()


def block(k):
    return slice(k * B, (k + 1) * B)


def tri_pieces(acc, mat, *more):
    pieces = [(5,), (4,), (3, 0), (2, 1)]

    def run(cols, fns):
        for j in cols:
            tri_col(acc, mat, j)
        for fn in fns:
            fn()

    return [functools.partial(run, cols, ()) for cols in pieces] + [functools.partial(run, (), fns) for fns in more]


def gelu_act(pre_out, new_s):
    def act(k, value):
        pre = value.astype(bf16)
        pre_out[block(k), :] = pre
        pre = pre.astype(f32)
        new_s[block(k), :] = (pre * half_sig(pre)[0]).astype(bf16)
    return act


def stage1(tok, grad, w_up, w_down, pre_out, next_out, tri, small_u, small_q, hid_s, up_s, down_s):
    def setup():
        up_s[...] = w_up[0].T
        down_s[...] = w_down[0].T

    def dot(k):
        return mm(up_s[block(k), :], tok[...], NT)

    def down():
        next_out[...] = mm(down_s[...], hid_s[...], NN).astype(bf16)

    def smalls():
        add_small_tn(small_u, tok)
        add_small_tn(small_q, grad)

    backs = [functools.partial(tri_col, tri, hid_s, j) for j in range(NB)] + [down, smalls]
    plain(dot, gelu_act(pre_out, hid_s), backs, (tri, small_u, small_q), setup)


def add_wide(acc, left, mat, dims, h):
    acc[h] += mm(left[...], mat[h * FF // 2:(h + 1) * FF // 2, :], dims)


def stage2(u_t, w_up, u_b, grad_b, pre_out, tri, small_u, dwd, new_s, hid_s, up_s):
    def setup():
        up_s[...] = w_up[0].T

    def dot(k):
        return mm(up_s[block(k), :], u_t[...], NN)

    wide = [functools.partial(add_wide, dwd, grad_b, hid_s, TT, h) for h in range(2)]
    backs = tri_pieces(tri, hid_s, wide[:1], (wide[1], lambda: add_small_nt(small_u, u_b)))
    staged(dot, gelu_act(pre_out, new_s), backs, ((hid_s, new_s),), (tri, small_u, dwd), setup)


def stage3(pre_in, grad, w_down, w_up, u_b, err_out, tri, dwu, new_s, g_s):
    def dot(k):
        return mm(w_down[0, block(k), :], grad[...], NT)

    def act(k, value):
        d_hid = value.astype(bf16).astype(f32)
        pre = pre_in[block(k), :].astype(f32)
        sig, cubic = half_sig(pre)
        new_s[block(k), :] = (d_hid * gelu_back(pre, sig, cubic)[1]).astype(bf16)

    def up():
        err_out[...] = mm(w_up[0], g_s[...], NN).astype(bf16)

    wide = [functools.partial(add_wide, dwu, u_b, g_s, NT, h) for h in range(2)]
    staged(dot, act, tri_pieces(tri, g_s, wide, (up,)), ((g_s, new_s),), (tri, dwu))


def stage4(pre_in, err_t, w_down, tok_b, err_b, g_out, small_q, dwd, dwu, new_h, hid_s, new_g, g_s):
    def dot(k):
        return mm(w_down[0, block(k), :], err_t[...], NN)

    def act(k, value):
        d_hid = value.astype(bf16).astype(f32)
        pre = pre_in[block(k), :].astype(f32)
        sig, cubic = half_sig(pre)
        hid, slope = gelu_back(pre, sig, cubic)
        new_h[block(k), :] = hid.astype(bf16)
        grad_up = (d_hid * slope).astype(bf16)
        new_g[block(k), :] = grad_up
        g_out[block(k), :] = grad_up

    def part(q, h):
        if q:
            dwd[h, :, :] += mm(err_b[...], hid_s[h * FF // 2:(h + 1) * FF // 2, :], NT)
        else:
            dwu[h, :, :] += mm(tok_b[...], g_s[h * FF // 2:(h + 1) * FF // 2, :], TT)

    backs = [functools.partial(part, q, h) for q in range(2) for h in range(2)]
    backs += [lambda: add_small_nt(small_q, err_b), lambda: None]
    staged(dot, act, backs, ((hid_s, new_h), (g_s, new_g)), (small_q, dwd, dwu))


def stage5(g_in, tri):
    zero_first((tri,))
    add_tri(tri, g_in)


SMALL = (2, 128, 384)
WIDE = (2, 384, 768)
TRI_SHAPE = (2, TRI // 2, B)
FORMS = {
    "tri": (TRI_SHAPE, ((512, ORDER_X), (512, ORDER_B), (512, ORDER_X), (512, ORDER_Z), (512, ORDER_Y), (128, ORDER_B))),
    "wide": (WIDE, ((128, ORDER_Y), (128, ORDER_Y), (128, ORDER_A))),
    "small": (SMALL, ((128, ORDER_X),)),
}


def flows_of(name, form):
    shape, cuts = FORMS[form]
    flows, row = [], 0
    for rows, order in cuts:
        flows.append(Flow(name, row, rows, shape[2], order, row // 16, form == "wide"))
        row += rows
    return flows


def precise(left, right):
    return lax.dot_general(left, right, NN, precision=lax.Precision.HIGHEST, preferred_element_type=f32)


def thirds(x):
    parts = []
    for _ in range(3):
        parts.append(x.astype(bf16))
        x = x - parts[-1].astype(f32)
    return parts


def tile_spec(kind, shape, tile):
    n = shape[0 if kind[0] == "r" else 1] // tile

    def at(i):
        if "b" in kind:
            return jnp.maximum(i - 1, 0)
        return jnp.minimum(i, n - 1) if "f" in kind else i

    if kind[0] == "r":
        return pl.BlockSpec((tile, D), lambda i: (at(i), 0))
    return pl.BlockSpec((shape[0], tile), lambda i: (0, at(i)))


def whole_spec(shape):
    zeros = (0,) * len(shape)
    return pl.BlockSpec(shape, lambda i: zeros, pipeline_mode=pl.Buffered(1))


def block_spec(shape, b):
    return pl.BlockSpec((1,) + shape[1:], lambda i: (b, 0, 0), pipeline_mode=pl.Buffered(1))


ANY = pl.BlockSpec(memory_space=pl.ANY)
SCALARS = pl.BlockSpec(memory_space=pltpu.SMEM)


class Board:
    def __init__(self):
        self.flows, self.firsts, self.arrays, self.forms, self.fresh = [], [], {}, {}, 0

    def add(self, name, form, array, other=None, block=0):
        flows = flows_of(name, form)
        self.flows += flows
        self.forms[name] = FORMS[form][0]
        self.arrays[name + ":src"] = array.reshape(self.forms[name])
        if form == "wide":
            self.firsts.append(First(name, flows, other, block))
            self.arrays[name + ":inv"] = other
        elif form == "tri":
            for f in flows:
                f.old = (block, TRI // 2)
            self.arrays[name + ":old"] = other

    def plan(self, tick_us, last):
        for f in self.flows:
            f.at = f.b if hasattr(f, "b") else f.at
        flows = [f for f in self.flows if f.at < LAST and not (f.wide and f.at == 5)]
        idle = [f for f in self.flows if f.wide and f.at == 5]
        for f in idle:
            f.a = f.b = f.at
        slots, rest, end = plan(flows, self.firsts, tick_us, last)
        runs = [f for f in self.firsts if f.fans[0] in flows]
        self.firsts = [f for f in self.firsts if f not in runs]
        self.flows = [f for f in flows + idle if f.b < LAST or f.a < f.b]
        moving = [f for f in flows if f.a < f.b]
        ins, outs = [], {}
        for f in moving:
            if f.a == 0:
                ins.append(f.name + ":src")
            elif f.a < 5 or (f.a == 5 and not f.wide):
                ins.append(f.part + ":in")
            if f.mixes():
                ins += ["decay", f.name + ":old"]
            if f.b <= 5:
                outs[f.part + ":out"] = (f.kept(f.b), f.cols)
            else:
                outs[f.name + ":dst"] = self.forms[f.name]
        for first in runs:
            ins.append(first.name + ":inv")
            ins += [f.part + ":in" for f in first.flows if f.part + ":out" not in outs]
        ins += [name for name in outs if name in self.arrays]
        return slots, rest, end, moving, runs, list(dict.fromkeys(ins)), outs

    def keep(self, outs, values):
        for name, value in zip(outs, values):
            self.arrays[name.replace(":out", ":in")] = value


def run_stage(board, body, name, tile, tick_us, ins, outs, scratch, flops, cid, last=False):
    def spec(kind, shape):
        if kind == "w":
            return whole_spec(shape)
        return block_spec(shape, kind) if isinstance(kind, int) else tile_spec(kind, shape, tile)

    steps = len(tick_us)
    slots, rest, end, moving, runs, m_ins, m_outs = board.plan(tick_us, last)
    scr = [job.open(job.a, job.b) if isinstance(job, Flow) else job.open() for job in runs + moving]
    n_in, n_min, n_out, n_mout, n_scr = len(ins), len(m_ins), len(outs), len(m_outs), len(scratch)

    def kernel(*refs):
        refs = list(refs)

        def pull(n):
            return [refs.pop(0) for _ in range(n)]

        c_in, m_in, c_out, m_out, c_scr = pull(n_in), pull(n_min), pull(n_out), pull(n_mout), pull(n_scr)
        named = dict(zip(m_ins, m_in))
        named.update(zip(m_outs, m_out))
        step = pl.program_id(0)
        events = {}
        if moving:
            pl.when(step == 0)(entry_barrier)
        for job, s in zip(runs + moving, scr):
            events[job] = job.bind(named, pull(len(s)))

        def fire(slot):
            for job, what, s in slot:
                if what in ("go", "stop"):
                    events[job][what](s)
                else:
                    events[job][what]()

        for t in range(steps):
            if slots[t]:
                pl.when(step == t)(functools.partial(fire, slots[t]))
        if body is not None:
            body(*c_in, *c_out, *c_scr)
        if rest:
            pl.when(step == steps - 1)(functools.partial(fire, rest))

    params = dict(vmem_limit_bytes=63 * MIB)
    if moving:
        params.update(collective_id=cid, has_side_effects=True)
    values = pl.pallas_call(
        kernel, grid=(steps,),
        in_specs=[spec(kind, arr.shape) for arr, kind in ins] + [SCALARS if m == "decay" else ANY for m in m_ins],
        out_specs=[spec(kind, shape) for shape, dtype, kind in outs] + [ANY] * n_mout,
        out_shape=[jax.ShapeDtypeStruct(shape, dtype) for shape, dtype, kind in outs]
        + [jax.ShapeDtypeStruct(shape, f32) for shape in m_outs.values()],
        scratch_shapes=list(scratch) + [x for s in scr for x in s],
        input_output_aliases={n_in + m_ins.index(m): n_out + i for i, m in enumerate(m_outs) if m in m_ins},
        compiler_params=pltpu.CompilerParams(**params),
        cost_estimate=pl.CostEstimate(flops=flops, bytes_accessed=40 * MIB, transcendentals=0),
        name=name)(*[arr for arr, _ in ins], *[board.arrays[m] for m in m_ins])
    board.keep(m_outs, values[n_out:])
    return values[:n_out]


def final_kernel(decay, t0, t1, t2, t3, n0, n1, n2, n3, s0, s1, s2, s3, old_u, old_q, inv_u, inv_q,
                 new_s, new_a, p_up, p_down, new_u, new_q, pk, tr, nv, pv, pt, inv_s, sem_in, sem_out):
    rho = decay[0]
    scale = (1.0 - rho) * decay[1]
    deep = pk.shape[0]
    ahead = deep // 2
    units = []
    for q, (src, new, n) in enumerate(((t0, new_a, n0), (t1, new_a, n1), (t2, new_s, n2), (t3, new_s, n3))):
        off = 0
        for j in range(NB):
            units.append((q, src, new, q % 2, j, off, n))
            off += (j + 1) * B

    def loads(u):
        q, src, new, b, j, off, n = units[u]
        rows, s = (j + 1) * B, u % deep
        parts = ((src.at[pl.ds(off, rows), :], pk.at[s, pl.ds(0, rows), :]),
                 (n.at[j // 3, :, pl.ds(j % 3 * B, B)], nv.at[s]))
        return [pltpu.make_async_copy(x, y, sem_in.at[s, i]) for i, (x, y) in enumerate(parts)]

    def stores(u):
        q, src, new, b, j, off, n = units[u]
        rows, s = (j + 1) * B, u % deep
        parts = [(pk.at[s, pl.ds(0, rows), :], new.at[b, pl.ds(0, rows), pl.ds(j * B, B)])]
        if q < 2:
            parts.append((pv.at[s], p_up.at[b, :, pl.ds(j * B, B)]))
        else:
            parts.append((pt.at[s], p_down.at[b, pl.ds(j * B, B), :]))
        if j:
            parts.append((tr.at[s, :, pl.ds(0, j * B)], new.at[b, pl.ds(j * B, B), pl.ds(0, j * B)]))
        return [pltpu.make_async_copy(x, y, sem_out.at[s, i]) for i, (x, y) in enumerate(parts)]

    for u in range(ahead):
        for c in loads(u):
            c.start()
    h = B // 2
    for acc, old, new, b in ((s0, old_u, new_u, 0), (s1, old_u, new_u, 1), (s2, old_q, new_q, 0), (s3, old_q, new_q, 1)):
        top = rho * old[b, :h, :] + scale * acc[0]
        mid = rho * old[b, h:B, h:] + scale * acc[1, :, :B]
        low = rho * old[b, B:, B:] + scale * acc[1, :, B:]
        new[b, :h, :] = top
        new[b, h:B, h:] = mid
        new[b, B:, B:] = low
        new[b, h:, :h] = top[:, h:].T
        new[b, B:, h:B] = mid[:, h:].T
    for u, (q, src, new, b, j, off, n) in enumerate(units):
        s = u % deep
        for c in loads(u):
            c.wait()
        for i in range(j):
            here = slice(i * B, (i + 1) * B)
            tr[s, :, here] = pk[s, here, :].T
        if j == 0:
            x, y, z = thirds((inv_u if q < 2 else inv_q)[b])
            for i, third in enumerate((x, x, y, x, y, z)):
                inv_s[:, i * D:(i + 1) * D] = third
        x, y, z = thirds(nv[s])
        prod = mm(inv_s[...], jnp.concatenate((x, y, x, z, y, x), axis=0), NN) * decay[1]
        if q < 2:
            pv[s] = prod
        else:
            pt[s] = prod.T
        for c in stores(u):
            c.start()
        if u + ahead < len(units):
            if u + ahead >= deep:
                for c in stores(u + ahead - deep):
                    c.wait()
            for c in loads(u + ahead):
                c.start()
    for u in range(len(units) - deep, len(units)):
        for c in stores(u):
            c.wait()


def finish(decay, tris, smalls, prods, s_up_old, a_up_old, s_down_old, inv_u, inv_q):
    vmem = pl.BlockSpec(memory_space=pltpu.VMEM)
    big = jax.ShapeDtypeStruct(s_up_old.shape, f32)
    small = jax.ShapeDtypeStruct(a_up_old.shape, f32)
    deep = 6
    return pl.pallas_call(
        final_kernel,
        in_specs=[SCALARS] + [ANY] * 8 + [vmem] * 8,
        out_specs=[ANY] * 4 + [vmem] * 2,
        out_shape=[big, big, jax.ShapeDtypeStruct((2, D, FF), f32), jax.ShapeDtypeStruct((2, FF, D), f32), small, small],
        scratch_shapes=[pltpu.VMEM((deep, FF, B), f32), pltpu.VMEM((deep, B, FF), f32)]
        + [pltpu.VMEM((deep, D, B), f32)] * 2 + [pltpu.VMEM((deep, B, D), f32), pltpu.VMEM((D, 6 * D), bf16)]
        + [pltpu.SemaphoreType.DMA((deep, 3))] * 2,
        compiler_params=pltpu.CompilerParams(vmem_limit_bytes=63 * MIB),
        name="finish")(decay, *[t.reshape(TRI, B) for t in tris], *prods, *smalls, a_up_old, s_down_old, inv_u, inv_q)


def solution(mesh):
    axis_size = mesh.shape["data"]
    tile = 512

    def local_step(tok, grad, w_up, w_down, a_up_old, s_up_old, a_down_old, s_down_old,
                   a_up_inv, s_up_inv, a_down_inv, s_down_inv, factor_decay):
        total = tok.shape[0]
        steps = total // tile
        inv_n = 1.0 / (total * axis_size)
        acts = [pltpu.VMEM((FF, tile), bf16)] * 2
        w_t = pltpu.VMEM((FF, D), bf16)
        unit = 2 * total * FF * D
        wide_out, small_out, tri_out = (WIDE, f32, "w"), (SMALL, f32, "w"), ((TRI, B), f32, "w")
        long_out, short_out = ((FF, total), bf16, "cf"), ((D, total), bf16, "cb")
        board = Board()
        decay = jnp.stack((factor_decay, jnp.float32(inv_n)))
        board.arrays["decay"] = decay
        pre0, u1, ad0, au0, sd1 = run_stage(
            board, stage1, "stage1", 2 * tile, [0.0] * (steps // 2),
            ((tok, "r"), (grad, "r"), (w_up, 0), (w_down, 0)),
            (long_out, ((D, total), bf16, "c"), tri_out, small_out, small_out),
            [pltpu.VMEM((FF, 2 * tile), bf16), w_t, pltpu.VMEM((D, FF), bf16)], 5 * unit, 0)
        board.add("ad0", "tri", ad0, a_down_old, 0)
        board.add("au0", "small", au0)
        board.add("sd1", "small", sd1)
        pre1, ad1, au1, dwd1 = run_stage(
            board, stage2, "stage2", tile, [2.4] + [4.0] * steps, ((u1, "cf"), (w_up, 1), (u1, "cb"), (grad, "rb")),
            (long_out, tri_out, small_out, wide_out), acts + [w_t], 5 * unit, 1)
        board.add("ad1", "tri", ad1, a_down_old, 1)
        board.add("au1", "small", au1)
        board.add("dwd1", "wide", dwd1, a_down_inv, 1)
        e1, su1, dwu1 = run_stage(
            board, stage3, "stage3", tile, [2.4] + [4.8] * steps,
            ((pre1, "cf"), (grad, "rf"), (w_down, 1), (w_up, 1), (u1, "cb")), (short_out, tri_out, wide_out), acts, 6 * unit, 2)
        board.add("su1", "tri", su1, s_up_old, 1)
        board.add("dwu1", "wide", dwu1, s_up_inv, 1)
        g0, sd0, dwd0, dwu0 = run_stage(
            board, stage4, "stage4", tile, [2.5] + [3.6] * steps,
            ((pre0, "cf"), (e1, "cf"), (w_down, 0), (tok, "rb"), (e1, "cb")),
            (long_out, small_out, wide_out, wide_out), acts * 2, 4 * unit, 3)
        board.add("sd0", "small", sd0)
        board.add("dwd0", "wide", dwd0, a_down_inv, 0)
        board.add("dwu0", "wide", dwu0, s_up_inv, 0)
        su0, = run_stage(board, stage5, "stage5", tile, [2.2] * steps, ((g0, "c"),), (tri_out,), [], 3 * unit, 4)
        board.add("su0", "tri", su0, s_up_old, 0)
        run_stage(board, None, "tail", tile, [0.1], (), (), [], unit, 5, last=True)
        done = board.arrays
        new_s, new_a, p_up, p_down, new_u, new_q = finish(
            decay, [done[n + ":dst"] for n in ("ad0", "ad1", "su0", "su1")],
            [done[n + ":dst"] for n in ("au0", "au1", "sd0", "sd1")],
            [done[n + ":dst"] for n in ("dwu0", "dwu1", "dwd0", "dwd1")],
            s_up_old, a_up_old, s_down_old, a_up_inv, s_down_inv)
        return p_up, p_down, new_u, new_s, new_a, new_q

    batch_spec = P("data", None)
    replicated = P()
    return jax.shard_map(local_step, mesh=mesh, in_specs=(batch_spec, batch_spec) + (replicated,) * 11,
                         out_specs=(replicated,) * 6, check_vma=False)
```

```python
import functools

import jax
import jax.numpy as jnp
from jax import lax
from jax.experimental import pallas as pl
from jax.experimental.pallas import tpu as pltpu
from jax.sharding import PartitionSpec as P

bf16 = jnp.bfloat16
f32 = jnp.float32
D, FF, B = 384, 1536, 256
NB = FF // B
TRI = sum((j + 1) * B for j in range(NB))
NN = (((1,), (0,)), ((), ()))
NT = (((1,), (1,)), ((), ()))
TN = (((0,), (0,)), ((), ()))
TT = (((0,), (1,)), ((), ()))
GELU_K = 0.7978845608028654
GELU_C = 0.044715 * GELU_K
MIB = 1 << 20


def mm(left, right, dims):
    return lax.dot_general(left, right, dims, preferred_element_type=f32)


def half_sig(pre):
    cubic = GELU_C * (pre * pre)
    return 0.5 * jnp.tanh(pre * (cubic + GELU_K)) + 0.5, cubic


def gelu_back(pre, sig, cubic):
    hid = pre * sig
    return hid, sig + (hid * (1.0 - sig)) * (6.0 * cubic + 2.0 * GELU_K)


def add_tri(acc, mat):
    off = 0
    for j in range(NB):
        rows = (j + 1) * B
        acc[off:off + rows, :] += mm(mat[:rows, :], mat[j * B:rows, :], NT)
        off += rows


def add_small_tn(acc, rows):
    acc[0] += mm(rows[:, 0:128], rows[...], TN)
    acc[1, :, 0:256] += mm(rows[:, 128:256], rows[:, 128:384], TN)
    acc[1, :, 256:384] += mm(rows[:, 256:384], rows[:, 256:384], TN)


def add_small_nt(acc, cols):
    acc[0] += mm(cols[0:128, :], cols[...], NT)
    acc[1, :, 0:256] += mm(cols[128:256, :], cols[128:384, :], NT)
    acc[1, :, 256:384] += mm(cols[256:384, :], cols[256:384, :], NT)


def zero_first(accs):
    @pl.when(pl.program_id(0) == 0)
    def _():
        for acc in accs:
            acc[...] = jnp.zeros_like(acc)


MESH = pl.DeviceIdType.MESH
ORDERS = {key: tuple(map(int, order)) for key, order in
          (("X", "1234"), ("Y", "2134"), ("Z", "3412"), ("A", "1342"), ("B", "2341"), ("C", "3421"))}
LINKS = {0: {0: 6e5}, 1: {1: 45e3}, 2: {2: 45e3}, 3: {3: 45e3}, 4: {3: 45e3, 4: 23e3}}
LAG = 2.0
SLACK = 3.0


def PRIORITY(f):
    return f.b


LAST = 10


def my_bits():
    me = lax.axis_index("data")
    bits = [(me // (1 << d)) % 2 for d in range(5)]
    return bits, [me + (1 - 2 * bits[d]) * (1 << d) for d in range(5)]


def entry_barrier():
    peers = my_bits()[1]
    barrier = pltpu.get_barrier_semaphore()
    for peer in peers:
        pl.semaphore_signal(barrier, inc=1, device_id=(peer,), device_id_type=MESH)
    pl.semaphore_wait(barrier, len(peers))


def al(row):
    return pl.multiple_of(row, 8)


class Flow:
    def __init__(self, name, row0, rows, cols, order, shard_row, wide):
        self.name, self.row0, self.rows, self.cols, self.order = name, row0, rows, cols, order
        self.shard_row, self.wide, self.old = shard_row, wide, None
        self.at, self.start = 0, 0.0
        self.part = name + ":part%d" % row0

    def fan(self):
        other = Flow(self.name, self.row0, self.rows, self.cols, self.order, self.shard_row, True)
        other.at = 5
        return other

    def dim(self, s):
        if s in (0, LAST - 1):
            return 0
        return self.order[s - 1] if s < 5 else self.order[LAST - 2 - s]

    def length(self, s):
        return self.rows >> s if s < 5 else self.rows >> (LAST - 1 - s)

    def kept(self, steps):
        return self.rows >> (steps - 1)

    def open(self, a, b):
        self.a, self.b = a, b
        n = b - a
        out = [pltpu.SemaphoreType.DMA((3,)), pltpu.SemaphoreType.DMA((n,)), pltpu.SemaphoreType.DMA((n,))]
        if a < 5:
            out.append(pltpu.VMEM((self.rows if a == 0 else self.kept(a), self.cols), f32))
            out.append(pltpu.VMEM((sum(self.length(s) for s in range(a, min(b, 5))), self.cols), f32))
            if self.mixes():
                out.append(pltpu.VMEM((self.kept(5), self.cols), f32))
        elif a == 5 and not self.wide:
            out.append(pltpu.VMEM((self.kept(5), self.cols), f32))
        return out

    def mixes(self):
        return self.old is not None and self.a < 5 <= self.b

    def bind(self, named, scr):
        a, b, row0, rows = self.a, self.b, self.row0, self.rows
        sem_l, sem_s, sem_r = scr[:3]
        bits, peers = my_bits()
        core = bits[0]
        lens, offs = [rows], [0]
        for d in self.order:
            lens.append(lens[-1] // 2)
            offs.append(offs[-1] + bits[d] * lens[-1])
        src, dst = named.get(self.name + ":src"), named.get(self.name + ":dst")
        part_in, part_out = named.get(self.part + ":in"), named.get(self.part + ":out")
        base = offs[min(max(a, 1), 5) - 1]
        work = recv = None
        if a < 5:
            work, recv = scr[3:5]
        elif a == 5:
            work = named[self.name + ":first"].at[pl.ds(self.shard_row, self.kept(5)), :] if self.wide else scr[3]
        sends, begin_recv, locals_ = {}, {}, []

        def remote(s, x, y):
            return pltpu.make_async_remote_copy(src_ref=x, dst_ref=y, send_sem=sem_s.at[s - a], recv_sem=sem_r.at[s - a],
                                                device_id=(peers[self.dim(s)],), device_id_type=MESH)

        def final():
            return work if a == 5 else work.at[pl.ds(al(offs[4] - base), lens[4]), :]

        def spot(k):
            return dst.at[core, pl.ds(al(row0 + offs[k]), lens[k]), :]

        at = 0
        for s in range(a, b):
            if s < 5:
                begin_recv[s] = at
                to = recv.at[pl.ds(at, self.length(s)), :]
                at += self.length(s)
                if s == 0:
                    sends[s] = remote(s, src.at[1 - core, pl.ds(row0, rows), :], to)
                else:
                    gone = al(offs[s - 1] - base + (1 - bits[self.dim(s)]) * lens[s])
                    sends[s] = remote(s, work.at[pl.ds(gone, lens[s]), :], to)
            else:
                k = LAST - 1 - s
                sends[s] = remote(s, final() if s == 5 else spot(k), spot(k))
        load = place = save = old = None
        if self.mixes():
            old_array, half = self.old
            spot4 = core * half + row0 + offs[4]
            j = sum((spot4 // (B // 2 * m * (m + 1)) + 31) // 32 for m in range(1, NB))
            old = pltpu.make_async_copy(
                named[self.name + ":old"].at[old_array, pl.ds(al(spot4 - B // 2 * j * (j + 1)), lens[4]),
                                             pl.ds(pl.multiple_of(j * B, B), B)], scr[5], sem_l.at[2])
        if a == 0:
            load = pltpu.make_async_copy(src.at[core, pl.ds(row0, rows), :], work, sem_l.at[0])
        elif a < 5 or (a == 5 and not self.wide):
            load = pltpu.make_async_copy(part_in, work, sem_l.at[0])
        if a <= 5 < b:
            place = pltpu.make_async_copy(final(), spot(4), sem_l.at[1])
        if b <= 5:
            kept = work.at[pl.ds(al(offs[b - 1] - base), lens[b - 1]), :]
            save = pltpu.make_async_copy(kept, part_out, sem_l.at[1])

        def add(row, frm, count):
            for q in range(0, count, 64):
                step = min(count - q, 64)
                x, y = al(row + q), al(frm + q)
                work[pl.ds(x, step), :] = work[pl.ds(x, step), :] + recv[pl.ds(y, step), :]

        def mix():
            rho = named["decay"][0]
            x, y = pl.ds(al(offs[4] - base), lens[4]), pl.ds(begin_recv[4], lens[4])
            total = (work[x, :] + recv[y, :]) * named["decay"][1]
            work[x, :] = rho * scr[5][...] + (1.0 - rho) * total

        def take(s, then):
            if s == a and load is not None and a == 0:
                load.wait()
            sends[s].wait_recv()
            if s == 5 and place is not None:
                place.wait()
            if s >= 5:
                then()
            elif s == 4 and old is not None:
                old.wait()
                mix()
                then()
            elif s == 4 or s + 1 == b:
                add(offs[s] - base, begin_recv[s], lens[s])
                then()
            else:
                half = lens[s + 1]
                bit = bits[self.dim(s + 1)]
                add(offs[s] - base + (1 - bit) * half, begin_recv[s] + (1 - bit) * half, half)
                then()
                add(offs[s] - base + bit * half, begin_recv[s] + bit * half, half)

        def send(s):
            if s == 5:
                place.start()
            sends[s].start()

        def begin():
            load.start()
            if old is not None:
                old.start()
            if a == 0:
                send(0)

        def go(s):
            if s > a:
                take(s - 1, lambda: send(s))
            else:
                if load is not None:
                    load.wait()
                send(s)

        def stop():
            take(b - 1, save.start if save is not None else lambda: None)

        def end():
            if save is not None:
                save.wait()
            for s in range(a, b):
                sends[s].wait_send()

        return {"begin": begin, "go": go, "stop": lambda s: stop(), "end": end}


class First:
    def __init__(self, name, flows, inverse, block):
        self.name, self.flows, self.inverse, self.block, self.done = name, flows, inverse, block, False
        self.fans = [f.fan() for f in flows]

    def open(self):
        rows = pltpu.VMEM((24, 768), f32)
        return [pltpu.SemaphoreType.DMA((4,)), pltpu.SemaphoreType.DMA((3,)), pltpu.SemaphoreType.DMA((3,)),
                rows, rows, rows, pltpu.VMEM((FF, 768), f32)]

    def bind(self, named, scr):
        sem_l, sem_s, sem_r, own, other, prod, inv_v = scr
        named[self.name + ":first"] = prod
        bits, peers = my_bits()
        core = bits[0]
        inv = named[self.name + ":inv"]
        copies, swaps = [], []
        for i, flow in enumerate(self.flows):
            rows = named.get(flow.part + ":out", named.get(flow.part + ":in"))
            spot = pl.ds(flow.shard_row, flow.kept(5))
            copies.append(pltpu.make_async_copy(rows, own.at[spot, :], sem_l.at[i]))
            swaps.append(pltpu.make_async_remote_copy(
                src_ref=rows, dst_ref=other.at[spot, :], send_sem=sem_s.at[i], recv_sem=sem_r.at[i],
                device_id=(peers[0],), device_id_type=MESH))
        copies.append(pltpu.make_async_copy(
            inv.at[self.block, :, pl.ds(pl.multiple_of(core * 768, 128), 768)], inv_v, sem_l.at[3]))

        def begin():
            for copy in copies + swaps:
                copy.start()

        def go(s):
            for copy in copies + swaps:
                copy.wait()
            prod[...] = (precise(own[...], inv_v[pl.ds(al(core * 768), 768), :])
                         + precise(other[...], inv_v[pl.ds(al((1 - core) * 768), 768), :]))

        return {"begin": begin, "go": go}


def plan(flows, firsts, tick_us, last, over=2.0):
    times = [0.0]
    for us in tick_us:
        times.append(times[-1] + us)
    limit = 1e9 if last else times[-1]
    free, now_rest = {}, times[-1]
    slots, rest = [[] for _ in tick_us], []
    ready = {f: f.start for f in flows}
    phase = {f: "new" for f in flows}
    for f in flows:
        f.a = f.b = f.at
    fstate = {f: "new" for f in firsts}
    fready = {}

    def arrival(f, s, now):
        links = LINKS[f.dim(s)]
        size = f.length(s) * f.cols * 4
        begin = max([now] + [free.get(link, 0.0) for link in links])
        return begin, max(begin + size / rate for rate in links.values()), size

    def send(f, s, now):
        begin, end, size = arrival(f, s, now)
        for link, rate in LINKS[f.dim(s)].items():
            free[link] = begin + size / rate
        f.b = s + 1
        ready[f] = end + LAG

    def allowed(f, s, now):
        return last or (now < limit and arrival(f, s, now)[1] + LAG < limit + over)

    def clear(f, s, now):
        return arrival(f, s, now)[0] <= now + SLACK

    def move(f, now):
        if ready[f] > now:
            return None
        if phase[f] == "new":
            if f.at >= LAST or f.wide and f.at == 5:
                return None
            if not allowed(f, f.at, now + (LAG if 0 < f.at <= 5 else 0.0)):
                return None
            if not clear(f, f.at, now):
                return None
            if f.at == 0:
                phase[f] = "run"
                send(f, 0, now)
                return "begin", 0
            if f.at <= 5:
                phase[f] = "loaded"
                ready[f] = now + LAG
                f.b = f.at + 1
                return "begin", 0
            phase[f] = "run"
            send(f, f.at, now)
            return "go", f.at
        if phase[f] == "loaded":
            phase[f] = "run"
            send(f, f.at, now)
            return "go", f.at
        if phase[f] == "run":
            s = f.b
            if s == LAST or f.wide and s == 5 or not allowed(f, s, now):
                phase[f] = "saved"
                ready[f] = now + LAG
                return "stop", s
            if not clear(f, s, now):
                return None
            send(f, s, now)
            return "go", s
        if phase[f] == "saved":
            phase[f] = "done"
            return "end", 0
        return None

    def first_move(f, now):
        if f.done or fready.get(f, 0.0) > now:
            return None
        if fstate[f] == "new":
            ok = all(x.b == 5 and phase.get(x, "done") in ("new", "done") for x in f.flows)
            if not ok or not (last or now + 20.0 < limit):
                return None
            fstate[f] = "loaded"
            fready[f] = now + 5.0
            return "begin", 0
        if fstate[f] == "loaded":
            fstate[f] = "done"
            return "go", 0
        return None

    def sweep(now, out):
        again = True
        while again:
            again = False
            for f in sorted(flows, key=PRIORITY):
                e = move(f, now)
                if e:
                    out.append((f,) + e)
                    again = True
                    break
            for f in firsts:
                e = first_move(f, now)
                if e:
                    out.append((f,) + e)
                    again = True
                    if fstate[f] == "done":
                        for x in f.fans:
                            flows.append(x)
                            x.a = 5
                            phase[x] = "run"
                            send(x, 5, now)
                            out.append((x, "go", 5))

    for t, now in enumerate(times[:-1]):
        sweep(now, slots[t])
    now = times[-1]
    while True:
        sweep(now, rest)
        later = [ready[f] for f in flows if phase[f] in ("loaded", "run", "saved") and ready[f] > now]
        later += [fready[f] for f in firsts if fstate[f] == "loaded" and fready[f] > now]
        held = any(phase[f] in ("loaded", "run") or last and phase[f] == "new" and f.at < LAST and not (f.wide and f.at == 5)
                   for f in flows)
        if not later and not held:
            return slots, rest, now
        now = min(later + ([now + 1.0] if held else []))


def tri_col(acc, mat, j):
    rows = (j + 1) * B
    off = B * j * (j + 1) // 2
    acc[off:off + rows, :] += mm(mat[:rows, :], mat[j * B:rows, :], NT)


def staged(dot, act, backs, shifts, accs, setup=None):
    step, last = pl.program_id(0), pl.num_programs(0) - 1

    def shift():
        for old, new in shifts:
            old[...] = new[...]

    @pl.when(step == 0)
    def _():
        for acc in accs:
            acc[...] = jnp.zeros_like(acc)
        if setup is not None:
            setup()
        for k in range(NB):
            act(k, dot(k))

    @pl.when((step > 0) & (step < last))
    def _():
        shift()
        for k, back in enumerate(backs):
            value = dot(k)
            back()
            act(k, value)

    @pl.when(step == last)
    def _():
        shift()
        for back in backs:
            back()


def plain(dot, act, backs, accs, setup):
    @pl.when(pl.program_id(0) == 0)
    def _():
        for acc in accs:
            acc[...] = jnp.zeros_like(acc)
        setup()

    for k in range(NB):
        act(k, dot(k))
    for back in backs:
        back()


def block(k):
    return slice(k * B, (k + 1) * B)


def tri_pieces(acc, mat, *more):
    pieces = [(5,), (4,), (3, 0), (2, 1)]

    def run(cols, fns):
        for j in cols:
            tri_col(acc, mat, j)
        for fn in fns:
            fn()

    return [functools.partial(run, cols, ()) for cols in pieces] + [functools.partial(run, (), fns) for fns in more]


def gelu_act(pre_out, new_s):
    def act(k, value):
        pre = value.astype(bf16)
        pre_out[block(k), :] = pre
        pre = pre.astype(f32)
        new_s[block(k), :] = (pre * half_sig(pre)[0]).astype(bf16)
    return act


def stage1(tok, grad, w_up, w_down, pre_out, next_out, tri, small_u, small_q, hid_s, up_s, down_s):
    def setup():
        up_s[...] = w_up[0].T
        down_s[...] = w_down[0].T

    def dot(k):
        return mm(up_s[block(k), :], tok[...], NT)

    def down():
        next_out[...] = mm(down_s[...], hid_s[...], NN).astype(bf16)

    def smalls():
        add_small_tn(small_u, tok)
        add_small_tn(small_q, grad)

    backs = [functools.partial(tri_col, tri, hid_s, j) for j in range(NB)] + [down, smalls]
    plain(dot, gelu_act(pre_out, hid_s), backs, (tri, small_u, small_q), setup)


def add_wide(acc, left, mat, dims, h):
    acc[h] += mm(left[...], mat[h * FF // 2:(h + 1) * FF // 2, :], dims)


def stage2(u_t, w_up, u_b, grad_b, pre_out, tri, small_u, dwd, new_s, hid_s, up_s):
    def setup():
        up_s[...] = w_up[0].T

    def dot(k):
        return mm(up_s[block(k), :], u_t[...], NN)

    wide = [functools.partial(add_wide, dwd, grad_b, hid_s, TT, h) for h in range(2)]
    backs = tri_pieces(tri, hid_s, wide[:1], (wide[1], lambda: add_small_nt(small_u, u_b)))
    staged(dot, gelu_act(pre_out, new_s), backs, ((hid_s, new_s),), (tri, small_u, dwd), setup)


def stage3(pre_in, grad, w_down, w_up, u_b, err_out, tri, dwu, new_s, g_s):
    def dot(k):
        return mm(w_down[0, block(k), :], grad[...], NT)

    def act(k, value):
        d_hid = value.astype(bf16).astype(f32)
        pre = pre_in[block(k), :].astype(f32)
        sig, cubic = half_sig(pre)
        new_s[block(k), :] = (d_hid * gelu_back(pre, sig, cubic)[1]).astype(bf16)

    def up():
        err_out[...] = mm(w_up[0], g_s[...], NN).astype(bf16)

    wide = [functools.partial(add_wide, dwu, u_b, g_s, NT, h) for h in range(2)]
    staged(dot, act, tri_pieces(tri, g_s, wide, (up,)), ((g_s, new_s),), (tri, dwu))


def stage4(pre_in, err_t, w_down, tok_b, err_b, g_out, small_q, dwd, dwu, new_h, hid_s, new_g, g_s):
    def dot(k):
        return mm(w_down[0, block(k), :], err_t[...], NN)

    def act(k, value):
        d_hid = value.astype(bf16).astype(f32)
        pre = pre_in[block(k), :].astype(f32)
        sig, cubic = half_sig(pre)
        hid, slope = gelu_back(pre, sig, cubic)
        new_h[block(k), :] = hid.astype(bf16)
        grad_up = (d_hid * slope).astype(bf16)
        new_g[block(k), :] = grad_up
        g_out[block(k), :] = grad_up

    def part(q, h):
        if q:
            dwd[h, :, :] += mm(err_b[...], hid_s[h * FF // 2:(h + 1) * FF // 2, :], NT)
        else:
            dwu[h, :, :] += mm(tok_b[...], g_s[h * FF // 2:(h + 1) * FF // 2, :], TT)

    backs = [functools.partial(part, q, h) for q in range(2) for h in range(2)]
    backs += [lambda: add_small_nt(small_q, err_b), lambda: None]
    staged(dot, act, backs, ((hid_s, new_h), (g_s, new_g)), (small_q, dwd, dwu))


def stage5(g_in, tri):
    zero_first((tri,))
    add_tri(tri, g_in)


SMALL = (2, 128, 384)
WIDE = (2, 384, 768)
TRI_SHAPE = (2, TRI // 2, B)
CUTS = {
    "ad0": "128X,1024X,512Y,512Z,512A", "au0": "128Z", "sd1": "128X",
    "ad1": "512X,128Y,512C,512Y,512A,512X", "au1": "128Z", "dwd1": "128X,256B",
    "su1": "512X,128X,512B,1024Y,512X", "dwu1": "256X,128C",
    "sd0": "128X", "dwd0": "128Z,256X", "dwu0": "256X,128B", "su0": "512C,512X,128Y,512B,512X,512Y",
}
FORMS = {"tri": TRI_SHAPE, "wide": WIDE, "small": SMALL}


def flows_of(name, form, cuts):
    flows, row = [], 0
    for cut in cuts.split(","):
        flows.append(Flow(name, row, int(cut[:-1]), FORMS[form][2], ORDERS[cut[-1]], row // 16, form == "wide"))
        row += flows[-1].rows
    return flows


def precise(left, right):
    return lax.dot_general(left, right, NN, precision=lax.Precision.HIGHEST, preferred_element_type=f32)


def thirds(x):
    parts = []
    for _ in range(3):
        parts.append(x.astype(bf16))
        x = x - parts[-1].astype(f32)
    return parts


def tile_spec(kind, shape, tile):
    n = shape[0 if kind[0] == "r" else 1] // tile

    def at(i):
        if "b" in kind:
            return jnp.maximum(i - 1, 0)
        return jnp.minimum(i, n - 1) if "f" in kind else i

    if kind[0] == "r":
        return pl.BlockSpec((tile, D), lambda i: (at(i), 0))
    return pl.BlockSpec((shape[0], tile), lambda i: (0, at(i)))


def whole_spec(shape):
    zeros = (0,) * len(shape)
    return pl.BlockSpec(shape, lambda i: zeros, pipeline_mode=pl.Buffered(1))


def block_spec(shape, b):
    return pl.BlockSpec((1,) + shape[1:], lambda i: (b, 0, 0), pipeline_mode=pl.Buffered(1))


ANY = pl.BlockSpec(memory_space=pl.ANY)
SCALARS = pl.BlockSpec(memory_space=pltpu.SMEM)


class Board:
    def __init__(self):
        self.flows, self.firsts, self.arrays, self.forms, self.fresh = [], [], {}, {}, 0

    def add(self, name, form, cuts, array, other=None, block=0):
        flows = flows_of(name, form, cuts)
        self.flows += flows
        self.forms[name] = FORMS[form]
        self.arrays[name + ":src"] = array.reshape(self.forms[name])
        if form == "wide":
            self.firsts.append(First(name, flows, other, block))
            self.arrays[name + ":inv"] = other
        elif form == "tri":
            for f in flows:
                f.old = (block, TRI // 2)
            self.arrays[name + ":old"] = other

    def plan(self, tick_us, last):
        for f in self.flows:
            f.at = f.b if hasattr(f, "b") else f.at
        flows = [f for f in self.flows if f.at < LAST and not (f.wide and f.at == 5)]
        idle = [f for f in self.flows if f.wide and f.at == 5]
        for f in idle:
            f.a = f.b = f.at
        slots, rest, end = plan(flows, self.firsts, tick_us, last)
        runs = [f for f in self.firsts if f.fans[0] in flows]
        self.firsts = [f for f in self.firsts if f not in runs]
        self.flows = [f for f in flows + idle if f.b < LAST or f.a < f.b]
        moving = [f for f in flows if f.a < f.b]
        ins, outs = [], {}
        for f in moving:
            if f.a == 0:
                ins.append(f.name + ":src")
            elif f.a < 5 or (f.a == 5 and not f.wide):
                ins.append(f.part + ":in")
            if f.mixes():
                ins += ["decay", f.name + ":old"]
            if f.b <= 5:
                outs[f.part + ":out"] = (f.kept(f.b), f.cols)
            else:
                outs[f.name + ":dst"] = self.forms[f.name]
        for first in runs:
            ins.append(first.name + ":inv")
            ins += [f.part + ":in" for f in first.flows if f.part + ":out" not in outs]
        ins += [name for name in outs if name in self.arrays]
        return slots, rest, end, moving, runs, list(dict.fromkeys(ins)), outs

    def keep(self, outs, values):
        for name, value in zip(outs, values):
            self.arrays[name.replace(":out", ":in")] = value


def run_stage(board, body, name, tile, tick_us, ins, outs, scratch, flops, cid, last=False):
    def spec(kind, shape):
        if kind == "w":
            return whole_spec(shape)
        return block_spec(shape, kind) if isinstance(kind, int) else tile_spec(kind, shape, tile)

    steps = len(tick_us)
    slots, rest, end, moving, runs, m_ins, m_outs = board.plan(tick_us, last)
    scr = [job.open(job.a, job.b) if isinstance(job, Flow) else job.open() for job in runs + moving]
    n_in, n_min, n_out, n_mout, n_scr = len(ins), len(m_ins), len(outs), len(m_outs), len(scratch)

    def kernel(*refs):
        refs = list(refs)

        def pull(n):
            return [refs.pop(0) for _ in range(n)]

        c_in, m_in, c_out, m_out, c_scr = pull(n_in), pull(n_min), pull(n_out), pull(n_mout), pull(n_scr)
        named = dict(zip(m_ins, m_in))
        named.update(zip(m_outs, m_out))
        step = pl.program_id(0)
        events = {}
        if moving:
            pl.when(step == 0)(entry_barrier)
        for job, s in zip(runs + moving, scr):
            events[job] = job.bind(named, pull(len(s)))

        def fire(slot):
            for job, what, s in slot:
                if what in ("go", "stop"):
                    events[job][what](s)
                else:
                    events[job][what]()

        for t in range(steps):
            if slots[t]:
                pl.when(step == t)(functools.partial(fire, slots[t]))
        if body is not None:
            body(*c_in, *c_out, *c_scr)
        if rest:
            pl.when(step == steps - 1)(functools.partial(fire, rest))

    params = dict(vmem_limit_bytes=63 * MIB)
    if moving:
        params.update(collective_id=cid, has_side_effects=True)
    values = pl.pallas_call(
        kernel, grid=(steps,),
        in_specs=[spec(kind, arr.shape) for arr, kind in ins] + [SCALARS if m == "decay" else ANY for m in m_ins],
        out_specs=[spec(kind, shape) for shape, dtype, kind in outs] + [ANY] * n_mout,
        out_shape=[jax.ShapeDtypeStruct(shape, dtype) for shape, dtype, kind in outs]
        + [jax.ShapeDtypeStruct(shape, f32) for shape in m_outs.values()],
        scratch_shapes=list(scratch) + [x for s in scr for x in s],
        input_output_aliases={n_in + m_ins.index(m): n_out + i for i, m in enumerate(m_outs) if m in m_ins},
        compiler_params=pltpu.CompilerParams(**params),
        cost_estimate=pl.CostEstimate(flops=flops, bytes_accessed=40 * MIB, transcendentals=0),
        name=name)(*[arr for arr, _ in ins], *[board.arrays[m] for m in m_ins])
    board.keep(m_outs, values[n_out:])
    return values[:n_out]


def final_kernel(decay, t0, t1, t2, t3, n0, n1, n2, n3, s0, s1, s2, s3, old_u, old_q, inv_u, inv_q,
                 new_s, new_a, p_up, p_down, new_u, new_q, pk, tr, nv, pv, pt, inv_s, sem_in, sem_out):
    rho = decay[0]
    scale = (1.0 - rho) * decay[1]
    deep = pk.shape[0]
    ahead = deep // 2
    units = []
    for q, (src, new, n) in enumerate(((t0, new_a, n0), (t1, new_a, n1), (t2, new_s, n2), (t3, new_s, n3))):
        off = 0
        for j in range(NB):
            units.append((q, src, new, q % 2, j, off, n))
            off += (j + 1) * B

    def loads(u):
        q, src, new, b, j, off, n = units[u]
        rows, s = (j + 1) * B, u % deep
        parts = ((src.at[pl.ds(off, rows), :], pk.at[s, pl.ds(0, rows), :]),
                 (n.at[j // 3, :, pl.ds(j % 3 * B, B)], nv.at[s]))
        return [pltpu.make_async_copy(x, y, sem_in.at[s, i]) for i, (x, y) in enumerate(parts)]

    def stores(u):
        q, src, new, b, j, off, n = units[u]
        rows, s = (j + 1) * B, u % deep
        parts = [(pk.at[s, pl.ds(0, rows), :], new.at[b, pl.ds(0, rows), pl.ds(j * B, B)])]
        if q < 2:
            parts.append((pv.at[s], p_up.at[b, :, pl.ds(j * B, B)]))
        else:
            parts.append((pt.at[s], p_down.at[b, pl.ds(j * B, B), :]))
        if j:
            parts.append((tr.at[s, :, pl.ds(0, j * B)], new.at[b, pl.ds(j * B, B), pl.ds(0, j * B)]))
        return [pltpu.make_async_copy(x, y, sem_out.at[s, i]) for i, (x, y) in enumerate(parts)]

    for u in range(ahead):
        for c in loads(u):
            c.start()
    h = B // 2
    for acc, old, new, b in ((s0, old_u, new_u, 0), (s1, old_u, new_u, 1), (s2, old_q, new_q, 0), (s3, old_q, new_q, 1)):
        top = rho * old[b, :h, :] + scale * acc[0]
        mid = rho * old[b, h:B, h:] + scale * acc[1, :, :B]
        low = rho * old[b, B:, B:] + scale * acc[1, :, B:]
        new[b, :h, :] = top
        new[b, h:B, h:] = mid
        new[b, B:, B:] = low
        new[b, h:, :h] = top[:, h:].T
        new[b, B:, h:B] = mid[:, h:].T
    for u, (q, src, new, b, j, off, n) in enumerate(units):
        s = u % deep
        for c in loads(u):
            c.wait()
        for i in range(j):
            here = slice(i * B, (i + 1) * B)
            tr[s, :, here] = pk[s, here, :].T
        if j == 0:
            x, y, z = thirds((inv_u if q < 2 else inv_q)[b])
            for i, third in enumerate((x, x, y, x, y, z)):
                inv_s[:, i * D:(i + 1) * D] = third
        x, y, z = thirds(nv[s])
        prod = mm(inv_s[...], jnp.concatenate((x, y, x, z, y, x), axis=0), NN) * decay[1]
        if q < 2:
            pv[s] = prod
        else:
            pt[s] = prod.T
        for c in stores(u):
            c.start()
        if u + ahead < len(units):
            if u + ahead >= deep:
                for c in stores(u + ahead - deep):
                    c.wait()
            for c in loads(u + ahead):
                c.start()
    for u in range(len(units) - deep, len(units)):
        for c in stores(u):
            c.wait()


def finish(decay, tris, smalls, prods, s_up_old, a_up_old, s_down_old, inv_u, inv_q):
    vmem = pl.BlockSpec(memory_space=pltpu.VMEM)
    big = jax.ShapeDtypeStruct(s_up_old.shape, f32)
    small = jax.ShapeDtypeStruct(a_up_old.shape, f32)
    deep = 6
    return pl.pallas_call(
        final_kernel,
        in_specs=[SCALARS] + [ANY] * 8 + [vmem] * 8,
        out_specs=[ANY] * 4 + [vmem] * 2,
        out_shape=[big, big, jax.ShapeDtypeStruct((2, D, FF), f32), jax.ShapeDtypeStruct((2, FF, D), f32), small, small],
        scratch_shapes=[pltpu.VMEM((deep, FF, B), f32), pltpu.VMEM((deep, B, FF), f32)]
        + [pltpu.VMEM((deep, D, B), f32)] * 2 + [pltpu.VMEM((deep, B, D), f32), pltpu.VMEM((D, 6 * D), bf16)]
        + [pltpu.SemaphoreType.DMA((deep, 3))] * 2,
        compiler_params=pltpu.CompilerParams(vmem_limit_bytes=63 * MIB),
        name="finish")(decay, *[t.reshape(TRI, B) for t in tris], *prods, *smalls, a_up_old, s_down_old, inv_u, inv_q)


def solution(mesh):
    axis_size = mesh.shape["data"]
    tile = 512

    def local_step(tok, grad, w_up, w_down, a_up_old, s_up_old, a_down_old, s_down_old,
                   a_up_inv, s_up_inv, a_down_inv, s_down_inv, factor_decay):
        total = tok.shape[0]
        steps = total // tile
        inv_n = 1.0 / (total * axis_size)
        acts = [pltpu.VMEM((FF, tile), bf16)] * 2
        w_t = pltpu.VMEM((FF, D), bf16)
        unit = 2 * total * FF * D
        wide_out, small_out, tri_out = (WIDE, f32, "w"), (SMALL, f32, "w"), ((TRI, B), f32, "w")
        long_out, short_out = ((FF, total), bf16, "cf"), ((D, total), bf16, "cb")
        board = Board()
        decay = jnp.stack((factor_decay, jnp.float32(inv_n)))
        board.arrays["decay"] = decay
        pre0, u1, ad0, au0, sd1 = run_stage(
            board, stage1, "stage1", 2 * tile, [0.0] * (steps // 2),
            ((tok, "r"), (grad, "r"), (w_up, 0), (w_down, 0)),
            (long_out, ((D, total), bf16, "c"), tri_out, small_out, small_out),
            [pltpu.VMEM((FF, 2 * tile), bf16), w_t, pltpu.VMEM((D, FF), bf16)], 5 * unit, 0)
        board.add("ad0", "tri", CUTS["ad0"], ad0, a_down_old, 0)
        board.add("au0", "small", CUTS["au0"], au0)
        board.add("sd1", "small", CUTS["sd1"], sd1)
        pre1, ad1, au1, dwd1 = run_stage(
            board, stage2, "stage2", tile, [2.2] + [3.47] * steps, ((u1, "cf"), (w_up, 1), (u1, "cb"), (grad, "rb")),
            (long_out, tri_out, small_out, wide_out), acts + [w_t], 5 * unit, 1)
        board.add("ad1", "tri", CUTS["ad1"], ad1, a_down_old, 1)
        board.add("au1", "small", CUTS["au1"], au1)
        board.add("dwd1", "wide", CUTS["dwd1"], dwd1, a_down_inv, 1)
        e1, su1, dwu1 = run_stage(
            board, stage3, "stage3", tile, [2.4] + [4.4] * steps,
            ((pre1, "cf"), (grad, "rf"), (w_down, 1), (w_up, 1), (u1, "cb")), (short_out, tri_out, wide_out), acts, 6 * unit, 2)
        board.add("su1", "tri", CUTS["su1"], su1, s_up_old, 1)
        board.add("dwu1", "wide", CUTS["dwu1"], dwu1, s_up_inv, 1)
        g0, sd0, dwd0, dwu0 = run_stage(
            board, stage4, "stage4", tile, [2.2] + [3.2] * steps,
            ((pre0, "cf"), (e1, "cf"), (w_down, 0), (tok, "rb"), (e1, "cb")),
            (long_out, small_out, wide_out, wide_out), acts * 2, 4 * unit, 3)
        board.add("sd0", "small", CUTS["sd0"], sd0)
        board.add("dwd0", "wide", CUTS["dwd0"], dwd0, a_down_inv, 0)
        board.add("dwu0", "wide", CUTS["dwu0"], dwu0, s_up_inv, 0)
        su0, = run_stage(board, stage5, "stage5", tile, [1.84] * steps, ((g0, "c"),), (tri_out,), [], 3 * unit, 4)
        board.add("su0", "tri", CUTS["su0"], su0, s_up_old, 0)
        run_stage(board, None, "tail", tile, [0.1], (), (), [], unit, 5, last=True)
        done = board.arrays
        new_s, new_a, p_up, p_down, new_u, new_q = finish(
            decay, [done[n + ":dst"] for n in ("ad0", "ad1", "su0", "su1")],
            [done[n + ":dst"] for n in ("au0", "au1", "sd0", "sd1")],
            [done[n + ":dst"] for n in ("dwu0", "dwu1", "dwd0", "dwd1")],
            s_up_old, a_up_old, s_down_old, a_up_inv, s_down_inv)
        return p_up, p_down, new_u, new_s, new_a, new_q

    batch_spec = P("data", None)
    replicated = P()
    return jax.shard_map(local_step, mesh=mesh, in_specs=(batch_spec, batch_spec) + (replicated,) * 11,
                         out_specs=(replicated,) * 6, check_vma=False)
```

```python
import functools

import jax
import jax.numpy as jnp
from jax import lax
from jax.experimental import pallas as pl
from jax.experimental.pallas import tpu as pltpu
from jax.sharding import PartitionSpec as P

bf16 = jnp.bfloat16
f32 = jnp.float32
D, FF, B = 384, 1536, 256
NB = FF // B
TRI = sum((j + 1) * B for j in range(NB))
NN = (((1,), (0,)), ((), ()))
NT = (((1,), (1,)), ((), ()))
TN = (((0,), (0,)), ((), ()))
TT = (((0,), (1,)), ((), ()))
GELU_K = 0.7978845608028654
GELU_C = 0.044715 * GELU_K
MIB = 1 << 20


def mm(left, right, dims):
    return lax.dot_general(left, right, dims, preferred_element_type=f32)


def half_sig(pre):
    cubic = GELU_C * (pre * pre)
    return 0.5 * jnp.tanh(pre * (cubic + GELU_K)) + 0.5, cubic


def gelu_back(pre, sig, cubic):
    hid = pre * sig
    return hid, sig + (hid * (1.0 - sig)) * (6.0 * cubic + 2.0 * GELU_K)


def add_tri(acc, mat):
    off = 0
    for j in range(NB):
        rows = (j + 1) * B
        acc[off:off + rows, :] += mm(mat[:rows, :], mat[j * B:rows, :], NT)
        off += rows


def add_small_tn(acc, rows):
    acc[0] += mm(rows[:, 0:128], rows[...], TN)
    acc[1, :, 0:256] += mm(rows[:, 128:256], rows[:, 128:384], TN)
    acc[1, :, 256:384] += mm(rows[:, 256:384], rows[:, 256:384], TN)


def add_small_nt(acc, cols):
    acc[0] += mm(cols[0:128, :], cols[...], NT)
    acc[1, :, 0:256] += mm(cols[128:256, :], cols[128:384, :], NT)
    acc[1, :, 256:384] += mm(cols[256:384, :], cols[256:384, :], NT)


def zero_first(accs):
    @pl.when(pl.program_id(0) == 0)
    def _():
        for acc in accs:
            acc[...] = jnp.zeros_like(acc)


MESH = pl.DeviceIdType.MESH
ORDERS = {key: tuple(map(int, order)) for key, order in
          (("X", "1234"), ("Y", "2134"), ("Z", "3412"), ("A", "1342"), ("B", "2341"), ("C", "3421"))}
LINKS = {0: {0: 6e5}, 1: {1: 45e3}, 2: {2: 45e3}, 3: {3: 45e3}, 4: {3: 45e3, 4: 23e3}}
LAG = 1.5
SLACK = 3.0


def PRIORITY(f):
    return f.b


LAST = 10


def my_bits():
    me = lax.axis_index("data")
    bits = [(me // (1 << d)) % 2 for d in range(5)]
    return bits, [me + (1 - 2 * bits[d]) * (1 << d) for d in range(5)]


def enter():
    for peer in my_bits()[1]:
        pl.semaphore_signal(pltpu.get_barrier_semaphore(), inc=1, device_id=(peer,), device_id_type=MESH)


def await_peers():
    pl.semaphore_wait(pltpu.get_barrier_semaphore(), 5)


def al(row):
    return pl.multiple_of(row, 8)


class Flow:
    def __init__(self, name, row0, rows, cols, order, shard_row, wide):
        self.name, self.row0, self.rows, self.cols, self.order = name, row0, rows, cols, order
        self.shard_row, self.wide, self.old = shard_row, wide, None
        self.at, self.start = 0, 0.0
        self.part = name + ":part%d" % row0

    def fan(self):
        other = Flow(self.name, self.row0, self.rows, self.cols, self.order, self.shard_row, True)
        other.at = 5
        return other

    def dim(self, s):
        if s in (0, LAST - 1):
            return 0
        return self.order[s - 1] if s < 5 else self.order[LAST - 2 - s]

    def length(self, s):
        return self.rows >> s if s < 5 else self.rows >> (LAST - 1 - s)

    def kept(self, steps):
        return self.rows >> (steps - 1)

    def open(self, a, b):
        self.a, self.b = a, b
        n = b - a
        out = [pltpu.SemaphoreType.DMA((3,)), pltpu.SemaphoreType.DMA((n,)), pltpu.SemaphoreType.DMA((n,))]
        if a < 5:
            out.append(pltpu.VMEM((self.rows if a == 0 else self.kept(a), self.cols), f32))
            out.append(pltpu.VMEM((sum(self.length(s) for s in range(a, min(b, 5))), self.cols), f32))
            if self.mixes():
                out.append(pltpu.VMEM((self.kept(5), self.cols), f32))
        elif a == 5 and not self.wide:
            out.append(pltpu.VMEM((self.kept(5), self.cols), f32))
        return out

    def mixes(self):
        return self.old is not None and self.a < 5 <= self.b

    def bind(self, named, scr):
        a, b, row0, rows = self.a, self.b, self.row0, self.rows
        sem_l, sem_s, sem_r = scr[:3]
        bits, peers = my_bits()
        core = bits[0]
        lens, offs = [rows], [0]
        for d in self.order:
            lens.append(lens[-1] // 2)
            offs.append(offs[-1] + bits[d] * lens[-1])
        src, dst = named.get(self.name + ":src"), named.get(self.name + ":dst")
        part_in, part_out = named.get(self.part + ":in"), named.get(self.part + ":out")
        base = offs[min(max(a, 1), 5) - 1]
        work = recv = None
        if a < 5:
            work, recv = scr[3:5]
        elif a == 5:
            work = named[self.name + ":first"].at[pl.ds(self.shard_row, self.kept(5)), :] if self.wide else scr[3]
        sends, begin_recv, locals_ = {}, {}, []

        def remote(s, x, y):
            return pltpu.make_async_remote_copy(src_ref=x, dst_ref=y, send_sem=sem_s.at[s - a], recv_sem=sem_r.at[s - a],
                                                device_id=(peers[self.dim(s)],), device_id_type=MESH)

        def final():
            return work if a == 5 else work.at[pl.ds(al(offs[4] - base), lens[4]), :]

        def spot(k):
            return dst.at[core, pl.ds(al(row0 + offs[k]), lens[k]), :]

        at = 0
        for s in range(a, b):
            if s < 5:
                begin_recv[s] = at
                to = recv.at[pl.ds(at, self.length(s)), :]
                at += self.length(s)
                if s == 0:
                    sends[s] = remote(s, src.at[1 - core, pl.ds(row0, rows), :], to)
                else:
                    gone = al(offs[s - 1] - base + (1 - bits[self.dim(s)]) * lens[s])
                    sends[s] = remote(s, work.at[pl.ds(gone, lens[s]), :], to)
            else:
                k = LAST - 1 - s
                sends[s] = remote(s, final() if s == 5 else spot(k), spot(k))
        load = place = save = old = None
        if self.mixes():
            old_array, half = self.old
            spot4 = core * half + row0 + offs[4]
            j = sum((spot4 // (B // 2 * m * (m + 1)) + 31) // 32 for m in range(1, NB))
            old = pltpu.make_async_copy(
                named[self.name + ":old"].at[old_array, pl.ds(al(spot4 - B // 2 * j * (j + 1)), lens[4]),
                                             pl.ds(pl.multiple_of(j * B, B), B)], scr[5], sem_l.at[2])
        if a == 0:
            load = pltpu.make_async_copy(src.at[core, pl.ds(row0, rows), :], work, sem_l.at[0])
        elif a < 5 or (a == 5 and not self.wide):
            load = pltpu.make_async_copy(part_in, work, sem_l.at[0])
        if a <= 5 < b:
            place = pltpu.make_async_copy(final(), spot(4), sem_l.at[1])
        if b <= 5:
            kept = work.at[pl.ds(al(offs[b - 1] - base), lens[b - 1]), :]
            save = pltpu.make_async_copy(kept, part_out, sem_l.at[1])

        def add(row, frm, count):
            for q in range(0, count, 64):
                step = min(count - q, 64)
                x, y = al(row + q), al(frm + q)
                work[pl.ds(x, step), :] = work[pl.ds(x, step), :] + recv[pl.ds(y, step), :]

        def mix():
            rho = named["decay"][0]
            x, y = pl.ds(al(offs[4] - base), lens[4]), pl.ds(begin_recv[4], lens[4])
            total = (work[x, :] + recv[y, :]) * named["decay"][1]
            work[x, :] = rho * scr[5][...] + (1.0 - rho) * total

        def take(s, then):
            if s == a and load is not None and a == 0:
                load.wait()
            sends[s].wait_recv()
            if s == 5 and place is not None:
                place.wait()
            if s >= 5:
                then()
            elif s == 4 and old is not None:
                old.wait()
                mix()
                then()
            elif s == 4 or s + 1 == b:
                add(offs[s] - base, begin_recv[s], lens[s])
                then()
            else:
                half = lens[s + 1]
                bit = bits[self.dim(s + 1)]
                add(offs[s] - base + (1 - bit) * half, begin_recv[s] + (1 - bit) * half, half)
                then()
                add(offs[s] - base + bit * half, begin_recv[s] + bit * half, half)

        def send(s):
            if s == 5:
                place.start()
            sends[s].start()

        def begin():
            load.start()
            if old is not None:
                old.start()
            if a == 0:
                send(0)

        def go(s):
            if s > a:
                take(s - 1, lambda: send(s))
            else:
                if load is not None:
                    load.wait()
                send(s)

        def stop():
            take(b - 1, save.start if save is not None else lambda: None)

        def end():
            if save is not None:
                save.wait()
            for s in range(a, b):
                sends[s].wait_send()

        return {"begin": begin, "go": go, "stop": lambda s: stop(), "end": end}


class First:
    def __init__(self, name, flows, inverse, block):
        self.name, self.flows, self.inverse, self.block, self.done = name, flows, inverse, block, False
        self.fans = [f.fan() for f in flows]

    def open(self):
        rows = pltpu.VMEM((24, 768), f32)
        return [pltpu.SemaphoreType.DMA((4,)), pltpu.SemaphoreType.DMA((3,)), pltpu.SemaphoreType.DMA((3,)),
                rows, rows, rows, pltpu.VMEM((FF, 768), f32)]

    def bind(self, named, scr):
        sem_l, sem_s, sem_r, own, other, prod, inv_v = scr
        named[self.name + ":first"] = prod
        bits, peers = my_bits()
        core = bits[0]
        inv = named[self.name + ":inv"]
        copies, swaps = [], []
        for i, flow in enumerate(self.flows):
            rows = named.get(flow.part + ":out", named.get(flow.part + ":in"))
            spot = pl.ds(flow.shard_row, flow.kept(5))
            copies.append(pltpu.make_async_copy(rows, own.at[spot, :], sem_l.at[i]))
            swaps.append(pltpu.make_async_remote_copy(
                src_ref=rows, dst_ref=other.at[spot, :], send_sem=sem_s.at[i], recv_sem=sem_r.at[i],
                device_id=(peers[0],), device_id_type=MESH))
        copies.append(pltpu.make_async_copy(
            inv.at[self.block, :, pl.ds(pl.multiple_of(core * 768, 128), 768)], inv_v, sem_l.at[3]))

        def begin():
            for copy in copies + swaps:
                copy.start()

        def go(s):
            for copy in copies + swaps:
                copy.wait()
            prod[...] = (precise(own[...], inv_v[pl.ds(al(core * 768), 768), :])
                         + precise(other[...], inv_v[pl.ds(al((1 - core) * 768), 768), :]))

        return {"begin": begin, "go": go}


def plan(flows, firsts, tick_us, last, over=2.0):
    times = [0.0]
    for us in tick_us:
        times.append(times[-1] + us)
    limit = 1e9 if last else times[-1]
    free, now_rest = {}, times[-1]
    slots, rest = [[] for _ in tick_us], []
    ready = {f: f.start for f in flows}
    phase = {f: "new" for f in flows}
    for f in flows:
        f.a = f.b = f.at
    fstate = {f: "new" for f in firsts}
    fready = {}

    def arrival(f, s, now):
        links = LINKS[f.dim(s)]
        size = f.length(s) * f.cols * 4
        begin = max([now] + [free.get(link, 0.0) for link in links])
        return begin, max(begin + size / rate for rate in links.values()), size

    def send(f, s, now):
        begin, end, size = arrival(f, s, now)
        for link, rate in LINKS[f.dim(s)].items():
            free[link] = begin + size / rate
        f.b = s + 1
        ready[f] = end + LAG

    def allowed(f, s, now):
        return last or (now < limit and arrival(f, s, now)[1] + LAG < limit + over)

    def clear(f, s, now):
        return arrival(f, s, now)[0] <= now + SLACK

    def move(f, now):
        if ready[f] > now:
            return None
        if phase[f] == "new":
            if f.at >= LAST or f.wide and f.at == 5:
                return None
            if not allowed(f, f.at, now + (LAG if 0 < f.at <= 5 else 0.0)):
                return None
            if not clear(f, f.at, now):
                return None
            if f.at == 0:
                phase[f] = "run"
                send(f, 0, now)
                return "begin", 0
            if f.at <= 5:
                phase[f] = "loaded"
                ready[f] = now + LAG
                f.b = f.at + 1
                return "begin", 0
            phase[f] = "run"
            send(f, f.at, now)
            return "go", f.at
        if phase[f] == "loaded":
            phase[f] = "run"
            send(f, f.at, now)
            return "go", f.at
        if phase[f] == "run":
            s = f.b
            if s == LAST or f.wide and s == 5 or not allowed(f, s, now):
                phase[f] = "saved"
                ready[f] = now + LAG
                return "stop", s
            if not clear(f, s, now):
                return None
            send(f, s, now)
            return "go", s
        if phase[f] == "saved":
            phase[f] = "done"
            return "end", 0
        return None

    def first_move(f, now):
        if f.done or fready.get(f, 0.0) > now:
            return None
        if fstate[f] == "new":
            ok = all(x.b == 5 and phase.get(x, "done") in ("new", "done") for x in f.flows)
            if not ok or not (last or now + 20.0 < limit):
                return None
            fstate[f] = "loaded"
            fready[f] = now + 5.0
            return "begin", 0
        if fstate[f] == "loaded":
            fstate[f] = "done"
            return "go", 0
        return None

    def sweep(now, out):
        again = True
        while again:
            again = False
            for f in sorted(flows, key=PRIORITY):
                e = move(f, now)
                if e:
                    out.append((f,) + e)
                    again = True
                    break
            for f in firsts:
                e = first_move(f, now)
                if e:
                    out.append((f,) + e)
                    again = True
                    if fstate[f] == "done":
                        for x in f.fans:
                            flows.append(x)
                            x.a = 5
                            phase[x] = "run"
                            send(x, 5, now)
                            out.append((x, "go", 5))

    for t, now in enumerate(times[:-1]):
        if t or last:
            sweep(now, slots[t])
    now = times[-1]
    while True:
        sweep(now, rest)
        later = [ready[f] for f in flows if phase[f] in ("loaded", "run", "saved") and ready[f] > now]
        later += [fready[f] for f in firsts if fstate[f] == "loaded" and fready[f] > now]
        held = any(phase[f] in ("loaded", "run") or last and phase[f] == "new" and f.at < LAST and not (f.wide and f.at == 5)
                   for f in flows)
        if not later and not held:
            return slots, rest, now
        now = min(later + ([now + 1.0] if held else []))


def tri_col(acc, mat, j):
    rows = (j + 1) * B
    off = B * j * (j + 1) // 2
    acc[off:off + rows, :] += mm(mat[:rows, :], mat[j * B:rows, :], NT)


def staged(dot, act, backs, shifts, accs, setup=None):
    step, last = pl.program_id(0), pl.num_programs(0) - 1

    def shift():
        for old, new in shifts:
            old[...] = new[...]

    @pl.when(step == 0)
    def _():
        for acc in accs:
            acc[...] = jnp.zeros_like(acc)
        if setup is not None:
            setup()
        for k in range(NB):
            act(k, dot(k))

    @pl.when((step > 0) & (step < last))
    def _():
        shift()
        for k, back in enumerate(backs):
            value = dot(k)
            back()
            act(k, value)

    @pl.when(step == last)
    def _():
        shift()
        for back in backs:
            back()


def plain(dot, act, backs, accs, setup):
    @pl.when(pl.program_id(0) == 0)
    def _():
        for acc in accs:
            acc[...] = jnp.zeros_like(acc)
        setup()

    for k in range(NB):
        act(k, dot(k))
    for back in backs:
        back()


def block(k):
    return slice(k * B, (k + 1) * B)


def tri_pieces(acc, mat, *more):
    pieces = [(5,), (4,), (3, 0), (2, 1)]

    def run(cols, fns):
        for j in cols:
            tri_col(acc, mat, j)
        for fn in fns:
            fn()

    return [functools.partial(run, cols, ()) for cols in pieces] + [functools.partial(run, (), fns) for fns in more]


def gelu_act(pre_out, new_s):
    def act(k, value):
        pre = value.astype(bf16)
        pre_out[block(k), :] = pre
        pre = pre.astype(f32)
        new_s[block(k), :] = (pre * half_sig(pre)[0]).astype(bf16)
    return act


def stage1(tok, grad, w_up, w_down, pre_out, next_out, tri, small_u, small_q, hid_s, up_s, down_s):
    def setup():
        up_s[...] = w_up[0].T
        down_s[...] = w_down[0].T

    def dot(k):
        return mm(up_s[block(k), :], tok[...], NT)

    def down():
        next_out[...] = mm(down_s[...], hid_s[...], NN).astype(bf16)

    def smalls():
        add_small_tn(small_u, tok)
        add_small_tn(small_q, grad)

    backs = [functools.partial(tri_col, tri, hid_s, j) for j in range(NB)] + [down, smalls]
    plain(dot, gelu_act(pre_out, hid_s), backs, (tri, small_u, small_q), setup)


def add_wide(acc, left, mat, dims, h):
    acc[h] += mm(left[...], mat[h * FF // 2:(h + 1) * FF // 2, :], dims)


def stage2(u_t, w_up, u_b, grad_b, pre_out, tri, small_u, dwd, new_s, hid_s, up_s):
    def setup():
        up_s[...] = w_up[0].T

    def dot(k):
        return mm(up_s[block(k), :], u_t[...], NN)

    wide = [functools.partial(add_wide, dwd, grad_b, hid_s, TT, h) for h in PAIR]
    backs = tri_pieces(tri, hid_s, wide[:1], (wide[1], lambda: add_small_nt(small_u, u_b)))
    staged(dot, gelu_act(pre_out, new_s), backs, ((hid_s, new_s),), (tri, small_u, dwd), setup)


def stage3(pre_in, grad, w_down, w_up, u_b, err_out, tri, dwu, new_s, g_s):
    def dot(k):
        return mm(w_down[0, block(k), :], grad[...], NT)

    def act(k, value):
        d_hid = value.astype(bf16).astype(f32)
        pre = pre_in[block(k), :].astype(f32)
        sig, cubic = half_sig(pre)
        new_s[block(k), :] = (d_hid * gelu_back(pre, sig, cubic)[1]).astype(bf16)

    def up():
        err_out[...] = mm(w_up[0], g_s[...], NN).astype(bf16)

    wide = [functools.partial(add_wide, dwu, u_b, g_s, NT, h) for h in PAIR]
    staged(dot, act, tri_pieces(tri, g_s, wide, (up,)), ((g_s, new_s),), (tri, dwu))


def stage4(pre_in, err_t, w_down, tok_b, err_b, g_out, small_q, dwd, dwu, new_h, hid_s, new_g, g_s):
    def dot(k):
        return mm(w_down[0, block(k), :], err_t[...], NN)

    def act(k, value):
        d_hid = value.astype(bf16).astype(f32)
        pre = pre_in[block(k), :].astype(f32)
        sig, cubic = half_sig(pre)
        hid, slope = gelu_back(pre, sig, cubic)
        new_h[block(k), :] = hid.astype(bf16)
        grad_up = (d_hid * slope).astype(bf16)
        new_g[block(k), :] = grad_up
        g_out[block(k), :] = grad_up

    def part(q, h):
        if q:
            dwd[h, :, :] += mm(err_b[...], hid_s[h * FF // 2:(h + 1) * FF // 2, :], NT)
        else:
            dwu[h, :, :] += mm(tok_b[...], g_s[h * FF // 2:(h + 1) * FF // 2, :], TT)

    backs = [functools.partial(part, q, h) for q in PAIR for h in PAIR]
    backs += [lambda: add_small_nt(small_q, err_b), lambda: None]
    staged(dot, act, backs, ((hid_s, new_h), (g_s, new_g)), (small_q, dwd, dwu))


def stage5(g_in, tri):
    zero_first((tri,))
    add_tri(tri, g_in)


SMALL = (2, 128, 384)
WIDE = (2, 384, 768)
TRI_SHAPE = (2, TRI // 2, B)
CUTS = {
    "ad0": "512Z,512A,128C,1024A,512X", "au0": "128X", "sd1": "128Y",
    "ad1": "128X,1024Y,512C,1024X", "au1": "128Z", "dwd1": "384Y",
    "su1": "512C,512X,128X,512X,512X,512Y", "dwu1": "128Y,256X",
    "sd0": "128Z", "dwd0": "128B,256X", "dwu0": "256Y,128C", "su0": "128X,512X,512X,512C,512X,512B",
}
FORMS = {"tri": TRI_SHAPE, "wide": WIDE, "small": SMALL}


def flows_of(name, form, cuts):
    flows, row = [], 0
    for cut in cuts.split(","):
        flows.append(Flow(name, row, int(cut[:-1]), FORMS[form][2], ORDERS[cut[-1]], row // 16, form == "wide"))
        row += flows[-1].rows
    return flows


def precise(left, right):
    return lax.dot_general(left, right, NN, precision=lax.Precision.HIGHEST, preferred_element_type=f32)


def thirds(x):
    parts = []
    for _ in range(3):
        parts.append(x.astype(bf16))
        x = x - parts[-1].astype(f32)
    return parts


def tile_spec(kind, shape, tile):
    n = shape[0 if kind[0] == "r" else 1] // tile

    def at(i):
        if "b" in kind:
            return jnp.maximum(i - 1, 0)
        return jnp.minimum(i, n - 1) if "f" in kind else i

    if kind[0] == "r":
        return pl.BlockSpec((tile, D), lambda i: (at(i), 0))
    return pl.BlockSpec((shape[0], tile), lambda i: (0, at(i)))


def whole_spec(shape):
    zeros = (0,) * len(shape)
    return pl.BlockSpec(shape, lambda i: zeros, pipeline_mode=pl.Buffered(1))


def block_spec(shape, b):
    return pl.BlockSpec((1,) + shape[1:], lambda i: (b, 0, 0), pipeline_mode=pl.Buffered(1))


PAIR = range(2)
ANY = pl.BlockSpec(memory_space=pl.ANY)
SCALARS = pl.BlockSpec(memory_space=pltpu.SMEM)


class Board:
    def __init__(self):
        self.flows, self.firsts, self.arrays, self.forms, self.fresh = [], [], {}, {}, 0

    def add(self, name, form, cuts, array, other=None, block=0):
        flows = flows_of(name, form, cuts)
        self.flows += flows
        self.forms[name] = FORMS[form]
        self.arrays[name + ":src"] = array.reshape(self.forms[name])
        if form == "wide":
            self.firsts.append(First(name, flows, other, block))
            self.arrays[name + ":inv"] = other
        elif form == "tri":
            for f in flows:
                f.old = (block, TRI // 2)
            self.arrays[name + ":old"] = other

    def plan(self, tick_us, last):
        for f in self.flows:
            f.at = f.b if hasattr(f, "b") else f.at
        flows = [f for f in self.flows if f.at < LAST and not (f.wide and f.at == 5)]
        idle = [f for f in self.flows if f.wide and f.at == 5]
        for f in idle:
            f.a = f.b = f.at
        slots, rest, end = plan(flows, self.firsts, tick_us, last)
        runs = [f for f in self.firsts if f.fans[0] in flows]
        self.firsts = [f for f in self.firsts if f not in runs]
        self.flows = [f for f in flows + idle if f.b < LAST or f.a < f.b]
        moving = [f for f in flows if f.a < f.b]
        ins, outs = [], {}
        for f in moving:
            if f.a == 0:
                ins.append(f.name + ":src")
            elif f.a < 5 or (f.a == 5 and not f.wide):
                ins.append(f.part + ":in")
            if f.mixes():
                ins += ["decay", f.name + ":old"]
            if f.b <= 5:
                outs[f.part + ":out"] = (f.kept(f.b), f.cols)
            else:
                outs[f.name + ":dst"] = self.forms[f.name]
        for first in runs:
            ins.append(first.name + ":inv")
            ins += [f.part + ":in" for f in first.flows if f.part + ":out" not in outs]
        ins += [name for name in outs if name in self.arrays]
        return slots, rest, end, moving, runs, list(dict.fromkeys(ins)), outs

    def keep(self, outs, values):
        for name, value in zip(outs, values):
            self.arrays[name.replace(":out", ":in")] = value


def run_stage(board, body, name, tile, tick_us, ins, outs, scratch, flops, cid, last=False):
    def spec(kind, shape):
        if kind == "w":
            return whole_spec(shape)
        return block_spec(shape, kind) if isinstance(kind, int) else tile_spec(kind, shape, tile)

    steps = len(tick_us)
    slots, rest, end, moving, runs, m_ins, m_outs = board.plan(tick_us, last)
    scr = [job.open(job.a, job.b) if isinstance(job, Flow) else job.open() for job in runs + moving]
    n_in, n_min, n_out, n_mout, n_scr = len(ins), len(m_ins), len(outs), len(m_outs), len(scratch)

    def kernel(*refs):
        refs = list(refs)

        def pull(n):
            return [refs.pop(0) for _ in range(n)]

        c_in, m_in, c_out, m_out, c_scr = pull(n_in), pull(n_min), pull(n_out), pull(n_mout), pull(n_scr)
        named = dict(zip(m_ins, m_in))
        named.update(zip(m_outs, m_out))
        step = pl.program_id(0)
        events = {}
        if moving:
            pl.when(step == 0)(enter)
            pl.when(step == min(1, steps - 1))(await_peers)
        for job, s in zip(runs + moving, scr):
            events[job] = job.bind(named, pull(len(s)))

        def fire(slot):
            for job, what, s in slot:
                if what in ("go", "stop"):
                    events[job][what](s)
                else:
                    events[job][what]()

        for t in range(steps):
            if slots[t]:
                pl.when(step == t)(functools.partial(fire, slots[t]))
        if body is not None:
            body(*c_in, *c_out, *c_scr)
        if rest:
            pl.when(step == steps - 1)(functools.partial(fire, rest))

    params = dict(vmem_limit_bytes=63 * MIB)
    if moving:
        params.update(collective_id=cid, has_side_effects=True)
    values = pl.pallas_call(
        kernel, grid=(steps,),
        in_specs=[spec(kind, arr.shape) for arr, kind in ins] + [SCALARS if m == "decay" else ANY for m in m_ins],
        out_specs=[spec(kind, shape) for shape, dtype, kind in outs] + [ANY] * n_mout,
        out_shape=[jax.ShapeDtypeStruct(shape, dtype) for shape, dtype, kind in outs]
        + [jax.ShapeDtypeStruct(shape, f32) for shape in m_outs.values()],
        scratch_shapes=list(scratch) + [x for s in scr for x in s],
        input_output_aliases={n_in + m_ins.index(m): n_out + i for i, m in enumerate(m_outs) if m in m_ins},
        compiler_params=pltpu.CompilerParams(**params),
        cost_estimate=pl.CostEstimate(flops=flops, bytes_accessed=40 * MIB, transcendentals=0),
        name=name)(*[arr for arr, _ in ins], *[board.arrays[m] for m in m_ins])
    board.keep(m_outs, values[n_out:])
    return values[:n_out]


def final_kernel(decay, t0, t1, t2, t3, n0, n1, n2, n3, *refs):
    small_in, small_out, outs, scratch = refs[:8], refs[12:14], refs[8:12], refs[14:]
    new_s, new_a, p_up, p_down = outs
    pk, tr, nv, pv, pt, inv_s, sums, olds, invs, news, sem_in, sem_out, sem_small = scratch
    rho = decay[0]
    scale = (1.0 - rho) * decay[1]
    deep = pk.shape[0]
    ahead = deep // 2
    units = []
    for q, (src, new, n) in enumerate(((t0, new_a, n0), (t1, new_a, n1), (t2, new_s, n2), (t3, new_s, n3))):
        off = 0
        for j in range(NB):
            units.append((q, src, new, q % 2, j, off, n))
            off += (j + 1) * B

    def loads(u):
        q, src, new, b, j, off, n = units[u]
        rows, s = (j + 1) * B, u % deep
        parts = ((src.at[pl.ds(off, rows), :], pk.at[s, pl.ds(0, rows), :]),
                 (n.at[j // 3, :, pl.ds(j % 3 * B, B)], nv.at[s]))
        return [pltpu.make_async_copy(x, y, sem_in.at[s, i]) for i, (x, y) in enumerate(parts)]

    def stores(u):
        q, src, new, b, j, off, n = units[u]
        rows, s = (j + 1) * B, u % deep
        parts = [(pk.at[s, pl.ds(0, rows), :], new.at[b, pl.ds(0, rows), pl.ds(j * B, B)])]
        if q < 2:
            parts.append((pv.at[s], p_up.at[b, :, pl.ds(j * B, B)]))
        else:
            parts.append((pt.at[s], p_down.at[b, pl.ds(j * B, B), :]))
        if j:
            parts.append((tr.at[s, :, pl.ds(0, j * B)], new.at[b, pl.ds(j * B, B), pl.ds(0, j * B)]))
        return [pltpu.make_async_copy(x, y, sem_out.at[s, i]) for i, (x, y) in enumerate(parts)]

    places = [sums.at[i] for i in range(4)] + [olds.at[i] for i in PAIR] + [invs.at[i] for i in PAIR]
    early = [pltpu.make_async_copy(x, y, sem_small.at[i]) for i, (x, y) in enumerate(zip(small_in, places))]
    late = [pltpu.make_async_copy(news.at[i], small_out[i], sem_small.at[len(early) + i]) for i in PAIR]

    def mix_small():
        h = B // 2
        for c in early[:6]:
            c.wait()
        for i in range(4):
            acc, old, new = sums.at[i], olds.at[i // 2, i % 2], news.at[i // 2, i % 2]
            top = rho * old[:h, :] + scale * acc[0]
            mid = rho * old[h:B, h:] + scale * acc[1, :, :B]
            low = rho * old[B:, B:] + scale * acc[1, :, B:]
            new[:h, :] = top
            new[h:B, h:] = mid
            new[B:, B:] = low
            new[h:, :h] = top[:, h:].T
            new[B:, h:B] = mid[:, h:].T
        for c in late:
            c.start()

    for c in early[6:]:
        c.start()
    for u in range(ahead):
        for c in loads(u):
            c.start()
    for c in early[:6]:
        c.start()
    for u, (q, src, new, b, j, off, n) in enumerate(units):
        s = u % deep
        for c in loads(u):
            c.wait()
        if u == NB:
            mix_small()
        if j == 0 and b == 0:
            early[6 + q // 2].wait()
        for i in range(j):
            here = slice(i * B, (i + 1) * B)
            tr[s, :, here] = pk[s, here, :].T
        if j == 0:
            x, y, z = thirds(invs[q // 2, b])
            for i, third in enumerate((x, x, y, x, y, z)):
                inv_s[:, i * D:(i + 1) * D] = third
        x, y, z = thirds(nv[s])
        prod = mm(inv_s[...], jnp.concatenate((x, y, x, z, y, x), axis=0), NN) * decay[1]
        if q < 2:
            pv[s] = prod
        else:
            pt[s] = prod.T
        for c in stores(u):
            c.start()
        if u + ahead < len(units):
            if u + ahead >= deep:
                for c in stores(u + ahead - deep):
                    c.wait()
            for c in loads(u + ahead):
                c.start()
    for c in late:
        c.wait()
    for u in range(len(units) - deep, len(units)):
        for c in stores(u):
            c.wait()


def finish(decay, tris, smalls, prods, s_up_old, a_up_old, s_down_old, inv_u, inv_q):
    big = jax.ShapeDtypeStruct(s_up_old.shape, f32)
    small = jax.ShapeDtypeStruct(a_up_old.shape, f32)
    deep = 6
    return pl.pallas_call(
        final_kernel,
        in_specs=[SCALARS] + [ANY] * 16,
        out_specs=[ANY] * 6,
        out_shape=[big, big, jax.ShapeDtypeStruct((2, D, FF), f32), jax.ShapeDtypeStruct((2, FF, D), f32), small, small],
        scratch_shapes=[pltpu.VMEM((deep, FF, B), f32), pltpu.VMEM((deep, B, FF), f32)]
        + [pltpu.VMEM((deep, D, B), f32)] * 2 + [pltpu.VMEM((deep, B, D), f32), pltpu.VMEM((D, 6 * D), bf16)]
        + [pltpu.VMEM((4,) + SMALL, f32)] + [pltpu.VMEM((2,) + a_up_old.shape, f32)] * 3
        + [pltpu.SemaphoreType.DMA((deep, 3))] * 2 + [pltpu.SemaphoreType.DMA((10,))],
        compiler_params=pltpu.CompilerParams(vmem_limit_bytes=63 * MIB),
        name="finish")(decay, *[t.reshape(TRI, B) for t in tris], *prods, *smalls, a_up_old, s_down_old, inv_u, inv_q)


def solution(mesh):
    axis_size = mesh.shape["data"]
    tile = 512

    def local_step(tok, grad, w_up, w_down, a_up_old, s_up_old, a_down_old, s_down_old,
                   a_up_inv, s_up_inv, a_down_inv, s_down_inv, factor_decay):
        total = tok.shape[0]
        steps = total // tile
        inv_n = 1.0 / (total * axis_size)
        acts = [pltpu.VMEM((FF, tile), bf16)] * 2
        w_t = pltpu.VMEM((FF, D), bf16)
        unit = 2 * total * FF * D
        wide_out, small_out, tri_out = (WIDE, f32, "w"), (SMALL, f32, "w"), ((TRI, B), f32, "w")
        long_out, short_out = ((FF, total), bf16, "cf"), ((D, total), bf16, "cb")
        board = Board()
        decay = jnp.stack((factor_decay, jnp.float32(inv_n)))
        board.arrays["decay"] = decay
        pre0, u1, ad0, au0, sd1 = run_stage(
            board, stage1, "stage1", 2 * tile, [0.0] * (steps // 2),
            ((tok, "r"), (grad, "r"), (w_up, 0), (w_down, 0)),
            (long_out, ((D, total), bf16, "c"), tri_out, small_out, small_out),
            [pltpu.VMEM((FF, 2 * tile), bf16), w_t, pltpu.VMEM((D, FF), bf16)], 5 * unit, 0)
        board.add("ad0", "tri", CUTS["ad0"], ad0, a_down_old, 0)
        board.add("au0", "small", CUTS["au0"], au0)
        board.add("sd1", "small", CUTS["sd1"], sd1)
        pre1, ad1, au1, dwd1 = run_stage(
            board, stage2, "stage2", tile, [2.2] + [3.36] * steps, ((u1, "cf"), (w_up, 1), (u1, "cb"), (grad, "rb")),
            (long_out, tri_out, small_out, wide_out), acts + [w_t], 5 * unit, 1)
        board.add("ad1", "tri", CUTS["ad1"], ad1, a_down_old, 1)
        board.add("au1", "small", CUTS["au1"], au1)
        board.add("dwd1", "wide", CUTS["dwd1"], dwd1, a_down_inv, 1)
        e1, su1, dwu1 = run_stage(
            board, stage3, "stage3", tile, [2.4] + [4.4] * steps,
            ((pre1, "cf"), (grad, "rf"), (w_down, 1), (w_up, 1), (u1, "cb")), (short_out, tri_out, wide_out), acts, 6 * unit, 2)
        board.add("su1", "tri", CUTS["su1"], su1, s_up_old, 1)
        board.add("dwu1", "wide", CUTS["dwu1"], dwu1, s_up_inv, 1)
        g0, sd0, dwd0, dwu0 = run_stage(
            board, stage4, "stage4", tile, [2.2] + [3.2] * steps,
            ((pre0, "cf"), (e1, "cf"), (w_down, 0), (tok, "rb"), (e1, "cb")),
            (long_out, small_out, wide_out, wide_out), acts * 2, 4 * unit, 3)
        board.add("sd0", "small", CUTS["sd0"], sd0)
        board.add("dwd0", "wide", CUTS["dwd0"], dwd0, a_down_inv, 0)
        board.add("dwu0", "wide", CUTS["dwu0"], dwu0, s_up_inv, 0)
        su0, = run_stage(board, stage5, "stage5", tile, [1.75] * steps, ((g0, "c"),), (tri_out,), [], 3 * unit, 4)
        board.add("su0", "tri", CUTS["su0"], su0, s_up_old, 0)
        run_stage(board, None, "tail", tile, [0.1], (), (), [], unit, 5, last=True)
        done = board.arrays
        new_s, new_a, p_up, p_down, new_u, new_q = finish(
            decay, [done[n + ":dst"] for n in ("ad0", "ad1", "su0", "su1")],
            [done[n + ":dst"] for n in ("au0", "au1", "sd0", "sd1")],
            [done[n + ":dst"] for n in ("dwu0", "dwu1", "dwd0", "dwd1")],
            s_up_old, a_up_old, s_down_old, a_up_inv, s_down_inv)
        return p_up, p_down, new_u, new_s, new_a, new_q

    batch_spec = P("data", None)
    replicated = P()
    return jax.shard_map(local_step, mesh=mesh, in_specs=(batch_spec, batch_spec) + (replicated,) * 11,
                         out_specs=(replicated,) * 6, check_vma=False)
```

```python
import functools

import jax
import jax.numpy as jnp
from jax import lax
from jax.experimental import pallas as pl
from jax.experimental.pallas import tpu as pltpu
from jax.sharding import PartitionSpec as P

bf16 = jnp.bfloat16
f32 = jnp.float32
D, FF, B = 384, 1536, 256
NB = FF // B
TRI = sum((j + 1) * B for j in range(NB))
NN = (((1,), (0,)), ((), ()))
NT = (((1,), (1,)), ((), ()))
TN = (((0,), (0,)), ((), ()))
TT = (((0,), (1,)), ((), ()))
GELU_K = 0.7978845608028654
GELU_C = 0.044715 * GELU_K
MIB = 1 << 20


def mm(left, right, dims):
    return lax.dot_general(left, right, dims, preferred_element_type=f32)


def half_sig(pre):
    cubic = GELU_C * (pre * pre)
    return 0.5 * jnp.tanh(pre * (cubic + GELU_K)) + 0.5, cubic


def gelu_back(pre, sig, cubic):
    hid = pre * sig
    return hid, sig + (hid * (1.0 - sig)) * (6.0 * cubic + 2.0 * GELU_K)


def add_tri(acc, mat):
    off = 0
    for j in range(NB):
        rows = (j + 1) * B
        acc[off:off + rows, :] += mm(mat[:rows, :], mat[j * B:rows, :], NT)
        off += rows


def add_small_tn(acc, rows):
    acc[0] += mm(rows[:, 0:128], rows[...], TN)
    acc[1, :, 0:256] += mm(rows[:, 128:256], rows[:, 128:384], TN)
    acc[1, :, 256:384] += mm(rows[:, 256:384], rows[:, 256:384], TN)


def add_small_nt(acc, cols):
    acc[0] += mm(cols[0:128, :], cols[...], NT)
    acc[1, :, 0:256] += mm(cols[128:256, :], cols[128:384, :], NT)
    acc[1, :, 256:384] += mm(cols[256:384, :], cols[256:384, :], NT)


def zero_first(accs):
    @pl.when(pl.program_id(0) == 0)
    def _():
        for acc in accs:
            acc[...] = jnp.zeros_like(acc)


MESH = pl.DeviceIdType.MESH
ORDERS = {key: tuple(map(int, order)) for key, order in
          (("X", "1234"), ("Y", "2134"), ("Z", "3412"), ("A", "1342"), ("B", "2341"), ("C", "3421"))}
LINKS = {0: {0: 6e5}, 1: {1: 45e3}, 2: {2: 45e3}, 3: {3: 45e3}, 4: {3: 45e3, 4: 23e3}}
LAG = 2.0
SLACK = 3.0


def PRIORITY(f):
    return f.b


LAST = 10


def my_bits():
    me = lax.axis_index("data")
    bits = [(me // (1 << d)) % 2 for d in range(5)]
    return bits, [me + (1 - 2 * bits[d]) * (1 << d) for d in range(5)]


def enter():
    for peer in my_bits()[1]:
        pl.semaphore_signal(pltpu.get_barrier_semaphore(), inc=1, device_id=(peer,), device_id_type=MESH)


def await_peers():
    pl.semaphore_wait(pltpu.get_barrier_semaphore(), 5)


def al(row):
    return pl.multiple_of(row, 8)


class Flow:
    def __init__(self, name, row0, rows, cols, order, shard_row, wide):
        self.name, self.row0, self.rows, self.cols, self.order = name, row0, rows, cols, order
        self.shard_row, self.wide, self.old = shard_row, wide, None
        self.at, self.start = 0, 0.0
        self.part = name + ":part%d" % row0

    def fan(self):
        other = Flow(self.name, self.row0, self.rows, self.cols, self.order, self.shard_row, True)
        other.at = 5
        return other

    def dim(self, s):
        if s in (0, LAST - 1):
            return 0
        return self.order[s - 1] if s < 5 else self.order[LAST - 2 - s]

    def length(self, s):
        return self.rows >> s if s < 5 else self.rows >> (LAST - 1 - s)

    def kept(self, steps):
        return self.rows >> (steps - 1)

    def open(self, a, b):
        self.a, self.b = a, b
        n = b - a
        out = [pltpu.SemaphoreType.DMA((3,)), pltpu.SemaphoreType.DMA((n,)), pltpu.SemaphoreType.DMA((n,))]
        if a < 5:
            out.append(pltpu.VMEM((self.rows if a == 0 else self.kept(a), self.cols), f32))
            out.append(pltpu.VMEM((sum(self.length(s) for s in range(a, min(b, 5))), self.cols), f32))
            if self.mixes():
                out.append(pltpu.VMEM((self.kept(5), self.cols), f32))
        elif a == 5 and not self.wide:
            out.append(pltpu.VMEM((self.kept(5), self.cols), f32))
        return out

    def mixes(self):
        return self.old is not None and self.a < 5 <= self.b

    def bind(self, named, scr):
        a, b, row0, rows = self.a, self.b, self.row0, self.rows
        sem_l, sem_s, sem_r = scr[:3]
        bits, peers = my_bits()
        core = bits[0]
        lens, offs = [rows], [0]
        for d in self.order:
            lens.append(lens[-1] // 2)
            offs.append(offs[-1] + bits[d] * lens[-1])
        src, dst = named.get(self.name + ":src"), named.get(self.name + ":dst")
        part_in, part_out = named.get(self.part + ":in"), named.get(self.part + ":out")
        base = offs[min(max(a, 1), 5) - 1]
        work = recv = None
        if a < 5:
            work, recv = scr[3:5]
        elif a == 5:
            work = named[self.name + ":first"].at[pl.ds(self.shard_row, self.kept(5)), :] if self.wide else scr[3]
        sends, begin_recv, locals_ = {}, {}, []

        def remote(s, x, y):
            return pltpu.make_async_remote_copy(src_ref=x, dst_ref=y, send_sem=sem_s.at[s - a], recv_sem=sem_r.at[s - a],
                                                device_id=(peers[self.dim(s)],), device_id_type=MESH)

        def final():
            return work if a == 5 else work.at[pl.ds(al(offs[4] - base), lens[4]), :]

        def spot(k):
            return dst.at[core, pl.ds(al(row0 + offs[k]), lens[k]), :]

        at = 0
        for s in range(a, b):
            if s < 5:
                begin_recv[s] = at
                to = recv.at[pl.ds(at, self.length(s)), :]
                at += self.length(s)
                if s == 0:
                    sends[s] = remote(s, src.at[1 - core, pl.ds(row0, rows), :], to)
                else:
                    gone = al(offs[s - 1] - base + (1 - bits[self.dim(s)]) * lens[s])
                    sends[s] = remote(s, work.at[pl.ds(gone, lens[s]), :], to)
            else:
                k = LAST - 1 - s
                sends[s] = remote(s, final() if s == 5 else spot(k), spot(k))
        load = place = save = old = None
        if self.mixes():
            old_array, half = self.old
            spot4 = core * half + row0 + offs[4]
            j = sum((spot4 // (B // 2 * m * (m + 1)) + 31) // 32 for m in range(1, NB))
            old = pltpu.make_async_copy(
                named[self.name + ":old"].at[old_array, pl.ds(al(spot4 - B // 2 * j * (j + 1)), lens[4]),
                                             pl.ds(pl.multiple_of(j * B, B), B)], scr[5], sem_l.at[2])
        if a == 0:
            load = pltpu.make_async_copy(src.at[core, pl.ds(row0, rows), :], work, sem_l.at[0])
        elif a < 5 or (a == 5 and not self.wide):
            load = pltpu.make_async_copy(part_in, work, sem_l.at[0])
        if a <= 5 < b:
            place = pltpu.make_async_copy(final(), spot(4), sem_l.at[1])
        if b <= 5:
            kept = work.at[pl.ds(al(offs[b - 1] - base), lens[b - 1]), :]
            save = pltpu.make_async_copy(kept, part_out, sem_l.at[1])

        def add(row, frm, count):
            for q in range(0, count, 64):
                step = min(count - q, 64)
                x, y = al(row + q), al(frm + q)
                work[pl.ds(x, step), :] = work[pl.ds(x, step), :] + recv[pl.ds(y, step), :]

        def mix():
            rho = named["decay"][0]
            x, y = pl.ds(al(offs[4] - base), lens[4]), pl.ds(begin_recv[4], lens[4])
            total = (work[x, :] + recv[y, :]) * named["decay"][1]
            work[x, :] = rho * scr[5][...] + (1.0 - rho) * total

        def take(s, then):
            if s == a and load is not None and a == 0:
                load.wait()
            sends[s].wait_recv()
            if s == 5 and place is not None:
                place.wait()
            if s >= 5:
                then()
            elif s == 4 and old is not None:
                old.wait()
                mix()
                then()
            elif s == 4 or s + 1 == b:
                add(offs[s] - base, begin_recv[s], lens[s])
                then()
            else:
                half = lens[s + 1]
                bit = bits[self.dim(s + 1)]
                add(offs[s] - base + (1 - bit) * half, begin_recv[s] + (1 - bit) * half, half)
                then()
                add(offs[s] - base + bit * half, begin_recv[s] + bit * half, half)

        def send(s):
            if s == 5:
                place.start()
            sends[s].start()

        def begin():
            load.start()
            if old is not None:
                old.start()
            if a == 0:
                send(0)

        def go(s):
            if s > a:
                take(s - 1, lambda: send(s))
            else:
                if load is not None:
                    load.wait()
                send(s)

        def stop():
            take(b - 1, save.start if save is not None else lambda: None)

        def end():
            if save is not None:
                save.wait()
            for s in range(a, b):
                sends[s].wait_send()

        return {"begin": begin, "go": go, "stop": lambda s: stop(), "end": end}


class First:
    def __init__(self, name, flows, inverse, block):
        self.name, self.flows, self.inverse, self.block, self.done = name, flows, inverse, block, False
        self.fans = [f.fan() for f in flows]

    def open(self):
        rows = pltpu.VMEM((24, 768), f32)
        return [pltpu.SemaphoreType.DMA((4,)), pltpu.SemaphoreType.DMA((3,)), pltpu.SemaphoreType.DMA((3,)),
                rows, rows, rows, pltpu.VMEM((FF, 768), f32)]

    def bind(self, named, scr):
        sem_l, sem_s, sem_r, own, other, prod, inv_v = scr
        named[self.name + ":first"] = prod
        bits, peers = my_bits()
        core = bits[0]
        inv = named[self.name + ":inv"]
        copies, swaps = [], []
        for i, flow in enumerate(self.flows):
            rows = named.get(flow.part + ":out", named.get(flow.part + ":in"))
            spot = pl.ds(flow.shard_row, flow.kept(5))
            copies.append(pltpu.make_async_copy(rows, own.at[spot, :], sem_l.at[i]))
            swaps.append(pltpu.make_async_remote_copy(
                src_ref=rows, dst_ref=other.at[spot, :], send_sem=sem_s.at[i], recv_sem=sem_r.at[i],
                device_id=(peers[0],), device_id_type=MESH))
        copies.append(pltpu.make_async_copy(
            inv.at[self.block, :, pl.ds(pl.multiple_of(core * 768, 128), 768)], inv_v, sem_l.at[3]))

        def begin():
            for copy in copies + swaps:
                copy.start()

        def go(s):
            for copy in copies + swaps:
                copy.wait()
            prod[...] = (precise(own[...], inv_v[pl.ds(al(core * 768), 768), :])
                         + precise(other[...], inv_v[pl.ds(al((1 - core) * 768), 768), :]))

        return {"begin": begin, "go": go}


def plan(flows, firsts, tick_us, last, over=2.0):
    times = [0.0]
    for us in tick_us:
        times.append(times[-1] + us)
    limit = 1e9 if last else times[-1]
    free, now_rest = {}, times[-1]
    slots, rest = [[] for _ in tick_us], []
    ready = {f: f.start for f in flows}
    phase = {f: "new" for f in flows}
    for f in flows:
        f.a = f.b = f.at
    fstate = {f: "new" for f in firsts}
    fready = {}

    def arrival(f, s, now):
        links = LINKS[f.dim(s)]
        size = f.length(s) * f.cols * 4
        begin = max([now] + [free.get(link, 0.0) for link in links])
        return begin, max(begin + size / rate for rate in links.values()), size

    def send(f, s, now):
        begin, end, size = arrival(f, s, now)
        for link, rate in LINKS[f.dim(s)].items():
            free[link] = begin + size / rate
        f.b = s + 1
        ready[f] = end + LAG

    def allowed(f, s, now):
        return last or (now < limit and arrival(f, s, now)[1] + LAG < limit + over)

    def clear(f, s, now):
        return arrival(f, s, now)[0] <= now + SLACK

    def move(f, now):
        if ready[f] > now:
            return None
        if phase[f] == "new":
            if f.at >= LAST or f.wide and f.at == 5:
                return None
            if not allowed(f, f.at, now + (LAG if 0 < f.at <= 5 else 0.0)):
                return None
            if not clear(f, f.at, now):
                return None
            if f.at == 0:
                phase[f] = "run"
                send(f, 0, now)
                return "begin", 0
            if f.at <= 5:
                phase[f] = "loaded"
                ready[f] = now + LAG
                f.b = f.at + 1
                return "begin", 0
            phase[f] = "run"
            send(f, f.at, now)
            return "go", f.at
        if phase[f] == "loaded":
            phase[f] = "run"
            send(f, f.at, now)
            return "go", f.at
        if phase[f] == "run":
            s = f.b
            if s == LAST or f.wide and s == 5 or not allowed(f, s, now):
                phase[f] = "saved"
                ready[f] = now + LAG
                return "stop", s
            if not clear(f, s, now):
                return None
            send(f, s, now)
            return "go", s
        if phase[f] == "saved":
            phase[f] = "done"
            return "end", 0
        return None

    def first_move(f, now):
        if f.done or fready.get(f, 0.0) > now:
            return None
        if fstate[f] == "new":
            ok = all(x.b == 5 and phase.get(x, "done") in ("new", "done") for x in f.flows)
            if not ok or not (last or now + 20.0 < limit):
                return None
            fstate[f] = "loaded"
            fready[f] = now + 5.0
            return "begin", 0
        if fstate[f] == "loaded":
            fstate[f] = "done"
            return "go", 0
        return None

    def sweep(now, out):
        again = True
        while again:
            again = False
            for f in sorted(flows, key=PRIORITY):
                e = move(f, now)
                if e:
                    out.append((f,) + e)
                    again = True
                    break
            for f in firsts:
                e = first_move(f, now)
                if e:
                    out.append((f,) + e)
                    again = True
                    if fstate[f] == "done":
                        for x in f.fans:
                            flows.append(x)
                            x.a = 5
                            phase[x] = "run"
                            send(x, 5, now)
                            out.append((x, "go", 5))

    for t, now in enumerate(times[:-1]):
        if t or last:
            sweep(now, slots[t])
    now = times[-1]
    while True:
        sweep(now, rest)
        later = [ready[f] for f in flows if phase[f] in ("loaded", "run", "saved") and ready[f] > now]
        later += [fready[f] for f in firsts if fstate[f] == "loaded" and fready[f] > now]
        held = any(phase[f] in ("loaded", "run") or last and phase[f] == "new" and f.at < LAST and not (f.wide and f.at == 5)
                   for f in flows)
        if not later and not held:
            return slots, rest, now
        now = min(later + ([now + 1.0] if held else []))


def tri_col(acc, mat, j):
    rows = (j + 1) * B
    off = B * j * (j + 1) // 2
    acc[off:off + rows, :] += mm(mat[:rows, :], mat[j * B:rows, :], NT)


def staged(dot, act, backs, shifts, accs, setup=None):
    step, last = pl.program_id(0), pl.num_programs(0) - 1

    def shift():
        for old, new in shifts:
            old[...] = new[...]

    @pl.when(step == 0)
    def _():
        for acc in accs:
            acc[...] = jnp.zeros_like(acc)
        if setup is not None:
            setup()
        for k in range(NB):
            act(k, dot(k))

    @pl.when((step > 0) & (step < last))
    def _():
        shift()
        for k, back in enumerate(backs):
            value = dot(k)
            back()
            act(k, value)

    @pl.when(step == last)
    def _():
        shift()
        for back in backs:
            back()


def plain(dot, act, backs, accs, setup):
    @pl.when(pl.program_id(0) == 0)
    def _():
        for acc in accs:
            acc[...] = jnp.zeros_like(acc)
        setup()

    for k in range(NB):
        act(k, dot(k))
    for back in backs:
        back()


def block(k):
    return slice(k * B, (k + 1) * B)


def tri_pieces(acc, mat, *more):
    pieces = [(5,), (4,), (3, 0), (2, 1)]

    def run(cols, fns):
        for j in cols:
            tri_col(acc, mat, j)
        for fn in fns:
            fn()

    return [functools.partial(run, cols, ()) for cols in pieces] + [functools.partial(run, (), fns) for fns in more]


def gelu_act(pre_out, new_s):
    def act(k, value):
        pre = value.astype(bf16)
        pre_out[block(k), :] = pre
        pre = pre.astype(f32)
        new_s[block(k), :] = (pre * half_sig(pre)[0]).astype(bf16)
    return act


def stage1(tok, grad, w_up, w_down, pre_out, next_out, tri, small_u, small_q, hid_s, up_s, down_s):
    def setup():
        up_s[...] = w_up[0].T
        down_s[...] = w_down[0].T

    def dot(k):
        return mm(up_s[block(k), :], tok[...], NT)

    def down():
        next_out[...] = mm(down_s[...], hid_s[...], NN).astype(bf16)

    def smalls():
        add_small_tn(small_u, tok)
        add_small_tn(small_q, grad)

    backs = [functools.partial(tri_col, tri, hid_s, j) for j in range(NB)] + [down, smalls]
    plain(dot, gelu_act(pre_out, hid_s), backs, (tri, small_u, small_q), setup)


def add_wide(acc, left, mat, dims, h):
    acc[h] += mm(left[...], mat[h * FF // 2:(h + 1) * FF // 2, :], dims)


def stage2(u_t, w_up, u_b, grad_b, pre_out, tri, small_u, dwd, new_s, hid_s, up_s):
    def setup():
        up_s[...] = w_up[0].T

    def dot(k):
        return mm(up_s[block(k), :], u_t[...], NN)

    wide = [functools.partial(add_wide, dwd, grad_b, hid_s, TT, h) for h in PAIR]
    backs = tri_pieces(tri, hid_s, wide[:1], (wide[1], lambda: add_small_nt(small_u, u_b)))
    staged(dot, gelu_act(pre_out, new_s), backs, ((hid_s, new_s),), (tri, small_u, dwd), setup)


def stage3(pre_in, grad, w_down, w_up, u_b, err_out, tri, dwu, new_s, g_s):
    def dot(k):
        return mm(w_down[0, block(k), :], grad[...], NT)

    def act(k, value):
        d_hid = value.astype(bf16).astype(f32)
        pre = pre_in[block(k), :].astype(f32)
        sig, cubic = half_sig(pre)
        new_s[block(k), :] = (d_hid * gelu_back(pre, sig, cubic)[1]).astype(bf16)

    def up():
        err_out[...] = mm(w_up[0], g_s[...], NN).astype(bf16)

    wide = [functools.partial(add_wide, dwu, u_b, g_s, NT, h) for h in PAIR]
    staged(dot, act, tri_pieces(tri, g_s, wide, (up,)), ((g_s, new_s),), (tri, dwu))


def stage4(pre_in, err_t, w_down, tok_b, err_b, tri, small_q, dwd, dwu, new_h, hid_s, new_g, g_s):
    def dot(k):
        return mm(w_down[0, block(k), :], err_t[...], NN)

    def act(k, value):
        d_hid = value.astype(bf16).astype(f32)
        pre = pre_in[block(k), :].astype(f32)
        sig, cubic = half_sig(pre)
        hid, slope = gelu_back(pre, sig, cubic)
        new_h[block(k), :] = hid.astype(bf16)
        new_g[block(k), :] = (d_hid * slope).astype(bf16)

    downs = [functools.partial(add_wide, dwd, err_b, hid_s, NT, h) for h in PAIR]
    ups = [functools.partial(add_wide, dwu, tok_b, g_s, TT, h) for h in PAIR]
    backs = tri_pieces(tri, g_s, downs, ups + [lambda: add_small_nt(small_q, err_b)])
    staged(dot, act, backs, ((hid_s, new_h), (g_s, new_g)), (tri, small_q, dwd, dwu))


SMALL = (2, 128, 384)
WIDE = (2, 384, 768)
TRI_SHAPE = (2, TRI // 2, B)
CUTS = {
    "ad0": "1024X,512A,1024Y,128B", "au0": "128X", "sd1": "128Y",
    "ad1": "128A,1024A,512B,512Y,512Y", "au1": "128Y", "dwd1": "128Y,256A",
    "su1": "128A,512B,512X,512X,512A,512Y", "dwu1": "384Y",
    "sd0": "128Y", "dwd0": "256B,128Z", "dwu0": "128Y,256X", "su0": "512A,512Y,512C,512X,128Z,512X",
}
FORMS = {"tri": TRI_SHAPE, "wide": WIDE, "small": SMALL}


def flows_of(name, form, cuts):
    flows, row = [], 0
    for cut in cuts.split(","):
        flows.append(Flow(name, row, int(cut[:-1]), FORMS[form][2], ORDERS[cut[-1]], row // 16, form == "wide"))
        row += flows[-1].rows
    return flows


def precise(left, right):
    return lax.dot_general(left, right, NN, precision=lax.Precision.HIGHEST, preferred_element_type=f32)


def thirds(x):
    parts = []
    for _ in range(3):
        parts.append(x.astype(bf16))
        x = x - parts[-1].astype(f32)
    return parts


def tile_spec(kind, shape, tile):
    n = shape[0 if kind[0] == "r" else 1] // tile

    def at(i):
        if "b" in kind:
            return jnp.maximum(i - 1, 0)
        return jnp.minimum(i, n - 1) if "f" in kind else i

    if kind[0] == "r":
        return pl.BlockSpec((tile, D), lambda i: (at(i), 0))
    return pl.BlockSpec((shape[0], tile), lambda i: (0, at(i)))


def whole_spec(shape):
    zeros = (0,) * len(shape)
    return pl.BlockSpec(shape, lambda i: zeros, pipeline_mode=pl.Buffered(1))


def block_spec(shape, b):
    return pl.BlockSpec((1,) + shape[1:], lambda i: (b, 0, 0), pipeline_mode=pl.Buffered(1))


PAIR = range(2)
ANY = pl.BlockSpec(memory_space=pl.ANY)
SCALARS = pl.BlockSpec(memory_space=pltpu.SMEM)


class Board:
    def __init__(self):
        self.flows, self.firsts, self.arrays, self.forms, self.fresh = [], [], {}, {}, 0

    def add(self, name, form, cuts, array, other=None, block=0):
        flows = flows_of(name, form, cuts)
        self.flows += flows
        self.forms[name] = FORMS[form]
        self.arrays[name + ":src"] = array.reshape(self.forms[name])
        if form == "wide":
            self.firsts.append(First(name, flows, other, block))
            self.arrays[name + ":inv"] = other
        elif form == "tri":
            for f in flows:
                f.old = (block, TRI // 2)
            self.arrays[name + ":old"] = other

    def plan(self, tick_us, last):
        for f in self.flows:
            f.at = f.b if hasattr(f, "b") else f.at
        flows = [f for f in self.flows if f.at < LAST and not (f.wide and f.at == 5)]
        idle = [f for f in self.flows if f.wide and f.at == 5]
        for f in idle:
            f.a = f.b = f.at
        slots, rest, end = plan(flows, self.firsts, tick_us, last)
        runs = [f for f in self.firsts if f.fans[0] in flows]
        self.firsts = [f for f in self.firsts if f not in runs]
        self.flows = [f for f in flows + idle if f.b < LAST or f.a < f.b]
        moving = [f for f in flows if f.a < f.b]
        ins, outs = [], {}
        for f in moving:
            if f.a == 0:
                ins.append(f.name + ":src")
            elif f.a < 5 or (f.a == 5 and not f.wide):
                ins.append(f.part + ":in")
            if f.mixes():
                ins += ["decay", f.name + ":old"]
            if f.b <= 5:
                outs[f.part + ":out"] = (f.kept(f.b), f.cols)
            else:
                outs[f.name + ":dst"] = self.forms[f.name]
        for first in runs:
            ins.append(first.name + ":inv")
            ins += [f.part + ":in" for f in first.flows if f.part + ":out" not in outs]
        ins += [name for name in outs if name in self.arrays]
        return slots, rest, end, moving, runs, list(dict.fromkeys(ins)), outs

    def keep(self, outs, values):
        for name, value in zip(outs, values):
            self.arrays[name.replace(":out", ":in")] = value


def run_stage(board, body, name, tile, tick_us, ins, outs, scratch, flops, cid, last=False):
    def spec(kind, shape):
        if kind == "w":
            return whole_spec(shape)
        return block_spec(shape, kind) if isinstance(kind, int) else tile_spec(kind, shape, tile)

    steps = len(tick_us)
    slots, rest, end, moving, runs, m_ins, m_outs = board.plan(tick_us, last)
    scr = [job.open(job.a, job.b) if isinstance(job, Flow) else job.open() for job in runs + moving]
    n_in, n_min, n_out, n_mout, n_scr = len(ins), len(m_ins), len(outs), len(m_outs), len(scratch)

    def kernel(*refs):
        refs = list(refs)

        def pull(n):
            return [refs.pop(0) for _ in range(n)]

        c_in, m_in, c_out, m_out, c_scr = pull(n_in), pull(n_min), pull(n_out), pull(n_mout), pull(n_scr)
        named = dict(zip(m_ins, m_in))
        named.update(zip(m_outs, m_out))
        step = pl.program_id(0)
        events = {}
        if moving:
            pl.when(step == 0)(enter)
            pl.when(step == min(1, steps - 1))(await_peers)
        for job, s in zip(runs + moving, scr):
            events[job] = job.bind(named, pull(len(s)))

        def fire(slot):
            for job, what, s in slot:
                if what in ("go", "stop"):
                    events[job][what](s)
                else:
                    events[job][what]()

        for t in range(steps):
            if slots[t]:
                pl.when(step == t)(functools.partial(fire, slots[t]))
        if body is not None:
            body(*c_in, *c_out, *c_scr)
        if rest:
            pl.when(step == steps - 1)(functools.partial(fire, rest))

    params = dict(vmem_limit_bytes=63 * MIB)
    if moving:
        params.update(collective_id=cid, has_side_effects=True)
    values = pl.pallas_call(
        kernel, grid=(steps,),
        in_specs=[spec(kind, arr.shape) for arr, kind in ins] + [SCALARS if m == "decay" else ANY for m in m_ins],
        out_specs=[spec(kind, shape) for shape, dtype, kind in outs] + [ANY] * n_mout,
        out_shape=[jax.ShapeDtypeStruct(shape, dtype) for shape, dtype, kind in outs]
        + [jax.ShapeDtypeStruct(shape, f32) for shape in m_outs.values()],
        scratch_shapes=list(scratch) + [x for s in scr for x in s],
        input_output_aliases={n_in + m_ins.index(m): n_out + i for i, m in enumerate(m_outs) if m in m_ins},
        compiler_params=pltpu.CompilerParams(**params),
        cost_estimate=pl.CostEstimate(flops=flops, bytes_accessed=40 * MIB, transcendentals=0),
        name=name)(*[arr for arr, _ in ins], *[board.arrays[m] for m in m_ins])
    board.keep(m_outs, values[n_out:])
    return values[:n_out]


def final_kernel(decay, t0, t1, t2, t3, n0, n1, n2, n3, *refs):
    small_in, small_out, outs, scratch = refs[:8], refs[12:14], refs[8:12], refs[14:]
    new_s, new_a, p_up, p_down = outs
    pk, tr, nv, pv, pt, inv_s, sums, olds, invs, news, sem_in, sem_out, sem_small = scratch
    rho = decay[0]
    scale = (1.0 - rho) * decay[1]
    deep = pk.shape[0]
    ahead = deep // 2
    units = []
    for q, (src, new, n) in enumerate(((t0, new_a, n0), (t1, new_a, n1), (t2, new_s, n2), (t3, new_s, n3))):
        off = 0
        for j in range(NB):
            units.append((q, src, new, q % 2, j, off, n))
            off += (j + 1) * B

    def loads(u):
        q, src, new, b, j, off, n = units[u]
        rows, s = (j + 1) * B, u % deep
        parts = ((src.at[pl.ds(off, rows), :], pk.at[s, pl.ds(0, rows), :]),
                 (n.at[j // 3, :, pl.ds(j % 3 * B, B)], nv.at[s]))
        return [pltpu.make_async_copy(x, y, sem_in.at[s, i]) for i, (x, y) in enumerate(parts)]

    def stores(u):
        q, src, new, b, j, off, n = units[u]
        rows, s = (j + 1) * B, u % deep
        parts = [(pk.at[s, pl.ds(0, rows), :], new.at[b, pl.ds(0, rows), pl.ds(j * B, B)])]
        if q < 2:
            parts.append((pv.at[s], p_up.at[b, :, pl.ds(j * B, B)]))
        else:
            parts.append((pt.at[s], p_down.at[b, pl.ds(j * B, B), :]))
        if j:
            parts.append((tr.at[s, :, pl.ds(0, j * B)], new.at[b, pl.ds(j * B, B), pl.ds(0, j * B)]))
        return [pltpu.make_async_copy(x, y, sem_out.at[s, i]) for i, (x, y) in enumerate(parts)]

    places = [sums.at[i] for i in range(4)] + [olds.at[i] for i in PAIR] + [invs.at[i] for i in PAIR]
    early = [pltpu.make_async_copy(x, y, sem_small.at[i]) for i, (x, y) in enumerate(zip(small_in, places))]
    late = [pltpu.make_async_copy(news.at[i], small_out[i], sem_small.at[len(early) + i]) for i in PAIR]

    def mix_small():
        h = B // 2
        for c in early[:6]:
            c.wait()
        for i in range(4):
            acc, old, new = sums.at[i], olds.at[i // 2, i % 2], news.at[i // 2, i % 2]
            top = rho * old[:h, :] + scale * acc[0]
            mid = rho * old[h:B, h:] + scale * acc[1, :, :B]
            low = rho * old[B:, B:] + scale * acc[1, :, B:]
            new[:h, :] = top
            new[h:B, h:] = mid
            new[B:, B:] = low
            new[h:, :h] = top[:, h:].T
            new[B:, h:B] = mid[:, h:].T
        for c in late:
            c.start()

    for c in early[6:]:
        c.start()
    for u in range(ahead):
        for c in loads(u):
            c.start()
    for c in early[:6]:
        c.start()
    for u, (q, src, new, b, j, off, n) in enumerate(units):
        s = u % deep
        for c in loads(u):
            c.wait()
        if u == NB:
            mix_small()
        if j == 0 and b == 0:
            early[6 + q // 2].wait()
        for i in range(j):
            here = slice(i * B, (i + 1) * B)
            tr[s, :, here] = pk[s, here, :].T
        if j == 0:
            x, y, z = thirds(invs[q // 2, b])
            for i, third in enumerate((x, x, y, x, y, z)):
                inv_s[:, i * D:(i + 1) * D] = third
        x, y, z = thirds(nv[s])
        prod = mm(inv_s[...], jnp.concatenate((x, y, x, z, y, x), axis=0), NN) * decay[1]
        if q < 2:
            pv[s] = prod
        else:
            pt[s] = prod.T
        for c in stores(u):
            c.start()
        if u + ahead < len(units):
            if u + ahead >= deep:
                for c in stores(u + ahead - deep):
                    c.wait()
            for c in loads(u + ahead):
                c.start()
    for c in late:
        c.wait()
    for u in range(len(units) - deep, len(units)):
        for c in stores(u):
            c.wait()


def finish(decay, tris, smalls, prods, s_up_old, a_up_old, s_down_old, inv_u, inv_q):
    big = jax.ShapeDtypeStruct(s_up_old.shape, f32)
    small = jax.ShapeDtypeStruct(a_up_old.shape, f32)
    deep = 6
    return pl.pallas_call(
        final_kernel,
        in_specs=[SCALARS] + [ANY] * 16,
        out_specs=[ANY] * 6,
        out_shape=[big, big, jax.ShapeDtypeStruct((2, D, FF), f32), jax.ShapeDtypeStruct((2, FF, D), f32), small, small],
        scratch_shapes=[pltpu.VMEM((deep, FF, B), f32), pltpu.VMEM((deep, B, FF), f32)]
        + [pltpu.VMEM((deep, D, B), f32)] * 2 + [pltpu.VMEM((deep, B, D), f32), pltpu.VMEM((D, 6 * D), bf16)]
        + [pltpu.VMEM((4,) + SMALL, f32)] + [pltpu.VMEM((2,) + a_up_old.shape, f32)] * 3
        + [pltpu.SemaphoreType.DMA((deep, 3))] * 2 + [pltpu.SemaphoreType.DMA((10,))],
        compiler_params=pltpu.CompilerParams(vmem_limit_bytes=63 * MIB),
        name="finish")(decay, *[t.reshape(TRI, B) for t in tris], *prods, *smalls, a_up_old, s_down_old, inv_u, inv_q)


def solution(mesh):
    axis_size = mesh.shape["data"]
    tile = 512

    def local_step(tok, grad, w_up, w_down, a_up_old, s_up_old, a_down_old, s_down_old,
                   a_up_inv, s_up_inv, a_down_inv, s_down_inv, factor_decay):
        total = tok.shape[0]
        steps = total // tile
        inv_n = 1.0 / (total * axis_size)
        acts = [pltpu.VMEM((FF, tile), bf16)] * 2
        w_t = pltpu.VMEM((FF, D), bf16)
        unit = 2 * total * FF * D
        wide_out, small_out, tri_out = (WIDE, f32, "w"), (SMALL, f32, "w"), ((TRI, B), f32, "w")
        long_out, short_out = ((FF, total), bf16, "cf"), ((D, total), bf16, "cb")
        board = Board()
        decay = jnp.stack((factor_decay, jnp.float32(inv_n)))
        board.arrays["decay"] = decay
        pre0, u1, ad0, au0, sd1 = run_stage(
            board, stage1, "stage1", 2 * tile, [0.0] * (steps // 2),
            ((tok, "r"), (grad, "r"), (w_up, 0), (w_down, 0)),
            (long_out, ((D, total), bf16, "c"), tri_out, small_out, small_out),
            [pltpu.VMEM((FF, 2 * tile), bf16), w_t, pltpu.VMEM((D, FF), bf16)], 5 * unit, 0)
        board.add("ad0", "tri", CUTS["ad0"], ad0, a_down_old, 0)
        board.add("au0", "small", CUTS["au0"], au0)
        board.add("sd1", "small", CUTS["sd1"], sd1)
        pre1, ad1, au1, dwd1 = run_stage(
            board, stage2, "stage2", tile, [2.2] + [3.5] * steps, ((u1, "cf"), (w_up, 1), (u1, "cb"), (grad, "rb")),
            (long_out, tri_out, small_out, wide_out), acts + [w_t], 5 * unit, 1)
        board.add("ad1", "tri", CUTS["ad1"], ad1, a_down_old, 1)
        board.add("au1", "small", CUTS["au1"], au1)
        board.add("dwd1", "wide", CUTS["dwd1"], dwd1, a_down_inv, 1)
        e1, su1, dwu1 = run_stage(
            board, stage3, "stage3", tile, [2.4] + [4.22] * steps,
            ((pre1, "cf"), (grad, "rf"), (w_down, 1), (w_up, 1), (u1, "cb")), (short_out, tri_out, wide_out), acts, 6 * unit, 2)
        board.add("su1", "tri", CUTS["su1"], su1, s_up_old, 1)
        board.add("dwu1", "wide", CUTS["dwu1"], dwu1, s_up_inv, 1)
        su0, sd0, dwd0, dwu0 = run_stage(
            board, stage4, "stage4", tile, [2.4] + [4.4] * steps,
            ((pre0, "cf"), (e1, "cf"), (w_down, 0), (tok, "rb"), (e1, "cb")),
            (tri_out, small_out, wide_out, wide_out), acts * 2, 7 * unit, 3)
        board.add("sd0", "small", CUTS["sd0"], sd0)
        board.add("dwd0", "wide", CUTS["dwd0"], dwd0, a_down_inv, 0)
        board.add("dwu0", "wide", CUTS["dwu0"], dwu0, s_up_inv, 0)
        board.add("su0", "tri", CUTS["su0"], su0, s_up_old, 0)
        run_stage(board, None, "tail", tile, [0.1], (), (), [], unit, 4, last=True)
        done = board.arrays
        new_s, new_a, p_up, p_down, new_u, new_q = finish(
            decay, [done[n + ":dst"] for n in ("ad0", "ad1", "su0", "su1")],
            [done[n + ":dst"] for n in ("au0", "au1", "sd0", "sd1")],
            [done[n + ":dst"] for n in ("dwu0", "dwu1", "dwd0", "dwd1")],
            s_up_old, a_up_old, s_down_old, a_up_inv, s_down_inv)
        return p_up, p_down, new_u, new_s, new_a, new_q

    batch_spec = P("data", None)
    replicated = P()
    return jax.shard_map(local_step, mesh=mesh, in_specs=(batch_spec, batch_spec) + (replicated,) * 11,
                         out_specs=(replicated,) * 6, check_vma=False)
```

```python
import functools

import jax
import jax.numpy as jnp
from jax import lax
from jax.experimental import pallas as pl
from jax.experimental.pallas import tpu as pltpu
from jax.sharding import PartitionSpec as P

bf16 = jnp.bfloat16
f32 = jnp.float32
D, FF, B = 384, 1536, 256
NB = FF // B
TRI = sum((j + 1) * B for j in range(NB))
NN = (((1,), (0,)), ((), ()))
NT = (((1,), (1,)), ((), ()))
TN = (((0,), (0,)), ((), ()))
TT = (((0,), (1,)), ((), ()))
GELU_K = 0.7978845608028654
GELU_C = 0.044715 * GELU_K
MIB = 1 << 20


def mm(left, right, dims):
    return lax.dot_general(left, right, dims, preferred_element_type=f32)


def half_sig(pre):
    cubic = GELU_C * (pre * pre)
    return 0.5 * jnp.tanh(pre * (cubic + GELU_K)) + 0.5, cubic


def gelu_back(pre, sig, cubic):
    hid = pre * sig
    return hid, sig + (hid * (1.0 - sig)) * (6.0 * cubic + 2.0 * GELU_K)


def add_tri(acc, mat):
    off = 0
    for j in range(NB):
        rows = (j + 1) * B
        acc[off:off + rows, :] += mm(mat[:rows, :], mat[j * B:rows, :], NT)
        off += rows


def add_small_tn(acc, rows):
    acc[0] += mm(rows[:, 0:128], rows[...], TN)
    acc[1, :, 0:256] += mm(rows[:, 128:256], rows[:, 128:384], TN)
    acc[1, :, 256:384] += mm(rows[:, 256:384], rows[:, 256:384], TN)


def add_small_nt(acc, cols):
    acc[0] += mm(cols[0:128, :], cols[...], NT)
    acc[1, :, 0:256] += mm(cols[128:256, :], cols[128:384, :], NT)
    acc[1, :, 256:384] += mm(cols[256:384, :], cols[256:384, :], NT)


def zero_first(accs):
    @pl.when(pl.program_id(0) == 0)
    def _():
        for acc in accs:
            acc[...] = jnp.zeros_like(acc)


MESH = pl.DeviceIdType.MESH
ORDERS = {key: tuple(map(int, order)) for key, order in
          (("X", "1234"), ("Y", "2134"), ("Z", "3412"), ("A", "1342"), ("B", "2341"), ("C", "3421"))}
LINKS = {0: {0: 6e5}, 1: {1: 45e3}, 2: {2: 45e3}, 3: {3: 45e3}, 4: {3: 45e3, 4: 23e3}}
LAG = 2.0
SLACK = 4.0


def PRIORITY(f):
    return f.b


LAST = 10


def my_bits():
    me = lax.axis_index("data")
    bits = [(me // (1 << d)) % 2 for d in range(5)]
    return bits, [me + (1 - 2 * bits[d]) * (1 << d) for d in range(5)]


def enter():
    for peer in my_bits()[1]:
        pl.semaphore_signal(pltpu.get_barrier_semaphore(), inc=1, device_id=(peer,), device_id_type=MESH)


def await_peers():
    pl.semaphore_wait(pltpu.get_barrier_semaphore(), 5)


def al(row):
    return pl.multiple_of(row, 8)


class Flow:
    def __init__(self, name, row0, rows, cols, order, shard_row, wide):
        self.name, self.row0, self.rows, self.cols, self.order = name, row0, rows, cols, order
        self.shard_row, self.wide, self.old = shard_row, wide, None
        self.at, self.start = 0, 0.0
        self.part = name + ":part%d" % row0

    def fan(self):
        other = Flow(self.name, self.row0, self.rows, self.cols, self.order, self.shard_row, True)
        other.at = 5
        return other

    def dim(self, s):
        if s in (0, LAST - 1):
            return 0
        return self.order[s - 1] if s < 5 else self.order[LAST - 2 - s]

    def length(self, s):
        return self.rows >> s if s < 5 else self.rows >> (LAST - 1 - s)

    def kept(self, steps):
        return self.rows >> (steps - 1)

    def open(self, a, b):
        self.a, self.b = a, b
        n = b - a
        out = [pltpu.SemaphoreType.DMA((3,)), pltpu.SemaphoreType.DMA((n,)), pltpu.SemaphoreType.DMA((n,))]
        if a < 5:
            out.append(pltpu.VMEM((self.rows if a == 0 else self.kept(a), self.cols), f32))
            out.append(pltpu.VMEM((sum(self.length(s) for s in range(a, min(b, 5))), self.cols), f32))
            if self.mixes():
                out.append(pltpu.VMEM((self.kept(5), self.cols), f32))
        elif a == 5 and not self.wide:
            out.append(pltpu.VMEM((self.kept(5), self.cols), f32))
        return out

    def mixes(self):
        return self.old is not None and self.a < 5 <= self.b

    def bind(self, named, scr):
        a, b, row0, rows = self.a, self.b, self.row0, self.rows
        sem_l, sem_s, sem_r = scr[:3]
        bits, peers = my_bits()
        core = bits[0]
        lens, offs = [rows], [0]
        for d in self.order:
            lens.append(lens[-1] // 2)
            offs.append(offs[-1] + bits[d] * lens[-1])
        src, dst = named.get(self.name + ":src"), named.get(self.name + ":dst")
        part_in, part_out = named.get(self.part + ":in"), named.get(self.part + ":out")
        base = offs[min(max(a, 1), 5) - 1]
        work = recv = None
        if a < 5:
            work, recv = scr[3:5]
        elif a == 5:
            work = named[self.name + ":first"].at[pl.ds(self.shard_row, self.kept(5)), :] if self.wide else scr[3]
        sends, begin_recv, locals_ = {}, {}, []

        def remote(s, x, y):
            return pltpu.make_async_remote_copy(src_ref=x, dst_ref=y, send_sem=sem_s.at[s - a], recv_sem=sem_r.at[s - a],
                                                device_id=(peers[self.dim(s)],), device_id_type=MESH)

        def final():
            return work if a == 5 else work.at[pl.ds(al(offs[4] - base), lens[4]), :]

        def spot(k):
            return dst.at[core, pl.ds(al(row0 + offs[k]), lens[k]), :]

        at = 0
        for s in range(a, b):
            if s < 5:
                begin_recv[s] = at
                to = recv.at[pl.ds(at, self.length(s)), :]
                at += self.length(s)
                if s == 0:
                    sends[s] = remote(s, src.at[1 - core, pl.ds(row0, rows), :], to)
                else:
                    gone = al(offs[s - 1] - base + (1 - bits[self.dim(s)]) * lens[s])
                    sends[s] = remote(s, work.at[pl.ds(gone, lens[s]), :], to)
            else:
                k = LAST - 1 - s
                sends[s] = remote(s, final() if s == 5 else spot(k), spot(k))
        load = place = save = old = None
        if self.mixes():
            old_array, half = self.old
            spot4 = core * half + row0 + offs[4]
            j = sum((spot4 // (B // 2 * m * (m + 1)) + 31) // 32 for m in range(1, NB))
            old = pltpu.make_async_copy(
                named[self.name + ":old"].at[old_array, pl.ds(al(spot4 - B // 2 * j * (j + 1)), lens[4]),
                                             pl.ds(pl.multiple_of(j * B, B), B)], scr[5], sem_l.at[2])
        if a == 0:
            load = pltpu.make_async_copy(src.at[core, pl.ds(row0, rows), :], work, sem_l.at[0])
        elif a < 5 or (a == 5 and not self.wide):
            load = pltpu.make_async_copy(part_in, work, sem_l.at[0])
        if a <= 5 < b:
            place = pltpu.make_async_copy(final(), spot(4), sem_l.at[1])
        if b <= 5:
            kept = work.at[pl.ds(al(offs[b - 1] - base), lens[b - 1]), :]
            save = pltpu.make_async_copy(kept, part_out, sem_l.at[1])

        def add(row, frm, count):
            for q in range(0, count, 64):
                step = min(count - q, 64)
                x, y = al(row + q), al(frm + q)
                work[pl.ds(x, step), :] = work[pl.ds(x, step), :] + recv[pl.ds(y, step), :]

        def mix():
            rho = named["decay"][0]
            x, y = pl.ds(al(offs[4] - base), lens[4]), pl.ds(begin_recv[4], lens[4])
            total = (work[x, :] + recv[y, :]) * named["scale"]
            work[x, :] = rho * scr[5][...] + (1.0 - rho) * total

        def take(s, then):
            if s == a and load is not None and a == 0:
                load.wait()
            sends[s].wait_recv()
            if s == 5 and place is not None:
                place.wait()
            if s >= 5:
                then()
            elif s == 4 and old is not None:
                old.wait()
                mix()
                then()
            elif s == 4 or s + 1 == b:
                add(offs[s] - base, begin_recv[s], lens[s])
                then()
            else:
                half = lens[s + 1]
                bit = bits[self.dim(s + 1)]
                add(offs[s] - base + (1 - bit) * half, begin_recv[s] + (1 - bit) * half, half)
                then()
                add(offs[s] - base + bit * half, begin_recv[s] + bit * half, half)

        def send(s):
            if s == 5:
                place.start()
            sends[s].start()

        def begin():
            load.start()
            if old is not None:
                old.start()
            if a == 0:
                send(0)

        def go(s):
            if s > a:
                take(s - 1, lambda: send(s))
            else:
                if load is not None:
                    load.wait()
                send(s)

        def stop():
            take(b - 1, save.start if save is not None else lambda: None)

        def end():
            if save is not None:
                save.wait()
            for s in range(a, b):
                sends[s].wait_send()

        return {"begin": begin, "go": go, "stop": lambda s: stop(), "end": end}


class First:
    def __init__(self, name, flows, inverse, block):
        self.name, self.flows, self.inverse, self.block, self.done = name, flows, inverse, block, False
        self.fans = [f.fan() for f in flows]

    def open(self):
        rows = pltpu.VMEM((24, 768), f32)
        return [pltpu.SemaphoreType.DMA((4,)), pltpu.SemaphoreType.DMA((3,)), pltpu.SemaphoreType.DMA((3,)),
                rows, rows, rows, pltpu.VMEM((FF, 768), f32)]

    def bind(self, named, scr):
        sem_l, sem_s, sem_r, own, other, prod, inv_v = scr
        named[self.name + ":first"] = prod
        bits, peers = my_bits()
        core = bits[0]
        inv = named[self.name + ":inv"]
        copies, swaps = [], []
        for i, flow in enumerate(self.flows):
            rows = named.get(flow.part + ":out", named.get(flow.part + ":in"))
            spot = pl.ds(flow.shard_row, flow.kept(5))
            copies.append(pltpu.make_async_copy(rows, own.at[spot, :], sem_l.at[i]))
            swaps.append(pltpu.make_async_remote_copy(
                src_ref=rows, dst_ref=other.at[spot, :], send_sem=sem_s.at[i], recv_sem=sem_r.at[i],
                device_id=(peers[0],), device_id_type=MESH))
        copies.append(pltpu.make_async_copy(
            inv.at[self.block, :, pl.ds(pl.multiple_of(core * 768, 128), 768)], inv_v, sem_l.at[3]))

        def begin():
            for copy in copies + swaps:
                copy.start()

        def go(s):
            for copy in copies + swaps:
                copy.wait()
            prod[...] = (precise(own[...], inv_v[pl.ds(al(core * 768), 768), :])
                         + precise(other[...], inv_v[pl.ds(al((1 - core) * 768), 768), :]))

        return {"begin": begin, "go": go}


def plan(flows, firsts, tick_us, last, over=0.0):
    times = [0.0]
    for us in tick_us:
        times.append(times[-1] + us)
    limit = 1e9 if last else times[-1]
    free, now_rest = {}, times[-1]
    slots, rest = [[] for _ in tick_us], []
    ready = {f: f.start for f in flows}
    phase = {f: "new" for f in flows}
    for f in flows:
        f.a = f.b = f.at
    fstate = {f: "new" for f in firsts}
    fready = {}

    def arrival(f, s, now):
        links = LINKS[f.dim(s)]
        size = f.length(s) * f.cols * 4
        begin = max([now] + [free.get(link, 0.0) for link in links])
        return begin, max(begin + size / rate for rate in links.values()), size

    def send(f, s, now):
        begin, end, size = arrival(f, s, now)
        for link, rate in LINKS[f.dim(s)].items():
            free[link] = begin + size / rate
        f.b = s + 1
        ready[f] = end + LAG

    def allowed(f, s, now):
        return last or (now < limit and arrival(f, s, now)[1] + LAG < limit + over)

    def clear(f, s, now):
        return arrival(f, s, now)[0] <= now + SLACK

    def move(f, now):
        if ready[f] > now:
            return None
        if phase[f] == "new":
            if f.at >= LAST or f.wide and f.at == 5:
                return None
            if not allowed(f, f.at, now + (LAG if 0 < f.at <= 5 else 0.0)):
                return None
            if not clear(f, f.at, now):
                return None
            if f.at == 0:
                phase[f] = "run"
                send(f, 0, now)
                return "begin", 0
            if f.at <= 5:
                phase[f] = "loaded"
                ready[f] = now + LAG
                f.b = f.at + 1
                return "begin", 0
            phase[f] = "run"
            send(f, f.at, now)
            return "go", f.at
        if phase[f] == "loaded":
            phase[f] = "run"
            send(f, f.at, now)
            return "go", f.at
        if phase[f] == "run":
            s = f.b
            if s == LAST or f.wide and s == 5 or not allowed(f, s, now):
                phase[f] = "saved"
                ready[f] = now + LAG
                return "stop", s
            if not clear(f, s, now):
                return None
            send(f, s, now)
            return "go", s
        if phase[f] == "saved":
            phase[f] = "done"
            return "end", 0
        return None

    def first_move(f, now):
        if f.done or fready.get(f, 0.0) > now:
            return None
        if fstate[f] == "new":
            ok = all(x.b == 5 and phase.get(x, "done") in ("new", "done") for x in f.flows)
            if not ok or not (last or now + 20.0 < limit):
                return None
            fstate[f] = "loaded"
            fready[f] = now + 5.0
            return "begin", 0
        if fstate[f] == "loaded":
            fstate[f] = "done"
            return "go", 0
        return None

    def sweep(now, out):
        again = True
        while again:
            again = False
            for f in sorted(flows, key=PRIORITY):
                e = move(f, now)
                if e:
                    out.append((f,) + e)
                    again = True
                    break
            for f in firsts:
                e = first_move(f, now)
                if e:
                    out.append((f,) + e)
                    again = True
                    if fstate[f] == "done":
                        for x in f.fans:
                            flows.append(x)
                            x.a = 5
                            phase[x] = "run"
                            send(x, 5, now)
                            out.append((x, "go", 5))

    for t, now in enumerate(times[:-1]):
        if t or last:
            sweep(now, slots[t])
    now = times[-1]
    while True:
        sweep(now, rest)
        later = [ready[f] for f in flows if phase[f] in ("loaded", "run", "saved") and ready[f] > now]
        later += [fready[f] for f in firsts if fstate[f] == "loaded" and fready[f] > now]
        held = any(phase[f] in ("loaded", "run") or last and phase[f] == "new" and f.at < LAST and not (f.wide and f.at == 5)
                   for f in flows)
        if not later and not held:
            return slots, rest, now
        now = min(later + ([now + 1.0] if held else []))


def tri_col(acc, mat, j):
    rows = (j + 1) * B
    off = B * j * (j + 1) // 2
    acc[off:off + rows, :] += mm(mat[:rows, :], mat[j * B:rows, :], NT)


def staged(dot, act, backs, shifts, accs, setup=None):
    step, last = pl.program_id(0), pl.num_programs(0) - 1

    def shift():
        for old, new in shifts:
            old[...] = new[...]

    @pl.when(step == 0)
    def _():
        for acc in accs:
            acc[...] = jnp.zeros_like(acc)
        if setup is not None:
            setup()
        for k in range(NB):
            act(k, dot(k))

    @pl.when((step > 0) & (step < last))
    def _():
        shift()
        for k, back in enumerate(backs):
            value = dot(k)
            back()
            act(k, value)

    @pl.when(step == last)
    def _():
        shift()
        for back in backs:
            back()


def plain(dot, act, backs, accs, setup):
    @pl.when(pl.program_id(0) == 0)
    def _():
        for acc in accs:
            acc[...] = jnp.zeros_like(acc)
        setup()

    for k in range(NB):
        act(k, dot(k))
    for back in backs:
        back()


def block(k):
    return slice(k * B, (k + 1) * B)


def tri_pieces(acc, mat, *more):
    pieces = [(5,), (4,), (3, 0), (2, 1)]

    def run(cols, fns):
        for j in cols:
            tri_col(acc, mat, j)
        for fn in fns:
            fn()

    return [functools.partial(run, cols, ()) for cols in pieces] + [functools.partial(run, (), fns) for fns in more]


def gelu_act(pre_out, new_s):
    def act(k, value):
        pre = value.astype(bf16)
        pre_out[block(k), :] = pre
        pre = pre.astype(f32)
        new_s[block(k), :] = (pre * half_sig(pre)[0]).astype(bf16)
    return act


def stage1(tok, grad, w_up, w_down, pre_out, next_out, tri, small_u, small_q, hid_s, up_s, down_s):
    def setup():
        up_s[...] = w_up[0].T
        down_s[...] = w_down[0].T

    def dot(k):
        return mm(up_s[block(k), :], tok[...], NT)

    def down():
        next_out[...] = mm(down_s[...], hid_s[...], NN).astype(bf16)

    def smalls():
        add_small_tn(small_u, tok)
        add_small_tn(small_q, grad)

    backs = [functools.partial(tri_col, tri, hid_s, j) for j in range(NB)] + [down, smalls]
    plain(dot, gelu_act(pre_out, hid_s), backs, (tri, small_u, small_q), setup)


def add_wide(acc, left, mat, dims, h):
    acc[h] += mm(left[...], mat[h * FF // 2:(h + 1) * FF // 2, :], dims)


def stage2(u_t, w_up, u_b, grad_b, pre_out, tri, small_u, dwd, new_s, hid_s, up_s):
    def setup():
        up_s[...] = w_up[0].T

    def dot(k):
        return mm(up_s[block(k), :], u_t[...], NN)

    wide = [functools.partial(add_wide, dwd, grad_b, hid_s, TT, h) for h in PAIR]
    backs = tri_pieces(tri, hid_s, wide[:1], (wide[1], lambda: add_small_nt(small_u, u_b)))
    staged(dot, gelu_act(pre_out, new_s), backs, ((hid_s, new_s),), (tri, small_u, dwd), setup)


def stage3(pre_in, grad, w_down, w_up, u_b, err_out, tri, dwu, new_s, g_s):
    def dot(k):
        return mm(w_down[0, block(k), :], grad[...], NT)

    def act(k, value):
        d_hid = value.astype(bf16).astype(f32)
        pre = pre_in[block(k), :].astype(f32)
        sig, cubic = half_sig(pre)
        new_s[block(k), :] = (d_hid * gelu_back(pre, sig, cubic)[1]).astype(bf16)

    def up():
        err_out[...] = mm(w_up[0], g_s[...], NN).astype(bf16)

    wide = [functools.partial(add_wide, dwu, u_b, g_s, NT, h) for h in PAIR]
    staged(dot, act, tri_pieces(tri, g_s, wide, (up,)), ((g_s, new_s),), (tri, dwu))


def stage4(pre_in, err_t, w_down, tok_b, err_b, tri, small_q, dwd, dwu, new_h, hid_s, new_g, g_s):
    def dot(k):
        return mm(w_down[0, block(k), :], err_t[...], NN)

    def act(k, value):
        d_hid = value.astype(bf16).astype(f32)
        pre = pre_in[block(k), :].astype(f32)
        sig, cubic = half_sig(pre)
        hid, slope = gelu_back(pre, sig, cubic)
        new_h[block(k), :] = hid.astype(bf16)
        new_g[block(k), :] = (d_hid * slope).astype(bf16)

    downs = [functools.partial(add_wide, dwd, err_b, hid_s, NT, h) for h in PAIR]
    ups = [functools.partial(add_wide, dwu, tok_b, g_s, TT, h) for h in PAIR]
    backs = tri_pieces(tri, g_s, downs, ups + [lambda: add_small_nt(small_q, err_b)])
    staged(dot, act, backs, ((hid_s, new_h), (g_s, new_g)), (tri, small_q, dwd, dwu))


SMALL = (2, 128, 384)
WIDE = (2, 384, 768)
TRI_SHAPE = (2, TRI // 2, B)
CUTS = {
    "ad0": "128B,1024A,1024X,512C", "au0": "128Z", "sd1": "128Y",
    "ad1": "512X,1024Y,512Z,128Z,512Y", "au1": "128Z", "dwd1": "256X,128Y",
    "su1": "512B,128A,512A,512Y,512X,512B", "dwu1": "384Y",
    "sd0": "128X", "dwd0": "128C,128B,128Y", "dwu0": "256X,128B", "su0": "512A,128Y,512A,512Y,512X,512Z",
}
FORMS = {"tri": TRI_SHAPE, "wide": WIDE, "small": SMALL}


def flows_of(name, form, cuts):
    flows, row = [], 0
    for cut in cuts.split(","):
        flows.append(Flow(name, row, int(cut[:-1]), FORMS[form][2], ORDERS[cut[-1]], row // 16, form == "wide"))
        row += flows[-1].rows
    return flows


def precise(left, right):
    return lax.dot_general(left, right, NN, precision=lax.Precision.HIGHEST, preferred_element_type=f32)


def thirds(x):
    parts = []
    for _ in range(3):
        parts.append(x.astype(bf16))
        x = x - parts[-1].astype(f32)
    return parts


def tile_spec(kind, shape, tile):
    n = shape[0 if kind[0] == "r" else 1] // tile

    def at(i):
        if "b" in kind:
            return jnp.maximum(i - 1, 0)
        return jnp.minimum(i, n - 1) if "f" in kind else i

    if kind[0] == "r":
        return pl.BlockSpec((tile, D), lambda i: (at(i), 0))
    return pl.BlockSpec((shape[0], tile), lambda i: (0, at(i)))


def whole_spec(shape):
    zeros = (0,) * len(shape)
    return pl.BlockSpec(shape, lambda i: zeros, pipeline_mode=pl.Buffered(1))


def block_spec(shape, b):
    return pl.BlockSpec((1,) + shape[1:], lambda i: (b, 0, 0), pipeline_mode=pl.Buffered(1))


PAIR = range(2)
ANY = pl.BlockSpec(memory_space=pl.ANY)
SCALARS = pl.BlockSpec(memory_space=pltpu.SMEM)


class Board:
    def __init__(self, decay, scale):
        self.flows, self.firsts, self.arrays, self.forms = [], [], {}, {}
        self.scale = scale
        self.arrays["decay"] = decay

    def add(self, name, form, cuts, array, other=None, block=0):
        flows = flows_of(name, form, cuts)
        self.flows += flows
        self.forms[name] = FORMS[form]
        self.arrays[name + ":src"] = array.reshape(self.forms[name])
        if form == "wide":
            self.firsts.append(First(name, flows, other, block))
            self.arrays[name + ":inv"] = other
        elif form == "tri":
            for f in flows:
                f.old = (block, TRI // 2)
            self.arrays[name + ":old"] = other

    def plan(self, tick_us, last):
        for f in self.flows:
            f.at = f.b if hasattr(f, "b") else f.at
        flows = [f for f in self.flows if f.at < LAST and not (f.wide and f.at == 5)]
        idle = [f for f in self.flows if f.wide and f.at == 5]
        for f in idle:
            f.a = f.b = f.at
        slots, rest, end = plan(flows, self.firsts, tick_us, last)
        runs = [f for f in self.firsts if f.fans[0] in flows]
        self.firsts = [f for f in self.firsts if f not in runs]
        self.flows = [f for f in flows + idle if f.b < LAST or f.a < f.b]
        moving = [f for f in flows if f.a < f.b]
        ins, outs = [], {}
        for f in moving:
            if f.a == 0:
                ins.append(f.name + ":src")
            elif f.a < 5 or (f.a == 5 and not f.wide):
                ins.append(f.part + ":in")
            if f.mixes():
                ins += ["decay", f.name + ":old"]
            if f.b <= 5:
                outs[f.part + ":out"] = (f.kept(f.b), f.cols)
            else:
                outs[f.name + ":dst"] = self.forms[f.name]
        for first in runs:
            ins.append(first.name + ":inv")
            ins += [f.part + ":in" for f in first.flows if f.part + ":out" not in outs]
        ins += [name for name in outs if name in self.arrays]
        return slots, rest, end, moving, runs, list(dict.fromkeys(ins)), outs

    def keep(self, outs, values):
        for name, value in zip(outs, values):
            self.arrays[name.replace(":out", ":in")] = value


def run_stage(board, body, name, tile, tick_us, ins, outs, scratch, flops, cid, last=False):
    def spec(kind, shape):
        if kind == "w":
            return whole_spec(shape)
        return block_spec(shape, kind) if isinstance(kind, int) else tile_spec(kind, shape, tile)

    steps = len(tick_us)
    slots, rest, end, moving, runs, m_ins, m_outs = board.plan(tick_us, last)
    scr = [job.open(job.a, job.b) if isinstance(job, Flow) else job.open() for job in runs + moving]
    n_in, n_min, n_out, n_mout, n_scr = len(ins), len(m_ins), len(outs), len(m_outs), len(scratch)

    def kernel(*refs):
        refs = list(refs)

        def pull(n):
            return [refs.pop(0) for _ in range(n)]

        c_in, m_in, c_out, m_out, c_scr = pull(n_in), pull(n_min), pull(n_out), pull(n_mout), pull(n_scr)
        named = dict(zip(m_ins, m_in))
        named.update(zip(m_outs, m_out), scale=board.scale)
        step = pl.program_id(0)
        events = {}
        if moving:
            pl.when(step == 0)(enter)
            pl.when(step == min(1, steps - 1))(await_peers)
        for job, s in zip(runs + moving, scr):
            events[job] = job.bind(named, pull(len(s)))

        def fire(slot):
            for job, what, s in slot:
                if what in ("go", "stop"):
                    events[job][what](s)
                else:
                    events[job][what]()

        for t in range(steps):
            if slots[t]:
                pl.when(step == t)(functools.partial(fire, slots[t]))
        if body is not None:
            body(*c_in, *c_out, *c_scr)
        if rest:
            pl.when(step == steps - 1)(functools.partial(fire, rest))

    params = dict(vmem_limit_bytes=63 * MIB)
    if moving:
        params.update(collective_id=cid, has_side_effects=True)
    values = pl.pallas_call(
        kernel, grid=(steps,),
        in_specs=[spec(kind, arr.shape) for arr, kind in ins] + [SCALARS if m == "decay" else ANY for m in m_ins],
        out_specs=[spec(kind, shape) for shape, dtype, kind in outs] + [ANY] * n_mout,
        out_shape=[jax.ShapeDtypeStruct(shape, dtype) for shape, dtype, kind in outs]
        + [jax.ShapeDtypeStruct(shape, f32) for shape in m_outs.values()],
        scratch_shapes=list(scratch) + [x for s in scr for x in s],
        input_output_aliases={n_in + m_ins.index(m): n_out + i for i, m in enumerate(m_outs) if m in m_ins},
        compiler_params=pltpu.CompilerParams(**params),
        cost_estimate=pl.CostEstimate(flops=flops, bytes_accessed=40 * MIB, transcendentals=0),
        name=name)(*[arr for arr, _ in ins], *[board.arrays[m] for m in m_ins])
    board.keep(m_outs, values[n_out:])
    return values[:n_out]


def final_kernel(mean, decay, t0, t1, t2, t3, n0, n1, n2, n3, *refs):
    small_in, small_out, outs, scratch = refs[:8], refs[12:14], refs[8:12], refs[14:]
    new_s, new_a, p_up, p_down = outs
    pk, tr, nv, pv, pt, inv_s, sums, olds, invs, news, sem_in, sem_out, sem_small = scratch
    rho = decay[0]
    scale = (1.0 - rho) * mean
    deep = pk.shape[0]
    ahead = deep // 2
    units = []
    for q, (src, new, n) in enumerate(((t0, new_a, n0), (t1, new_a, n1), (t2, new_s, n2), (t3, new_s, n3))):
        off = 0
        for j in range(NB):
            units.append((q, src, new, q % 2, j, off, n))
            off += (j + 1) * B

    def loads(u):
        q, src, new, b, j, off, n = units[u]
        rows, s = (j + 1) * B, u % deep
        parts = ((src.at[pl.ds(off, rows), :], pk.at[s, pl.ds(0, rows), :]),
                 (n.at[j // 3, :, pl.ds(j % 3 * B, B)], nv.at[s]))
        return [pltpu.make_async_copy(x, y, sem_in.at[s, i]) for i, (x, y) in enumerate(parts)]

    def stores(u):
        q, src, new, b, j, off, n = units[u]
        rows, s = (j + 1) * B, u % deep
        parts = [(pk.at[s, pl.ds(0, rows), :], new.at[b, pl.ds(0, rows), pl.ds(j * B, B)])]
        if q < 2:
            parts.append((pv.at[s], p_up.at[b, :, pl.ds(j * B, B)]))
        else:
            parts.append((pt.at[s], p_down.at[b, pl.ds(j * B, B), :]))
        if j:
            parts.append((tr.at[s, :, pl.ds(0, j * B)], new.at[b, pl.ds(j * B, B), pl.ds(0, j * B)]))
        return [pltpu.make_async_copy(x, y, sem_out.at[s, i]) for i, (x, y) in enumerate(parts)]

    places = [sums.at[i] for i in range(4)] + [olds.at[i] for i in PAIR] + [invs.at[i] for i in PAIR]
    early = [pltpu.make_async_copy(x, y, sem_small.at[i]) for i, (x, y) in enumerate(zip(small_in, places))]
    late = [pltpu.make_async_copy(news.at[i], small_out[i], sem_small.at[len(early) + i]) for i in PAIR]

    def mix_small():
        h = B // 2
        for c in early[:6]:
            c.wait()
        for i in range(4):
            acc, old, new = sums.at[i], olds.at[i // 2, i % 2], news.at[i // 2, i % 2]
            top = rho * old[:h, :] + scale * acc[0]
            mid = rho * old[h:B, h:] + scale * acc[1, :, :B]
            low = rho * old[B:, B:] + scale * acc[1, :, B:]
            new[:h, :] = top
            new[h:B, h:] = mid
            new[B:, B:] = low
            new[h:, :h] = top[:, h:].T
            new[B:, h:B] = mid[:, h:].T
        for c in late:
            c.start()

    for c in early[6:]:
        c.start()
    for u in range(ahead):
        for c in loads(u):
            c.start()
    for c in early[:6]:
        c.start()
    for u, (q, src, new, b, j, off, n) in enumerate(units):
        s = u % deep
        for c in loads(u):
            c.wait()
        if u == NB:
            mix_small()
        if j == 0 and b == 0:
            early[6 + q // 2].wait()
        for i in range(j):
            here = slice(i * B, (i + 1) * B)
            tr[s, :, here] = pk[s, here, :].T
        if j == 0:
            x, y, z = thirds(invs[q // 2, b])
            for i, third in enumerate((x, x, y, x, y, z)):
                inv_s[:, i * D:(i + 1) * D] = third
        x, y, z = thirds(nv[s])
        prod = mm(inv_s[...], jnp.concatenate((x, y, x, z, y, x), axis=0), NN) * mean
        if q < 2:
            pv[s] = prod
        else:
            pt[s] = prod.T
        for c in stores(u):
            c.start()
        if u + ahead < len(units):
            if u + ahead >= deep:
                for c in stores(u + ahead - deep):
                    c.wait()
            for c in loads(u + ahead):
                c.start()
    for c in late:
        c.wait()
    for u in range(len(units) - deep, len(units)):
        for c in stores(u):
            c.wait()


def finish(mean, decay, tris, smalls, prods, s_up_old, a_up_old, s_down_old, inv_u, inv_q):
    big = jax.ShapeDtypeStruct(s_up_old.shape, f32)
    small = jax.ShapeDtypeStruct(a_up_old.shape, f32)
    deep = 6
    return pl.pallas_call(
        functools.partial(final_kernel, mean),
        in_specs=[SCALARS] + [ANY] * 16,
        out_specs=[ANY] * 6,
        out_shape=[big, big, jax.ShapeDtypeStruct((2, D, FF), f32), jax.ShapeDtypeStruct((2, FF, D), f32), small, small],
        scratch_shapes=[pltpu.VMEM((deep, FF, B), f32), pltpu.VMEM((deep, B, FF), f32)]
        + [pltpu.VMEM((deep, D, B), f32)] * 2 + [pltpu.VMEM((deep, B, D), f32), pltpu.VMEM((D, 6 * D), bf16)]
        + [pltpu.VMEM((4,) + SMALL, f32)] + [pltpu.VMEM((2,) + a_up_old.shape, f32)] * 3
        + [pltpu.SemaphoreType.DMA((deep, 3))] * 2 + [pltpu.SemaphoreType.DMA((10,))],
        compiler_params=pltpu.CompilerParams(vmem_limit_bytes=63 * MIB),
        name="finish")(decay, *[t.reshape(TRI, B) for t in tris], *prods, *smalls, a_up_old, s_down_old, inv_u, inv_q)


def solution(mesh):
    axis_size = mesh.shape["data"]
    tile = 512

    def local_step(tok, grad, w_up, w_down, a_up_old, s_up_old, a_down_old, s_down_old,
                   a_up_inv, s_up_inv, a_down_inv, s_down_inv, factor_decay):
        total = tok.shape[0]
        steps = total // tile
        inv_n = 1.0 / (total * axis_size)
        acts = [pltpu.VMEM((FF, tile), bf16)] * 2
        w_t = pltpu.VMEM((FF, D), bf16)
        unit = 2 * total * FF * D
        wide_out, small_out, tri_out = (WIDE, f32, "w"), (SMALL, f32, "w"), ((TRI, B), f32, "w")
        long_out, short_out = ((FF, total), bf16, "cf"), ((D, total), bf16, "cb")
        decay = factor_decay.reshape(1)
        board = Board(decay, inv_n)
        pre0, u1, ad0, au0, sd1 = run_stage(
            board, stage1, "stage1", 2 * tile, [0.0] * (steps // 2),
            ((tok, "r"), (grad, "r"), (w_up, 0), (w_down, 0)),
            (long_out, ((D, total), bf16, "c"), tri_out, small_out, small_out),
            [pltpu.VMEM((FF, 2 * tile), bf16), w_t, pltpu.VMEM((D, FF), bf16)], 5 * unit, 0)
        board.add("ad0", "tri", CUTS["ad0"], ad0, a_down_old, 0)
        board.add("au0", "small", CUTS["au0"], au0)
        board.add("sd1", "small", CUTS["sd1"], sd1)
        pre1, ad1, au1, dwd1 = run_stage(
            board, stage2, "stage2", tile, [2.2] + [3.85] * steps, ((u1, "cf"), (w_up, 1), (u1, "cb"), (grad, "rb")),
            (long_out, tri_out, small_out, wide_out), acts + [w_t], 5 * unit, 1)
        board.add("ad1", "tri", CUTS["ad1"], ad1, a_down_old, 1)
        board.add("au1", "small", CUTS["au1"], au1)
        board.add("dwd1", "wide", CUTS["dwd1"], dwd1, a_down_inv, 1)
        e1, su1, dwu1 = run_stage(
            board, stage3, "stage3", tile, [2.4] + [4.5] * steps,
            ((pre1, "cf"), (grad, "rf"), (w_down, 1), (w_up, 1), (u1, "cb")), (short_out, tri_out, wide_out), acts, 6 * unit, 2)
        board.add("su1", "tri", CUTS["su1"], su1, s_up_old, 1)
        board.add("dwu1", "wide", CUTS["dwu1"], dwu1, s_up_inv, 1)
        su0, sd0, dwd0, dwu0 = run_stage(
            board, stage4, "stage4", tile, [2.5] + [4.65] * steps,
            ((pre0, "cf"), (e1, "cf"), (w_down, 0), (tok, "rb"), (e1, "cb")),
            (tri_out, small_out, wide_out, wide_out), acts * 2, 7 * unit, 3)
        board.add("sd0", "small", CUTS["sd0"], sd0)
        board.add("dwd0", "wide", CUTS["dwd0"], dwd0, a_down_inv, 0)
        board.add("dwu0", "wide", CUTS["dwu0"], dwu0, s_up_inv, 0)
        board.add("su0", "tri", CUTS["su0"], su0, s_up_old, 0)
        run_stage(board, None, "tail", tile, [0.1], (), (), [], unit, 4, last=True)
        done = board.arrays
        new_s, new_a, p_up, p_down, new_u, new_q = finish(
            inv_n, decay, [done[n + ":dst"] for n in ("ad0", "ad1", "su0", "su1")],
            [done[n + ":dst"] for n in ("au0", "au1", "sd0", "sd1")],
            [done[n + ":dst"] for n in ("dwu0", "dwu1", "dwd0", "dwd1")],
            s_up_old, a_up_old, s_down_old, a_up_inv, s_down_inv)
        return p_up, p_down, new_u, new_s, new_a, new_q

    batch_spec = P("data", None)
    replicated = P()
    return jax.shard_map(local_step, mesh=mesh, in_specs=(batch_spec, batch_spec) + (replicated,) * 11,
                         out_specs=(replicated,) * 6, check_vma=False)
```
